32 devices in a mesh: aper: 2 (over x), rng: 4 (over z), ang: 4 (over y, core).
Axes of the slice: x: 2, y: 2, z: 4, core: 2. Of those that a mesh axis runs over, the one named last changes fastest.
Arguments:
- subimages: bfloat16 [8, 2, 1024, 512], P('aper', None, 'ang', 'rng'), may hold values from -6 to 6
- beam_offsets: int32 [3, 2, 2, 1024], P(None, None, None, 'ang'), may hold values from -4 to 0
- range_offsets: int32 [3, 2, 2, 1024], P(None, None, None, 'ang'), may hold values from -4 to 3
- beam_taps: bfloat16 [3, 2, 2, 4, 1024], P(None, None, None, None, 'ang'), may hold values from 0.14941406 to 0.59765625
- range_frac: float32 [3, 2, 2, 1024], P(None, None, None, 'ang'), may hold values from 0 to 1
- phase_base: float32 [8, 3, 2, 1024], P('aper', None, None, 'ang'), may hold values from -3.140625 to 3.140625
- phase_rate: float32 [3, 2, 1024], P(None, None, 'ang'), may hold values from -6 to 6
- final_phase: float32 [8, 1024], P(None, 'ang'), may hold values from -3.140625 to 3.140625
Outputs:
- image: float32 [2, 4, 256, 512], P(None, 'ang', 'aper', 'rng')
The draws below stay inside these ranges and needn't reach their ends.
Inputs may be any that keep to these rules, and one draw needn't show every extreme that they name: `beam_offsets`: the taps of parent beam p read child beams p + offset to p + offset + 3. `range_offsets`: range bin r reads the bins r + offset and r + offset + 1.
All inputs are finite; a program needn't handle non-finite values.
Results may differ from the reference program's by a relative error of at most 0.0046.
Values may be sent and summed in bfloat16 or wider, within the bound.
No kernel may reach another device: no remote copies, remote signals or barrier semaphores. Data moves between devices by JAX's collectives and lax.ppermute only.
A program may use at most 64 MiB of HBM per device.

```python
import math
import jax
import jax.numpy as jnp
from jax import lax

B_DEV = 256
LEVELS = 3
TAPS = 4
HALO = 4
S = 8
NB = 1024
NR = 512
N_ANG = 4


def place_ends(values, own_key, low, largest):
    longest = values.shape.index(max(values.shape))
    spots = []
    for shift in (0, 1):
        where = [jax.random.randint(jax.random.fold_in(own_key, axis), (), 0, length) for axis, length in enumerate(values.shape)]
        where[longest] = (where[longest] + shift) % values.shape[longest]
        spots.append(tuple(where))
    return values.at[spots[0]].set(low).at[spots[1]].set(largest)


def steps_of(key, shape, shards, low, largest):
    def one(axis_at, blocks):
        draws = jax.random.uniform(jax.random.fold_in(jax.random.fold_in(key, 6), axis_at), (blocks,), jnp.float32, low / len(shards), largest / len(shards))
        return jnp.repeat(jnp.exp(draws), shape[axis_at] // blocks).reshape((-1,) + (1,) * (len(shape) - axis_at - 1))

    gain = one(*shards[0])
    for cut in shards[1:]:
        gain = gain * one(*cut)
    return gain


def normal_values(own_key, extent, width, limit, cuts=(), kind=jnp.bfloat16):
    entries = width * jax.random.normal(own_key, extent, jnp.float32)
    if cuts:
        entries = entries * steps_of(own_key, extent, cuts, -0.22, 0.18)
    return jnp.clip(entries, -limit, limit).astype(kind)


def setup_inputs(seed: int = 0) -> dict:
    keys = jax.random.split(jax.random.key(seed), 9)
    return {
        "subimages": normal_values(keys[0], (S, 2, NB, NR), 1.0, 6.0, ((0, 2), (2, 4), (3, 4))),
        "beam_offsets": place_ends(jax.random.randint(keys[1], (LEVELS, 2, 2, NB), -HALO, HALO - TAPS + 1), jax.random.fold_in(keys[1], 1), -HALO, HALO - TAPS).astype(jnp.int32),
        "range_offsets": place_ends(jax.random.randint(keys[2], (LEVELS, 2, 2, NB), -HALO, HALO), jax.random.fold_in(keys[2], 1), -HALO, HALO - 1).astype(jnp.int32),
        "beam_taps": jnp.clip(0.14941406 + 0.4482422 * jax.random.uniform(keys[3], (LEVELS, 2, 2, TAPS, NB), jnp.float32) ** steps_of(keys[3], (LEVELS, 2, 2, TAPS, NB), ((4, 4),), -0.2, 0.2), 0.14941406, 0.59765625).astype(jnp.bfloat16),
        "range_frac": jnp.clip(1.0 * jax.random.uniform(keys[4], (LEVELS, 2, 2, NB), jnp.float32) ** steps_of(keys[4], (LEVELS, 2, 2, NB), ((3, 4),), -0.2, 0.2), 0.0, 1.0),
        "phase_base": jnp.clip(jax.random.uniform(keys[5], (S, LEVELS, 2, NB), jnp.float32, -3.140625, 3.140625), -3.140625, 3.140625),
        "phase_rate": jnp.clip(jax.random.uniform(keys[6], (LEVELS, 2, NB), jnp.float32, -6.0, 6.0) * steps_of(keys[6], (LEVELS, 2, NB), ((2, 4),), -0.4, 0.0), -6.0, 6.0),
        "final_phase": jnp.clip(jax.random.uniform(keys[7], (S, NB), jnp.float32, -3.140625, 3.140625), -3.140625, 3.140625),
    }


def merge_one(blocks_in, level_idx, sub_index, beam_offsets, range_offsets, beam_taps, range_frac, phase_base, phase_rate):
    distance = S >> LEVELS - level_idx
    half_bit = sub_index // distance % 2
    first_sub = sub_index - half_bit * distance
    beam_ids = jnp.arange(NB, dtype=jnp.int32)
    range_ramp = jnp.arange(NR, dtype=jnp.int32).astype(jnp.float32) / NR - 0.5
    summed = jnp.zeros((2, NB, NR), jnp.float32)
    for child_idx in range(2):
        child_block = lax.dynamic_index_in_dim(blocks_in, (first_sub + child_idx * distance).astype(jnp.int32), 0, keepdims=False).astype(jnp.float32)
        padded = jnp.pad(child_block, ((0, 0), (HALO, HALO), (0, 0)))
        offsets = beam_offsets[level_idx, child_idx][half_bit]
        tap_weights = beam_taps[level_idx, child_idx][half_bit].astype(jnp.float32)
        interpolated = jnp.zeros((2, NB, NR), jnp.float32)
        for tap_idx in range(TAPS):
            row_ids = (beam_ids + HALO + offsets + tap_idx).astype(jnp.int32)
            interpolated = interpolated + tap_weights[tap_idx][None, :, None] * jnp.take(padded, row_ids, axis=1)
        range_shift = range_offsets[level_idx, child_idx][half_bit] + HALO
        fraction = range_frac[level_idx, child_idx][half_bit]
        widened = jnp.pad(interpolated, ((0, 0), (0, 0), (HALO, HALO)))
        shifted = jnp.zeros((2, NB, NR), jnp.float32)
        for offset_step in range(2 * HALO + 1):
            weight = jnp.where(range_shift == offset_step, 1.0 - fraction, 0.0) + jnp.where(range_shift + 1 == offset_step, fraction, 0.0)
            shifted = shifted + weight[None, :, None] * widened[:, :, offset_step:offset_step + NR]
        angles = phase_base[sub_index, level_idx, child_idx][:, None] + phase_rate[level_idx, child_idx][:, None] * range_ramp[None, :]
        cosine = jnp.cos(angles)
        sine_part = jnp.sin(angles)
        summed = summed + jnp.stack([cosine * shifted[0] - sine_part * shifted[1], sine_part * shifted[0] + cosine * shifted[1]])
    return summed.astype(jnp.bfloat16)

def reference(subimages, beam_offsets, range_offsets, beam_taps, range_frac, phase_base, phase_rate, final_phase):
    blocks = subimages
    for level_idx in range(LEVELS):
        blocks = lax.map(lambda sub_index: merge_one(blocks, level_idx, sub_index, beam_offsets, range_offsets, beam_taps, range_frac, phase_base, phase_rate), jnp.arange(S, dtype=jnp.int32))

    def accumulate(running, sub_index):
        child_block = blocks[sub_index].astype(jnp.float32)
        angles = final_phase[sub_index]
        cosine = jnp.cos(angles)[:, None]
        sine_part = jnp.sin(angles)[:, None]
        term = jnp.stack([cosine * child_block[0] - sine_part * child_block[1], sine_part * child_block[0] + cosine * child_block[1]])
        return (running + term, None)
    summed, unused = lax.scan(accumulate, jnp.zeros((2, NB, NR), jnp.float32), jnp.arange(S, dtype=jnp.int32))
    image = summed * (1.0 / math.sqrt(S))
    return image.reshape(2, N_ANG, B_DEV, NR)
```

```python
import functools
import math

import jax
import jax.numpy as jnp
from jax import lax
from jax.experimental import pallas as pl
from jax.experimental.pallas import tpu as pltpu
from jax.sharding import PartitionSpec as P

LEVELS = 3
TAPS = 4
HALO = 4


def with_halo(cells, sides, width):
    for axis, dim in sides:
        count = lax.axis_size(axis)
        ends = count - 1
        head = lax.slice_in_dim(cells, 0, width, axis=dim)
        tail = lax.slice_in_dim(cells, cells.shape[dim] - width, cells.shape[dim], axis=dim)
        cells = jnp.concatenate(
            [
                lax.ppermute(tail, axis, [(i, (i + 1) % count) for i in range(ends)]),
                cells,
                lax.ppermute(head, axis, [((i + 1) % count, i) for i in range(ends)]),
            ],
            axis=dim,
        )
    return cells


def partner_2(x, axis, stride):
    return lax.ppermute(x, axis, [(i, i ^ 1 << stride) for i in range(lax.axis_size(axis))])


def block_edges(blocks):
    return with_halo(blocks, (("ang", 2), ("rng", 3)), HALO)


def band_matrices(offsets, tap_weights):
    beam_count = offsets.shape[1]
    columns = jnp.arange(beam_count + 2 * HALO, dtype=jnp.int32)
    row_ids = jnp.arange(beam_count, dtype=jnp.int32)
    starting = row_ids[None, :] + HALO + offsets
    lagging = columns[None, None, :] - starting[:, :, None]
    weights = jnp.zeros(lagging.shape, jnp.float32)
    for tap_idx in range(TAPS):
        weights = weights + jnp.where(
            lagging == tap_idx, tap_weights[:, tap_idx, :, None].astype(jnp.float32), 0.0
        )
    return weights.astype(jnp.bfloat16)


def merge_level(child_blocks, halves, level_idx, tables, range_ramp):
    beam_offsets, range_offsets, beam_taps, range_frac, phase_base, phase_rate = tables
    slot_count = halves.shape[0]
    cell_count = range_ramp.shape[0]
    slot_ids = jnp.arange(slot_count, dtype=jnp.int32)
    summed = None
    for side_idx in range(2):
        child_ids = halves if side_idx == 0 else 1 - halves
        extended = child_blocks[side_idx]
        matrices = band_matrices(
            beam_offsets[level_idx][child_ids, halves], beam_taps[level_idx][child_ids, halves]
        )
        interpolated = jnp.einsum(
            "snm,sxmr->sxnr", matrices, extended, preferred_element_type=jnp.float32
        )
        range_shift = range_offsets[level_idx][child_ids, halves] + HALO
        fraction = range_frac[level_idx][child_ids, halves]
        shifted = jnp.zeros(interpolated.shape[:3] + (cell_count,), jnp.float32)
        for offset_step in range(2 * HALO + 1):
            weight = jnp.where(range_shift == offset_step, 1.0 - fraction, 0.0) + jnp.where(
                range_shift + 1 == offset_step, fraction, 0.0
            )
            shifted = (
                shifted
                + weight[:, None, :, None]
                * interpolated[:, :, :, offset_step : offset_step + cell_count]
            )
        angles = (
            phase_base[slot_ids, level_idx, child_ids][:, :, None]
            + phase_rate[level_idx][child_ids][:, :, None] * range_ramp[None, None, :]
        )
        cosine = jnp.cos(angles)
        sine_part = jnp.sin(angles)
        term = jnp.stack(
            [
                cosine * shifted[:, 0] - sine_part * shifted[:, 1],
                sine_part * shifted[:, 0] + cosine * shifted[:, 1],
            ],
            axis=1,
        )
        summed = term if summed is None else summed + term
    return summed.astype(jnp.bfloat16)


def body(
    subimages,
    beam_offsets,
    range_offsets,
    beam_taps,
    range_frac,
    phase_base,
    phase_rate,
    final_phase,
):
    slot_count = subimages.shape[0]
    beam_count = subimages.shape[2]
    cell_count = subimages.shape[3]
    aper_count = lax.axis_size("aper")
    total_subs = slot_count * aper_count
    aper_pos = lax.axis_index("aper")
    full_range = cell_count * lax.axis_size("rng")
    range_ramp = (
        lax.axis_index("rng") * cell_count + jnp.arange(cell_count, dtype=jnp.int32)
    ).astype(jnp.float32) / full_range - 0.5
    tables = (beam_offsets, range_offsets, beam_taps, range_frac, phase_base, phase_rate)
    sub_ids = aper_pos * slot_count + jnp.arange(slot_count, dtype=jnp.int32)
    current = subimages
    for level_idx in range(LEVELS):
        distance = total_subs >> LEVELS - level_idx
        halves = sub_ids // distance % 2
        if distance >= slot_count:
            which_bit = (distance // slot_count).bit_length() - 1
            partner = partner_2(current, "aper", which_bit)
            joined = block_edges(jnp.concatenate([current, partner], 0))
            own_block = joined[:slot_count]
            other_block = joined[slot_count:]
        else:
            own_block = block_edges(current)
            block_shape = own_block.shape
            paired = own_block.reshape(
                (slot_count // (2 * distance), 2, distance) + block_shape[1:]
            )
            other_block = paired[:, ::-1].reshape(block_shape)
        current = merge_level((own_block, other_block), halves, level_idx, tables, range_ramp)
    scale = 1.0 / math.sqrt(total_subs)
    sector = beam_count // aper_count
    regrouped = lax.all_to_all(current[:, None], "aper", split_axis=3, concat_axis=1, tiled=True)
    angles = lax.dynamic_slice_in_dim(final_phase, aper_pos * sector, sector, 1)
    angles = angles.reshape(aper_count, slot_count, sector).transpose(1, 0, 2)
    cosine = jnp.cos(angles)[:, :, :, None]
    sine_part = jnp.sin(angles)[:, :, :, None]
    real_part = regrouped[:, :, 0].astype(jnp.float32)
    imag_part = regrouped[:, :, 1].astype(jnp.float32)
    summed = jnp.stack(
        [
            jnp.sum(cosine * real_part - sine_part * imag_part, axis=(0, 1)),
            jnp.sum(sine_part * real_part + cosine * imag_part, axis=(0, 1)),
        ]
    )
    image = summed * scale
    return image[:, None]


F32 = jnp.float32
BF16 = jnp.bfloat16
LANES = 128
EDGE = -(-HALO * LEVELS // 16) * 16
SEG = 4 * EDGE
FIELDS = 3 + TAPS
VMEM_LIMIT = 24 * 1024 * 1024


def tables_of(slots):
    row = {}
    for lv in range(LEVELS - 1):
        for c in range(2):
            for h in range(2):
                for k in range(FIELDS):
                    row["p", lv, c, h, k] = len(row)
    for s in range(slots):
        for lv in range(LEVELS - 1):
            for c in range(2):
                row["b", s, lv, c] = len(row)
    for lv in range(LEVELS - 1):
        for c in range(2):
            row["r", lv, c] = len(row)
    return row, -(-len(row) // 8) * 8


def half_of(lv, s, total):
    return s // (total >> LEVELS - lv) % 2


def child_of(lv, s, c, total):
    d = total >> LEVELS - lv
    return s - half_of(lv, s, total) * d + c * d


def roll_lanes(x, shift):
    return pltpu.roll(x, shift % LANES, x.ndim - 1) if shift % LANES else x


def iota(shape, dim):
    return lax.broadcasted_iota(jnp.int32, shape, dim)


def pack_kernel(slots, head, tail, bo, ro, bt, rf, pb, pr, out_a, out_b, p_ref, base_ref):
    row, rows = tables_of(slots)
    p_ref[...] = jnp.zeros_like(p_ref)
    for lv in range(LEVELS - 1):
        for c in range(2):
            for h in range(2):
                at = row["p", lv, c, h, 0]
                p_ref[at : at + 1] = bo[lv, c, h : h + 1, :].astype(F32)
                p_ref[at + 1 : at + 2] = (ro[lv, c, h : h + 1, :] + HALO).astype(F32)
                p_ref[at + 2 : at + 3] = rf[lv, c, h : h + 1, :]
                p_ref[at + 3 : at + 3 + TAPS] = bt[lv, c, h].astype(F32)
            at = row["r", lv, c]
            p_ref[at : at + 1] = pr[lv, c : c + 1, :]
            for s in range(slots):
                at = row["b", s, lv, c]
                p_ref[at : at + 1] = pb[s, lv, c : c + 1, :]
    for c in range(2):
        for s in range(slots):
            base_ref[c * slots + s : c * slots + s + 1] = pb[s, LEVELS - 1, c : c + 1, :]

    per = LANES // EDGE
    beams = p_ref.shape[1]
    lane = iota((8, LANES), 1) // EDGE

    def packed(tile, start):
        parts = []
        for first in range(0, rows // 8, per):
            total = jnp.zeros((8, LANES), F32)
            for g in range(first, min(first + per, rows // 8)):
                piece = p_ref[8 * g : 8 * g + 8, tile : tile + LANES]
                spot = (g - first) * EDGE
                total = jnp.where(lane == g - first, roll_lanes(piece, spot - start), total)
            parts.append(total)
        x = jnp.concatenate(parts, 0)
        high = x.astype(BF16)
        return high, (x - high.astype(F32)).astype(BF16)

    def fill(out, sub, tile, start):
        n = slots * 2 * EDGE
        out[:n] = sub[...].reshape(n, LANES)
        high, low = packed(tile, start)
        m = high.shape[0]
        out[n : n + m] = high
        out[n + m : n + 2 * m] = low

    even = lax.axis_index("ang") % 2 == 0

    @pl.when(even)
    def _():
        fill(out_a, tail, beams - LANES, LANES - EDGE)
        fill(out_b, head, 0, 0)

    @pl.when(jnp.logical_not(even))
    def _():
        fill(out_a, head, 0, 0)
        fill(out_b, tail, beams - LANES, LANES - EDGE)


def turned(x):
    return x.astype(F32).T.astype(BF16)


def band(lag, taps):
    out = jnp.zeros(lag.shape, F32)
    for t in range(TAPS):
        out = jnp.where(lag == t, taps[t], out)
    return out.astype(BF16)


def phasors(rate, first, delta, count, low, high, store):
    n = rate.shape[1]
    r8 = iota((8, n), 0)
    small = rate * (r8.astype(F32) * delta)
    other = jnp.where(r8 == 0, rate * (8 * delta), rate * first)
    cs, ss = jnp.cos(small), jnp.sin(small)
    co, so = jnp.cos(other), jnp.sin(other)
    cu, su = co[1:2], so[1:2]
    ck, sk = jnp.broadcast_to(co[0:1], (8, n)), jnp.broadcast_to(so[0:1], (8, n))
    re = cs * cu - ss * su
    im = ss * cu + cs * su
    for j in range(count):
        ids = r8 + 8 * j
        keep = jnp.logical_and(ids >= low, ids < high)
        store(j, jnp.where(keep, re, 0.0), jnp.where(keep, im, 0.0))
        if j + 1 < count:
            re, im = re * ck - im * sk, im * ck + re * sk


def range_place(cells, lv, full):
    reach = (LEVELS - 1 - lv) * HALO
    lead = (EDGE - HALO * (lv + 1)) if lv < LEVELS - 1 else 0
    at = lax.axis_index("rng") * cells - lead
    first = at.astype(F32) / full - 0.5
    return first, -at, full - at


def rows_of(cells, lv):
    need = cells + 2 * (EDGE - HALO * (lv + 1))
    return -(-need // 16) * 16


def main_tables_kernel(slots, full, sub, p_ref, bo, ro, bt, rf, pr, xt, w1, w2, v1, v2, o2, e_refs, th):
    row, rows = tables_of(slots)
    total = 2 * slots
    cells = sub.shape[3]
    beams = sub.shape[2]
    tiles = beams // LANES
    for s in range(slots):
        for x in range(2):
            xt[x, :, s * beams : (s + 1) * beams] = turned(sub[s, x])

    w1[...] = jnp.zeros_like(w1)
    w2[...] = jnp.zeros_like(w2)
    v1[...] = jnp.zeros_like(v1)
    v2[...] = jnp.zeros_like(v2)
    own = lax.axis_index("aper")

    def main_band(first_col, off, taps, put):
        low = max(first_col - 16, 0)
        top = min(first_col + LANES + 16, beams)
        m = iota((top - low, LANES), 0) + low
        p = iota((top - low, LANES), 1) + first_col
        put(low, top, band(m - p - off, taps))

    def strip_band(first_col, off, taps, put):
        if first_col + LANES == beams:
            m = iota((EDGE, LANES), 0) + beams
            put(EDGE, band(m - (iota((EDGE, LANES), 1) + first_col) - off, taps))
        if first_col == 0:
            m = iota((EDGE, LANES), 0) - EDGE
            put(2 * EDGE, band(m - iota((EDGE, LANES), 1) - off, taps))

    for lv in range(LEVELS - 1):
        for c in range(2):
            for h in range(2):
                for t in range(tiles):
                    cols = slice(t * LANES, (t + 1) * LANES)
                    at = row["p", lv, c, h, 0]
                    off = p_ref[at : at + 1, cols].astype(jnp.int32)
                    taps = [p_ref[at + 3 + k : at + 4 + k, cols] for k in range(TAPS)]

                    def put(low, top, v):
                        w1[lv, c, h, low:top, cols] = v

                    main_band(t * LANES, off, taps, put)

                    def put(at_row, v):
                        for s in range(slots):
                            if half_of(lv, s, total) == h:
                                base = child_of(lv, s, c, total) * SEG % LANES + at_row
                                w2[lv, c, s, base : base + EDGE, cols] = v

                    strip_band(t * LANES, off, taps, put)
    lv = LEVELS - 1
    for h in range(2):
        for t in range(tiles):
            cols = slice(t * LANES, (t + 1) * LANES)
            outs = slice(h * LANES, (h + 1) * LANES)
            off = bo[lv, own, h : h + 1, cols]
            tap_rows = bt[lv, own, h, :, cols].astype(F32)
            taps = [tap_rows[k : k + 1] for k in range(TAPS)]

            def put(low, top, v):
                v1[t, low:top, outs] = v

            main_band(t * LANES, off, taps, put)

            def put(at_row, v):
                for par in range(LANES // SEG):
                    base = par * SEG + at_row
                    v2[t, par, base : base + EDGE, outs] = v

            strip_band(t * LANES, off, taps, put)
            o2[t, 0:1, outs] = (ro[lv, own, h : h + 1, cols] + HALO).astype(F32)
            o2[t, 1:2, outs] = rf[lv, own, h : h + 1, cols]

    for lv in range(LEVELS):
        first, low, high = range_place(cells, lv, full)
        count = (rows_of(cells, lv) if lv < LEVELS - 1 else cells) // 8
        for c in range(2 if lv < LEVELS - 1 else 1):
            if lv < LEVELS - 1:
                at = row["r", lv, c]
                rate = p_ref[at : at + 1, :]
            else:
                rate = jnp.where(own == 0, pr[lv, 0:1, :], pr[lv, 1:2, :])

            def store(j, re, im):
                e_refs[lv][c, 0, 8 * j : 8 * j + 8, :] = re
                e_refs[lv][c, 1, 8 * j : 8 * j + 8, :] = im

            phasors(rate, first, 1.0 / full, count, low, high, store)
    at = row["b", 0, 0, 0]
    n = slots * (LEVELS - 1) * 2
    base = p_ref[at : at + n, :]
    th[0] = jnp.cos(base)
    th[1] = jnp.sin(base)


def strip_kernel(slots, got_a, got_b, head, tail, xt, strip, out_c, out_d, nat):
    beams = slots * SEG
    even = lax.axis_index("ang") % 2 == 0

    def place(right, left):
        for s in range(slots):
            for x in range(2):
                at = (s * 2 + x) * EDGE
                nat[x, s * SEG + EDGE : s * SEG + 2 * EDGE] = right[at : at + EDGE]
                nat[x, s * SEG + 2 * EDGE : s * SEG + 3 * EDGE] = left[at : at + EDGE]

    for s in range(slots):
        for x in range(2):
            nat[x, s * SEG : s * SEG + EDGE] = tail[s, x]
            nat[x, s * SEG + 3 * EDGE : (s + 1) * SEG] = head[s, x]

    @pl.when(even)
    def _():
        place(got_a, got_b)

    @pl.when(jnp.logical_not(even))
    def _():
        place(got_b, got_a)

    for x in range(2):
        strip[x] = turned(nat[x])
    cells = strip.shape[1]
    mains = xt.shape[2]

    def send(first, last):
        for x in range(2):
            first[x, :, :mains] = xt[x, cells - EDGE :, :]
            first[x, :, mains:] = strip[x, cells - EDGE :, :]
            last[x, :, :mains] = xt[x, :EDGE, :]
            last[x, :, mains:] = strip[x, :EDGE, :]

    even_r = lax.axis_index("rng") % 2 == 0

    @pl.when(even_r)
    def _():
        send(out_c, out_d)

    @pl.when(jnp.logical_not(even_r))
    def _():
        send(out_d, out_c)


def strip_tables_kernel(slots, full, got_a, got_b, p_ref, base_ref, got_base, fp, ws, es_refs, ths, os_, th2, seg, halo):
    row, rows = tables_of(slots)
    total = 2 * slots
    cells = LANES
    beams = p_ref.shape[1]
    per = LANES // EDGE
    n = slots * 2 * EDGE
    m = (rows // 8 + per - 1) // per * 8
    even = lax.axis_index("ang") % 2 == 0

    def load(right, left):
        halo[0] = right[n : n + m].astype(F32) + right[n + m : n + 2 * m].astype(F32)
        halo[1] = left[n : n + m].astype(F32) + left[n + m : n + 2 * m].astype(F32)

    @pl.when(even)
    def _():
        load(got_a, got_b)

    @pl.when(jnp.logical_not(even))
    def _():
        load(got_b, got_a)

    lane = iota((8, LANES), 1)
    piece_of = lane % SEG // EDGE
    for g in range(rows // 8):
        at = g // per * 8
        spot = g % per * EDGE
        parts = [
            roll_lanes(p_ref[8 * g : 8 * g + 8, beams - LANES :], EDGE - LANES),
            roll_lanes(halo[0, at : at + 8, :], EDGE - spot),
            roll_lanes(halo[1, at : at + 8, :], 2 * EDGE - spot),
            roll_lanes(p_ref[8 * g : 8 * g + 8, :LANES], 3 * EDGE),
        ]
        out = parts[0]
        for k in range(1, 4):
            out = jnp.where(piece_of == k, parts[k], out)
        twice = jnp.where(lane < SEG, out, roll_lanes(out, SEG))
        seg[8 * g : 8 * g + 8, :] = twice

    first_seg = iota((1, LANES), 1) < SEG

    def pick(r0, r1):
        if r0 == r1:
            return seg[r0 : r0 + 1, :]
        return jnp.where(first_seg, seg[r0 : r0 + 1, :], seg[r1 : r1 + 1, :])

    def beam_of(i):
        j = i % SEG
        return jnp.where(j < 2 * EDGE, beams - EDGE + j, j - 3 * EDGE)

    base_rows = []
    for lv in range(LEVELS - 1):
        first, low, high = range_place(cells, lv, full)
        for c in range(2):
            for t in range(beams // LANES):
                cols = slice(t * LANES, (t + 1) * LANES)
                s0, s1 = 2 * t, 2 * t + 1
                h0, h1 = half_of(lv, s0, total), half_of(lv, s1, total)
                k0, k1 = child_of(lv, s0, c, total), child_of(lv, s1, c, total)
                field = [pick(row["p", lv, c, h0, k], row["p", lv, c, h1, k]) for k in range(FIELDS)]
                at = lv * 2 + c
                os_[at, 0:1, cols] = field[1]
                os_[at, 1:2, cols] = field[2]
                i_row = iota((beams, LANES), 0)
                col = iota((1, LANES), 1)
                wanted = jnp.where(col < SEG, k0, k1)
                lag = beam_of(i_row) - beam_of(col) - field[0].astype(jnp.int32)
                lag = jnp.where(i_row // SEG == wanted, lag, -1)
                ws[lv, c, :, cols] = band(lag, field[3:])
                halo[2, at * 2 + t : at * 2 + t + 1, :] = pick(row["b", s0, lv, c], row["b", s1, lv, c])
            rate = jnp.concatenate([pick(row["r", lv, c], row["r", lv, c])] * (beams // LANES), 1)

            def store(j, re, im):
                es_refs[lv][c, 0, 8 * j : 8 * j + 8, :] = re
                es_refs[lv][c, 1, 8 * j : 8 * j + 8, :] = im

            phasors(rate[:, :LANES], first, 1.0 / full, rows_of(cells, lv) // 8, low, high, store)
    angles = halo[2, : 2 * 2 * (LEVELS - 1)]
    ths[0] = jnp.cos(angles)
    ths[1] = jnp.sin(angles)

    own = lax.axis_index("aper")
    scale = 1.0 / math.sqrt(total)
    for h in range(2):
        mine = own == h
        for t in range(beams // LANES):
            cols = slice(t * LANES, (t + 1) * LANES)
            here = jnp.where(own == 0, base_ref[:slots, cols], base_ref[slots:, cols])
            there = jnp.where(own == 0, got_base[:slots, cols], got_base[slots:, cols])
            angles = jnp.where(mine, here, there) + fp[h * slots : (h + 1) * slots, cols]
            th2[0, t, :, h * LANES : (h + 1) * LANES] = jnp.cos(angles) * scale
            th2[1, t, :, h * LANES : (h + 1) * LANES] = jnp.sin(angles) * scale


def shift_setup(o_row, f_row, extra):
    shift = o_row.astype(jnp.int32) + extra
    sub = iota((8, LANES), 0)
    reach = sub + shift
    return dict(
        one=jnp.broadcast_to(1.0 - f_row, (8, LANES)),
        two=jnp.broadcast_to(f_row, (8, LANES)),
        bits=[jnp.broadcast_to(shift % (2 * b) >= b, (8, LANES)) for b in (1, 2, 4)],
        in0=reach < 8,
        in1=reach < 16,
        last=sub == 7,
    )


def rotated(setup, v):
    n = v.shape[0] - 1
    spun = pltpu.roll(v, 7, 1)
    ahead = jnp.where(setup["last"][None], spun[1:], spun[:n])
    g = setup["one"][None] * v[:n] + setup["two"][None] * ahead
    for b, bit in zip((1, 2, 4), setup["bits"]):
        g = jnp.where(bit[None], pltpu.roll(g, 8 - b, 1), g)
    return g


def level_step(slots, total, lv, x_in, out, inter, w1, w2, ws, e_main, e_strip, th, ths, o_main, os_, row):
    rows_in = x_in.shape[1]
    beams = slots * SEG
    rows_out = out.shape[1]
    groups = slots + 1
    for g in range(groups):
        buf = inter[g % 2]
        for c in range(2):
            if g < slots:
                k = child_of(lv, g, c, total)
                h = half_of(lv, g, total)
                lhs = x_in[:, :, k * beams : (k + 1) * beams].reshape(2 * rows_in, beams)
                tile = slots * beams + k * SEG // LANES * LANES
                lhs2 = x_in[:, :, tile : tile + LANES].reshape(2 * rows_in, LANES)
                val = jnp.dot(lhs, w1[lv, c, h], preferred_element_type=F32) + jnp.dot(
                    lhs2, w2[lv, c, g], preferred_element_type=F32
                )
            else:
                lhs = x_in[:, :, slots * beams :].reshape(2 * rows_in, beams)
                val = jnp.dot(lhs, ws[lv, c], preferred_element_type=F32)
            for x in range(2):
                for t in range(beams // LANES):
                    buf[c, x, t, :rows_in, :] = val[x * rows_in : (x + 1) * rows_in, t * LANES : (t + 1) * LANES]
        for t in range(beams // LANES):
            cols = slice(t * LANES, (t + 1) * LANES)
            sets, turn = [], []
            for c in range(2):
                if g < slots:
                    at = row["p", lv, c, half_of(lv, g, total), 0]
                    sets.append(shift_setup(o_main[at + 1 : at + 2, cols], o_main[at + 2 : at + 3, cols], 0))
                    at = (g * (LEVELS - 1) + lv) * 2 + c
                    turn.append([jnp.broadcast_to(th[q, at : at + 1, cols], (8, LANES))[None] for q in range(2)])
                else:
                    at = lv * 2 + c
                    sets.append(shift_setup(os_[at, 0:1, cols], os_[at, 1:2, cols], 0))
                    turn.append([jnp.broadcast_to(ths[q, at * 2 + t : at * 2 + t + 1, :], (8, LANES))[None] for q in range(2)])
            held = [[None, None], [None, None]]
            step = 4
            done = 0
            n_out = rows_out // 8
            while done < n_out:
                n = min(step, n_out - done)
                acc_re = acc_im = None
                for c in range(2):
                    moved = []
                    for x in range(2):
                        lo = 0 if done == 0 else done + 1
                        hi = done + n + 2
                        v = buf[c, x, t, 8 * lo : 8 * hi, :].reshape(hi - lo, 8, LANES)
                        g_new = rotated(sets[c], v)
                        if done == 0:
                            seq = g_new
                        else:
                            seq = jnp.concatenate([held[c][x], g_new], 0)
                        held[c][x] = seq[n : n + 1]
                        moved.append(jnp.where(sets[c]["in0"][None], seq[:n], seq[1 : n + 1]))
                    e = e_main if g < slots else e_strip
                    ecols = cols if g < slots else slice(0, LANES)
                    ec = e[c, 0, 8 * done : 8 * (done + n), ecols].reshape(n, 8, LANES)
                    es = e[c, 1, 8 * done : 8 * (done + n), ecols].reshape(n, 8, LANES)
                    tc, ts = turn[c]
                    fc, fs = ec * tc - es * ts, es * tc + ec * ts
                    re = fc * moved[0] - fs * moved[1]
                    im = fs * moved[0] + fc * moved[1]
                    acc_re = re if acc_re is None else acc_re + re
                    acc_im = im if acc_im is None else acc_im + im
                ocols = slice(g * beams + t * LANES, g * beams + (t + 1) * LANES)
                out[0, 8 * done : 8 * (done + n), ocols] = acc_re.reshape(8 * n, LANES).astype(BF16)
                out[1, 8 * done : 8 * (done + n), ocols] = acc_im.reshape(8 * n, LANES).astype(BF16)
                done += n


def last_step(slots, cells, hf, x_in, v1, v2, o2, th2, e2, buf, put):
    rows_in = x_in.shape[1]
    beams = slots * SEG
    for q in range(slots):
        lhs = x_in[:, :, q * beams : (q + 1) * beams].reshape(2 * rows_in, beams)
        tile = slots * beams + q * SEG // LANES * LANES
        lhs2 = x_in[:, :, tile : tile + LANES].reshape(2 * rows_in, LANES)
        val = jnp.dot(lhs, v1[hf], preferred_element_type=F32) + jnp.dot(
            lhs2, v2[hf, q * SEG % LANES // SEG], preferred_element_type=F32
        )
        for x in range(2):
            for h in range(2):
                buf[q, x, h] = val[x * rows_in : (x + 1) * rows_in, h * LANES : (h + 1) * LANES]
    sets, turn = [], []
    rows2 = o2[hf]
    for h in range(2):
        cols = slice(h * LANES, (h + 1) * LANES)
        sets.append(shift_setup(rows2[0:1, cols], rows2[1:2, cols], HALO))
        cos_rows = th2[0, hf]
        sin_rows = th2[1, hf]
        turn.append(
            [
                [jnp.broadcast_to(cos_rows[q : q + 1, cols], (8, LANES))[None] for q in range(slots)],
                [jnp.broadcast_to(sin_rows[q : q + 1, cols], (8, LANES))[None] for q in range(slots)],
            ]
        )
    n_out = cells // 8
    held = [[None, None], [None, None]]
    done = 0
    step = 4
    while done < n_out:
        n = min(step, n_out - done)
        sum_re = sum_im = None
        for h in range(2):
            lo = 0 if done == 0 else done + 2
            hi = min(done + n + 3, rows_in // 8)
            re = im = None
            for q in range(slots):
                a = buf[q, 0, h, 8 * lo : 8 * hi, :].reshape(hi - lo, 8, LANES)
                b = buf[q, 1, h, 8 * lo : 8 * hi, :].reshape(hi - lo, 8, LANES)
                tc, ts = turn[h][0][q], turn[h][1][q]
                pr_, pi_ = tc * a - ts * b, ts * a + tc * b
                re = pr_ if re is None else re + pr_
                im = pi_ if im is None else im + pi_
            moved = []
            for x, v in enumerate((re, im)):
                if hi - lo < n + (3 if done == 0 else 1):
                    v = jnp.concatenate([v, jnp.zeros((1, 8, LANES), F32)], 0)
                g_new = rotated(sets[h], v)
                seq = g_new if done == 0 else jnp.concatenate([held[h][x], g_new], 0)
                held[h][x] = seq[n : n + 2]
                moved.append(
                    jnp.where(
                        sets[h]["in0"][None],
                        seq[:n],
                        jnp.where(sets[h]["in1"][None], seq[1 : n + 1], seq[2 : n + 2]),
                    )
                )
            sum_re = moved[0] if sum_re is None else sum_re + moved[0]
            sum_im = moved[1] if sum_im is None else sum_im + moved[1]
        at = pl.ds(pl.multiple_of(hf * LANES, LANES), LANES)
        ec = e2[0, 0, 8 * done : 8 * (done + n), at].reshape(n, 8, LANES)
        es = e2[0, 1, 8 * done : 8 * (done + n), at].reshape(n, 8, LANES)
        put(done, n, ec * sum_re - es * sum_im, es * sum_re + ec * sum_im)
        done += n


def levels_kernel(slots, full, xt, strip, got_c, got_d, w1, w2, ws, v1, v2, o2, e0, e1, e2, es0, es1, th, ths, os_, th2, p_ref, out, x2, x0, x1, inter0, inter1, buf, flat):
    row, rows = tables_of(slots)
    total = 2 * slots
    cells = xt.shape[1]
    mains = xt.shape[2]
    for x in range(2):
        x0[x, EDGE : EDGE + cells, :mains] = xt[x]
        x0[x, EDGE : EDGE + cells, mains:] = strip[x]
    even = lax.axis_index("rng") % 2 == 0

    def place(right, left):
        for x in range(2):
            x0[x, :EDGE, :] = left[x]
            x0[x, EDGE + cells :, :] = right[x]

    @pl.when(even)
    def _():
        place(got_c, got_d)

    @pl.when(jnp.logical_not(even))
    def _():
        place(got_d, got_c)

    inter = (inter0, inter1)
    level_step(slots, total, 0, x0, x1, inter, w1, w2, ws, e0, es0, th, ths, p_ref, os_, row)
    level_step(slots, total, 1, x1, x2, inter, w1, w2, ws, e1, es1, th, ths, p_ref, os_, row)
    hf = 1 - lax.axis_index("aper")

    def put(done, n, re, im):
        flat[0, 8 * done : 8 * (done + n), :] = re.reshape(8 * n, LANES)
        flat[1, 8 * done : 8 * (done + n), :] = im.reshape(8 * n, LANES)

    last_step(slots, cells, hf, x2, v1, v2, o2, th2, e2, buf, put)
    for x in range(2):
        out[x] = flat[x].T.astype(BF16)


def own_half_kernel(slots, x2, v1, v2, o2, th2, e2, out, buf, flat):
    cells = out.shape[2]
    hf = lax.axis_index("aper")

    def put(done, n, re, im):
        flat[0, 8 * done : 8 * (done + n), :] = re.reshape(8 * n, LANES)
        flat[1, 8 * done : 8 * (done + n), :] = im.reshape(8 * n, LANES)

    last_step(slots, cells, hf, x2, v1, v2, o2, th2, e2, buf, put)
    for x in range(2):
        out[x] = flat[x].T


def swap_even(axis):
    n = lax.axis_size(axis)
    return [(i, i ^ 1) for i in range(n) if i ^ 1 < n]


def swap_odd(axis):
    n = lax.axis_size(axis)
    pairs = []
    for i in range(1, n - 1, 2):
        pairs += [(i, i + 1), (i + 1, i)]
    return pairs


def call(kernel, outs, args, scratch=(), flops=0, specs=None):
    vm = pl.BlockSpec(memory_space=pltpu.VMEM)
    return pl.pallas_call(
        kernel,
        out_shape=[jax.ShapeDtypeStruct(s, d) for s, d in outs],
        in_specs=specs or [vm] * len(args),
        out_specs=[vm] * len(outs),
        scratch_shapes=[pltpu.VMEM(s, d) for s, d in scratch],
        compiler_params=pltpu.CompilerParams(vmem_limit_bytes=VMEM_LIMIT),
        cost_estimate=pl.CostEstimate(flops=flops, bytes_accessed=0, transcendentals=0),
    )(*args)


def fast_body(subimages, beam_offsets, range_offsets, beam_taps, range_frac, phase_base, phase_rate, final_phase):
    slots, _, beams, cells = subimages.shape
    full = cells * lax.axis_size("rng")
    row, rows = tables_of(slots)
    m = (rows // 8 + LANES // EDGE - 1) // (LANES // EDGE) * 8
    msg = slots * 2 * EDGE + 2 * m
    head = subimages[:, :, :EDGE]
    tail = subimages[:, :, beams - EDGE :]
    vm = pl.BlockSpec(memory_space=pltpu.VMEM)
    lv_rows = [rows_of(cells, lv) for lv in range(LEVELS - 1)]

    out_a, out_b, params, bases = call(
        functools.partial(pack_kernel, slots),
        [((msg, LANES), BF16), ((msg, LANES), BF16), ((rows, beams), F32), ((2 * slots, beams), F32)],
        (head, tail, beam_offsets, range_offsets, beam_taps, range_frac, phase_base, phase_rate),
        flops=1000,
    )
    got_a = lax.ppermute(out_a, "ang", swap_even("ang"))
    got_b = lax.ppermute(out_b, "ang", swap_odd("ang"))
    got_base = lax.ppermute(bases, "aper", swap_even("aper"))

    def main_tables(*refs):
        ins, outs = refs[:7], refs[7:]
        main_tables_kernel(slots, full, *ins, *outs[:6], outs[6 : 6 + LEVELS], outs[6 + LEVELS])

    n_th = slots * (LEVELS - 1) * 2
    tiles = beams // LANES
    res = call(
        main_tables,
        [
            ((2, cells, slots * beams), BF16),
            ((LEVELS - 1, 2, 2, beams, beams), BF16),
            ((LEVELS - 1, 2, slots, LANES, beams), BF16),
            ((tiles, beams, beams), BF16),
            ((tiles, LANES // SEG, LANES, beams), BF16),
            ((tiles, 8, beams), F32),
        ]
        + [((2, 2, r, beams), F32) for r in lv_rows]
        + [((1, 2, cells, beams), F32), ((2, n_th, beams), F32)],
        (subimages, params, beam_offsets, range_offsets, beam_taps, range_frac, phase_rate),
        flops=20_000_000,
    )
    xt, w1, w2, v1, v2, o2, e0, e1, e2, th = res

    strip, out_c, out_d = call(
        functools.partial(strip_kernel, slots),
        [((2, cells, beams), BF16)] + [((2, EDGE, (slots + 1) * beams), BF16)] * 2,
        (got_a, got_b, head, tail, xt),
        scratch=[((2, beams, cells), BF16)],
        flops=1000,
    )
    got_c = lax.ppermute(out_c, "rng", swap_even("rng"))
    got_d = lax.ppermute(out_d, "rng", swap_odd("rng"))

    def strip_tables(*refs):
        ins, outs = refs[:6], refs[6:]
        strip_tables_kernel(slots, full, *ins, outs[0], outs[1:LEVELS], *outs[LEVELS:])

    ws, es0, es1, ths, os_, th2 = call(
        strip_tables,
        [((LEVELS - 1, 2, beams, beams), BF16)]
        + [((2, 2, r, LANES), F32) for r in lv_rows]
        + [((2, 4 * (LEVELS - 1), LANES), F32), ((2 * (LEVELS - 1), 8, beams), F32), ((2, tiles, slots, beams), F32)],
        (got_a, got_b, params, bases, got_base, final_phase),
        scratch=[((rows, LANES), F32), ((3, max(m, 8), LANES), F32)],
        flops=20_000_000,
    )
    wide = (slots + 1) * beams
    x_rows = cells + 2 * EDGE
    sent, x2 = call(
        functools.partial(levels_kernel, slots, full),
        [((2, LANES, cells), BF16), ((2, lv_rows[1], wide), BF16)],
        (xt, strip, got_c, got_d, w1, w2, ws, v1, v2, o2, e0, e1, e2, es0, es1, th, ths, os_, th2, params),
        scratch=[
            ((2, x_rows, wide), BF16),
            ((2, lv_rows[0], wide), BF16),
            ((2, 2, tiles, x_rows + 16, LANES), F32),
            ((2, 2, tiles, x_rows + 16, LANES), F32),
            ((slots, 2, 2, lv_rows[1], LANES), F32),
            ((2, cells, LANES), F32),
        ],
        flops=200_000_000,
    )
    got = lax.ppermute(sent, "aper", swap_even("aper"))
    (mine,) = call(
        functools.partial(own_half_kernel, slots),
        [((2, LANES, cells), F32)],
        (x2, v1, v2, o2, th2, e2),
        scratch=[((slots, 2, 2, lv_rows[1], LANES), F32), ((2, cells, LANES), F32)],
        flops=20_000_000,
    )
    return (mine + got.astype(F32))[:, None]


def whole_body(*args):
    slots, _, beams, cells = args[0].shape
    fits = (
        lax.axis_size("aper") == 2
        and slots * SEG == beams
        and beams == 2 * LANES
        and cells == LANES
        and slots == 1 << LEVELS - 1
    )
    return fast_body(*args) if fits else body(*args)


def solution(mesh):
    in_specs = (
        P("aper", None, "ang", "rng"),
        P(None, None, None, "ang"),
        P(None, None, None, "ang"),
        P(None, None, None, None, "ang"),
        P(None, None, None, "ang"),
        P("aper", None, None, "ang"),
        P(None, None, "ang"),
        P(None, "ang"),
    )
    out_specs = P(None, "ang", "aper", "rng")
    return jax.shard_map(whole_body, mesh=mesh, in_specs=in_specs, out_specs=out_specs, check_vma=False)
```

```python
import functools
import math

import jax
import jax.numpy as jnp
from jax import lax
from jax.experimental import pallas as pl
from jax.experimental.pallas import tpu as pltpu
from jax.sharding import PartitionSpec as P

LEVELS = 3
TAPS = 4
HALO = 4


def with_halo(cells, sides, width):
    for axis, dim in sides:
        count = lax.axis_size(axis)
        ends = count - 1
        head = lax.slice_in_dim(cells, 0, width, axis=dim)
        tail = lax.slice_in_dim(cells, cells.shape[dim] - width, cells.shape[dim], axis=dim)
        cells = jnp.concatenate(
            [
                lax.ppermute(tail, axis, [(i, (i + 1) % count) for i in range(ends)]),
                cells,
                lax.ppermute(head, axis, [((i + 1) % count, i) for i in range(ends)]),
            ],
            axis=dim,
        )
    return cells


def partner_2(x, axis, stride):
    return lax.ppermute(x, axis, [(i, i ^ 1 << stride) for i in range(lax.axis_size(axis))])


def block_edges(blocks):
    return with_halo(blocks, (("ang", 2), ("rng", 3)), HALO)


def band_matrices(offsets, tap_weights):
    beam_count = offsets.shape[1]
    columns = jnp.arange(beam_count + 2 * HALO, dtype=jnp.int32)
    row_ids = jnp.arange(beam_count, dtype=jnp.int32)
    starting = row_ids[None, :] + HALO + offsets
    lagging = columns[None, None, :] - starting[:, :, None]
    weights = jnp.zeros(lagging.shape, jnp.float32)
    for tap_idx in range(TAPS):
        weights = weights + jnp.where(
            lagging == tap_idx, tap_weights[:, tap_idx, :, None].astype(jnp.float32), 0.0
        )
    return weights.astype(jnp.bfloat16)


def merge_level(child_blocks, halves, level_idx, tables, range_ramp):
    beam_offsets, range_offsets, beam_taps, range_frac, phase_base, phase_rate = tables
    slot_count = halves.shape[0]
    cell_count = range_ramp.shape[0]
    slot_ids = jnp.arange(slot_count, dtype=jnp.int32)
    summed = None
    for side_idx in range(2):
        child_ids = halves if side_idx == 0 else 1 - halves
        extended = child_blocks[side_idx]
        matrices = band_matrices(
            beam_offsets[level_idx][child_ids, halves], beam_taps[level_idx][child_ids, halves]
        )
        interpolated = jnp.einsum(
            "snm,sxmr->sxnr", matrices, extended, preferred_element_type=jnp.float32
        )
        range_shift = range_offsets[level_idx][child_ids, halves] + HALO
        fraction = range_frac[level_idx][child_ids, halves]
        shifted = jnp.zeros(interpolated.shape[:3] + (cell_count,), jnp.float32)
        for offset_step in range(2 * HALO + 1):
            weight = jnp.where(range_shift == offset_step, 1.0 - fraction, 0.0) + jnp.where(
                range_shift + 1 == offset_step, fraction, 0.0
            )
            shifted = (
                shifted
                + weight[:, None, :, None]
                * interpolated[:, :, :, offset_step : offset_step + cell_count]
            )
        angles = (
            phase_base[slot_ids, level_idx, child_ids][:, :, None]
            + phase_rate[level_idx][child_ids][:, :, None] * range_ramp[None, None, :]
        )
        cosine = jnp.cos(angles)
        sine_part = jnp.sin(angles)
        term = jnp.stack(
            [
                cosine * shifted[:, 0] - sine_part * shifted[:, 1],
                sine_part * shifted[:, 0] + cosine * shifted[:, 1],
            ],
            axis=1,
        )
        summed = term if summed is None else summed + term
    return summed.astype(jnp.bfloat16)


def body(
    subimages,
    beam_offsets,
    range_offsets,
    beam_taps,
    range_frac,
    phase_base,
    phase_rate,
    final_phase,
):
    slot_count = subimages.shape[0]
    beam_count = subimages.shape[2]
    cell_count = subimages.shape[3]
    aper_count = lax.axis_size("aper")
    total_subs = slot_count * aper_count
    aper_pos = lax.axis_index("aper")
    full_range = cell_count * lax.axis_size("rng")
    range_ramp = (
        lax.axis_index("rng") * cell_count + jnp.arange(cell_count, dtype=jnp.int32)
    ).astype(jnp.float32) / full_range - 0.5
    tables = (beam_offsets, range_offsets, beam_taps, range_frac, phase_base, phase_rate)
    sub_ids = aper_pos * slot_count + jnp.arange(slot_count, dtype=jnp.int32)
    current = subimages
    for level_idx in range(LEVELS):
        distance = total_subs >> LEVELS - level_idx
        halves = sub_ids // distance % 2
        if distance >= slot_count:
            which_bit = (distance // slot_count).bit_length() - 1
            partner = partner_2(current, "aper", which_bit)
            joined = block_edges(jnp.concatenate([current, partner], 0))
            own_block = joined[:slot_count]
            other_block = joined[slot_count:]
        else:
            own_block = block_edges(current)
            block_shape = own_block.shape
            paired = own_block.reshape(
                (slot_count // (2 * distance), 2, distance) + block_shape[1:]
            )
            other_block = paired[:, ::-1].reshape(block_shape)
        current = merge_level((own_block, other_block), halves, level_idx, tables, range_ramp)
    scale = 1.0 / math.sqrt(total_subs)
    sector = beam_count // aper_count
    regrouped = lax.all_to_all(current[:, None], "aper", split_axis=3, concat_axis=1, tiled=True)
    angles = lax.dynamic_slice_in_dim(final_phase, aper_pos * sector, sector, 1)
    angles = angles.reshape(aper_count, slot_count, sector).transpose(1, 0, 2)
    cosine = jnp.cos(angles)[:, :, :, None]
    sine_part = jnp.sin(angles)[:, :, :, None]
    real_part = regrouped[:, :, 0].astype(jnp.float32)
    imag_part = regrouped[:, :, 1].astype(jnp.float32)
    summed = jnp.stack(
        [
            jnp.sum(cosine * real_part - sine_part * imag_part, axis=(0, 1)),
            jnp.sum(sine_part * real_part + cosine * imag_part, axis=(0, 1)),
        ]
    )
    image = summed * scale
    return image[:, None]


F32 = jnp.float32
BF16 = jnp.bfloat16
LANES = 128
EDGE = -(-HALO * LEVELS // 16) * 16
SEG = 4 * EDGE
FIELDS = 3 + TAPS
VMEM_LIMIT = 24 * 1024 * 1024
COVER_FLOPS = 400_000_000


def tables_of(slots):
    row = {}
    for lv in range(LEVELS - 1):
        for c in range(2):
            for h in range(2):
                for k in range(FIELDS):
                    row["p", lv, c, h, k] = len(row)
    for s in range(slots):
        for lv in range(LEVELS - 1):
            for c in range(2):
                row["b", s, lv, c] = len(row)
    for lv in range(LEVELS - 1):
        for c in range(2):
            row["r", lv, c] = len(row)
    return row, -(-len(row) // 8) * 8


def half_of(lv, s, total):
    return s // (total >> LEVELS - lv) % 2


def child_of(lv, s, c, total):
    d = total >> LEVELS - lv
    return s - half_of(lv, s, total) * d + c * d


def roll_lanes(x, shift):
    return pltpu.roll(x, shift % LANES, x.ndim - 1) if shift % LANES else x


def iota(shape, dim):
    return lax.broadcasted_iota(jnp.int32, shape, dim)


def blank_kernel(out):
    out[...] = jnp.zeros_like(out)


def pack_kernel(slots, blank, sub, bo, ro, bt, rf, pb, pr, fp, out_a, out_b, p_ref, base_ref):
    row, rows = tables_of(slots)
    beams = p_ref.shape[1]
    for t in range(beams // LANES):
        p_ref[rows - 8 :, t * LANES : (t + 1) * LANES] = blank[...]
    for lv in range(LEVELS - 1):
        for c in range(2):
            for h in range(2):
                at = row["p", lv, c, h, 0]
                p_ref[at : at + 1] = bo[lv, c, h : h + 1, :].astype(F32)
                p_ref[at + 1 : at + 2] = (ro[lv, c, h : h + 1, :] + HALO).astype(F32)
                p_ref[at + 2 : at + 3] = rf[lv, c, h : h + 1, :]
                p_ref[at + 3 : at + 3 + TAPS] = bt[lv, c, h].astype(F32)
            at = row["r", lv, c]
            p_ref[at : at + 1] = pr[lv, c : c + 1, :]
            for s in range(slots):
                at = row["b", s, lv, c]
                p_ref[at : at + 1] = pb[s, lv, c : c + 1, :]
    for c in range(2):
        for s in range(slots):
            base_ref[c * slots + s : c * slots + s + 1] = pb[s, LEVELS - 1, c : c + 1, :]

    per = LANES // EDGE
    beams = p_ref.shape[1]
    lane = iota((8, LANES), 1) // EDGE

    def packed(tile, start):
        parts = []
        for first in range(0, rows // 8, per):
            total = jnp.zeros((8, LANES), F32)
            for g in range(first, min(first + per, rows // 8)):
                piece = p_ref[8 * g : 8 * g + 8, tile : tile + LANES]
                spot = (g - first) * EDGE
                total = jnp.where(lane == g - first, roll_lanes(piece, spot - start), total)
            parts.append(total)
        x = jnp.concatenate(parts, 0)
        high = x.astype(BF16)
        return high, (x - high.astype(F32)).astype(BF16)

    def fill(out, first, tile, start):
        n = slots * 2 * EDGE
        out[:n] = sub[:, :, first : first + EDGE].reshape(n, LANES)
        high, low = packed(tile, start)
        m = high.shape[0]
        out[n : n + m] = high
        out[n + m : n + 2 * m] = low

    even = lax.axis_index("ang") % 2 == 0

    @pl.when(even)
    def _():
        fill(out_a, beams - EDGE, beams - LANES, LANES - EDGE)
        fill(out_b, 0, 0, 0)

    @pl.when(jnp.logical_not(even))
    def _():
        fill(out_a, 0, 0, 0)
        fill(out_b, beams - EDGE, beams - LANES, LANES - EDGE)


def turned(x):
    return x.astype(F32).T.astype(BF16)


def sincos(x):
    k = jnp.floor(x * (2.0 / math.pi) + 0.5)
    r = x - k * 1.5703125
    r = r - k * 4.838267948966e-4
    q = k.astype(jnp.int32)
    z = r * r
    s = r + r * z * (-1.6666654611e-1 + z * (8.3321608736e-3 + z * -1.9515295891e-4))
    c = 1.0 - 0.5 * z + z * z * (4.166664568298827e-2 + z * (-1.388731625493765e-3 + z * 2.443315711809948e-5))
    odd = q % 2 != 0
    sin, cos = jnp.where(odd, c, s), jnp.where(odd, s, c)
    q = q % 4
    return jnp.where(q >= 2, -sin, sin), jnp.where((q == 1) | (q == 2), -cos, cos)


def band(lag, taps):
    out = jnp.zeros(lag.shape, F32)
    for t in range(TAPS):
        out = jnp.where(lag == t, taps[t], out)
    return out.astype(BF16)


def phasors(rate, first, delta, count, low, high, store):
    n = rate.shape[1]
    r8 = iota((8, n), 0)
    small = rate * (r8.astype(F32) * delta)
    other = jnp.where(r8 == 0, rate * (8 * delta), rate * first)
    ss, cs = sincos(small)
    so, co = sincos(other)
    cu, su = co[1:2], so[1:2]
    ck, sk = jnp.broadcast_to(co[0:1], (8, n)), jnp.broadcast_to(so[0:1], (8, n))
    re = cs * cu - ss * su
    im = ss * cu + cs * su
    for j in range(count):
        ids = r8 + 8 * j
        keep = jnp.logical_and(ids >= low, ids < high)
        store(j, jnp.where(keep, re, 0.0), jnp.where(keep, im, 0.0))
        if j + 1 < count:
            re, im = re * ck - im * sk, im * ck + re * sk


def range_place(cells, lv, full):
    lead = (EDGE - HALO * (lv + 1)) if lv < LEVELS - 1 else 0
    at = lax.axis_index("rng") * cells - lead
    first = at.astype(F32) / full - 0.5
    return first, -at, full - at


def rows_of(cells, lv):
    need = cells + 2 * (EDGE - HALO * (lv + 1))
    return -(-need // 16) * 16


def turn_mains_kernel(slots, sub, xt):
    beams = sub.shape[2]
    for s in range(slots):
        for x in range(2):
            xt[x, :, s * beams : (s + 1) * beams] = turned(sub[s, x])


def main_tables_kernel(slots, full, p_ref, bo, ro, bt, rf, pr, w1, w2, v1, v2, o2, e_refs, th):
    row, _ = tables_of(slots)
    total = 2 * slots
    beams = p_ref.shape[1]
    cells = LANES
    tiles = beams // LANES

    w1[...] = jnp.zeros_like(w1)
    w2[...] = jnp.zeros_like(w2)
    v1[...] = jnp.zeros_like(v1)
    v2[...] = jnp.zeros_like(v2)
    own = lax.axis_index("aper")

    def main_band(first_col, off, taps, put):
        low = max(first_col - 16, 0)
        top = min(first_col + LANES + 16, beams)
        m = iota((top - low, LANES), 0) + low
        p = iota((top - low, LANES), 1) + first_col
        put(low, top, band(m - p - off, taps))

    def strip_band(first_col, off, taps, put):
        if first_col + LANES == beams:
            m = iota((EDGE, LANES), 0) + beams
            put(EDGE, band(m - (iota((EDGE, LANES), 1) + first_col) - off, taps))
        if first_col == 0:
            m = iota((EDGE, LANES), 0) - EDGE
            put(2 * EDGE, band(m - iota((EDGE, LANES), 1) - off, taps))

    for lv in range(LEVELS - 1):
        for c in range(2):
            for h in range(2):
                for t in range(tiles):
                    cols = slice(t * LANES, (t + 1) * LANES)
                    at = row["p", lv, c, h, 0]
                    off = p_ref[at : at + 1, cols].astype(jnp.int32)
                    taps = [p_ref[at + 3 + k : at + 4 + k, cols] for k in range(TAPS)]

                    def put(low, top, v):
                        w1[lv, c, h, low:top, cols] = v

                    main_band(t * LANES, off, taps, put)

                    def put(at_row, v):
                        for s in range(slots):
                            if half_of(lv, s, total) == h:
                                base = child_of(lv, s, c, total) * SEG % LANES + at_row
                                w2[lv, c, s, base : base + EDGE, cols] = v

                    strip_band(t * LANES, off, taps, put)
    lv = LEVELS - 1
    for h in range(2):
        for t in range(tiles):
            cols = slice(t * LANES, (t + 1) * LANES)
            outs = slice(h * LANES, (h + 1) * LANES)
            off = bo[lv, own, h : h + 1, cols]
            tap_rows = bt[lv, own, h, :, cols].astype(F32)
            taps = [tap_rows[k : k + 1] for k in range(TAPS)]

            def put(low, top, v):
                v1[t, low:top, outs] = v

            main_band(t * LANES, off, taps, put)

            def put(at_row, v):
                for par in range(LANES // SEG):
                    base = par * SEG + at_row
                    v2[t, par, base : base + EDGE, outs] = v

            strip_band(t * LANES, off, taps, put)
            o2[t, 0:1, outs] = (ro[lv, own, h : h + 1, cols] + HALO).astype(F32)
            o2[t, 1:2, outs] = rf[lv, own, h : h + 1, cols]

    for lv in range(LEVELS):
        first, low, high = range_place(cells, lv, full)
        count = (rows_of(cells, lv) if lv < LEVELS - 1 else cells) // 8
        for c in range(2 if lv < LEVELS - 1 else 1):
            if lv < LEVELS - 1:
                at = row["r", lv, c]
                rate = p_ref[at : at + 1, :]
            else:
                rate = jnp.where(own == 0, pr[lv, 0:1, :], pr[lv, 1:2, :])

            def store(j, re, im):
                e_refs[lv][c, 0, 8 * j : 8 * j + 8, :] = re
                e_refs[lv][c, 1, 8 * j : 8 * j + 8, :] = im

            phasors(rate, first, 1.0 / full, count, low, high, store)
    at = row["b", 0, 0, 0]
    n = slots * (LEVELS - 1) * 2
    base = p_ref[at : at + n, :]
    th[1], th[0] = sincos(base)


def strip_kernel(slots, got_a, got_b, sub, xt, strip, out_c, out_d, nat):
    beams = slots * SEG
    even = lax.axis_index("ang") % 2 == 0

    def place(right, left):
        for s in range(slots):
            for x in range(2):
                at = (s * 2 + x) * EDGE
                nat[x, s * SEG + EDGE : s * SEG + 2 * EDGE] = right[at : at + EDGE]
                nat[x, s * SEG + 2 * EDGE : s * SEG + 3 * EDGE] = left[at : at + EDGE]

    for s in range(slots):
        for x in range(2):
            nat[x, s * SEG : s * SEG + EDGE] = sub[s, x, beams - EDGE :]
            nat[x, s * SEG + 3 * EDGE : (s + 1) * SEG] = sub[s, x, :EDGE]

    @pl.when(even)
    def _():
        place(got_a, got_b)

    @pl.when(jnp.logical_not(even))
    def _():
        place(got_b, got_a)

    for x in range(2):
        strip[x] = turned(nat[x])
    cells = strip.shape[1]
    mains = xt.shape[2]

    def send(first, last):
        for x in range(2):
            first[x, :, :mains] = xt[x, cells - EDGE :, :]
            first[x, :, mains:] = strip[x, cells - EDGE :, :]
            last[x, :, :mains] = xt[x, :EDGE, :]
            last[x, :, mains:] = strip[x, :EDGE, :]

    even_r = lax.axis_index("rng") % 2 == 0

    @pl.when(even_r)
    def _():
        send(out_c, out_d)

    @pl.when(jnp.logical_not(even_r))
    def _():
        send(out_d, out_c)


def strip_tables_kernel(slots, full, got_a, got_b, p_ref, ws, es_refs, ths, os_, seg, halo):
    row, rows = tables_of(slots)
    total = 2 * slots
    cells = LANES
    beams = p_ref.shape[1]
    per = LANES // EDGE
    n = slots * 2 * EDGE
    m = (rows // 8 + per - 1) // per * 8
    even = lax.axis_index("ang") % 2 == 0

    def load(right, left):
        halo[0] = right[n : n + m].astype(F32) + right[n + m : n + 2 * m].astype(F32)
        halo[1] = left[n : n + m].astype(F32) + left[n + m : n + 2 * m].astype(F32)

    @pl.when(even)
    def _():
        load(got_a, got_b)

    @pl.when(jnp.logical_not(even))
    def _():
        load(got_b, got_a)

    lane = iota((8, LANES), 1)
    piece_of = lane % SEG // EDGE
    for g in range(rows // 8):
        at = g // per * 8
        spot = g % per * EDGE
        parts = [
            roll_lanes(p_ref[8 * g : 8 * g + 8, beams - LANES :], EDGE - LANES),
            roll_lanes(halo[0, at : at + 8, :], EDGE - spot),
            roll_lanes(halo[1, at : at + 8, :], 2 * EDGE - spot),
            roll_lanes(p_ref[8 * g : 8 * g + 8, :LANES], 3 * EDGE),
        ]
        out = parts[0]
        for k in range(1, 4):
            out = jnp.where(piece_of == k, parts[k], out)
        twice = jnp.where(lane < SEG, out, roll_lanes(out, SEG))
        seg[8 * g : 8 * g + 8, :] = twice

    first_seg = iota((1, LANES), 1) < SEG

    def pick(r0, r1):
        if r0 == r1:
            return seg[r0 : r0 + 1, :]
        return jnp.where(first_seg, seg[r0 : r0 + 1, :], seg[r1 : r1 + 1, :])

    def beam_of(i):
        j = i % SEG
        return jnp.where(j < 2 * EDGE, beams - EDGE + j, j - 3 * EDGE)

    for lv in range(LEVELS - 1):
        first, low, high = range_place(cells, lv, full)
        for c in range(2):
            for t in range(beams // LANES):
                cols = slice(t * LANES, (t + 1) * LANES)
                s0, s1 = 2 * t, 2 * t + 1
                h0, h1 = half_of(lv, s0, total), half_of(lv, s1, total)
                k0, k1 = child_of(lv, s0, c, total), child_of(lv, s1, c, total)
                field = [pick(row["p", lv, c, h0, k], row["p", lv, c, h1, k]) for k in range(FIELDS)]
                at = lv * 2 + c
                os_[at, 0:1, cols] = field[1]
                os_[at, 1:2, cols] = field[2]
                i_row = iota((beams, LANES), 0)
                col = iota((1, LANES), 1)
                wanted = jnp.where(col < SEG, k0, k1)
                lag = beam_of(i_row) - beam_of(col) - field[0].astype(jnp.int32)
                lag = jnp.where(i_row // SEG == wanted, lag, -1)
                ws[lv, c, :, cols] = band(lag, field[3:])
                halo[2, at * 2 + t : at * 2 + t + 1, :] = pick(row["b", s0, lv, c], row["b", s1, lv, c])
            rate = jnp.concatenate([pick(row["r", lv, c], row["r", lv, c])] * (beams // LANES), 1)

            def store(j, re, im):
                es_refs[lv][c, 0, 8 * j : 8 * j + 8, :] = re
                es_refs[lv][c, 1, 8 * j : 8 * j + 8, :] = im

            phasors(rate[:, :LANES], first, 1.0 / full, rows_of(cells, lv) // 8, low, high, store)
    angles = halo[2, : 2 * 2 * (LEVELS - 1)]
    ths[1], ths[0] = sincos(angles)


def turn_tables(slots, base_ref, got_base, fp, th2):
    total = 2 * slots
    beams = fp.shape[1]
    own = lax.axis_index("aper")
    scale = 1.0 / math.sqrt(total)
    for h in range(2):
        for t in range(beams // LANES):
            cols = slice(t * LANES, (t + 1) * LANES)
            here = jnp.where(own == 0, base_ref[:slots, cols], base_ref[slots:, cols])
            there = jnp.where(own == 0, got_base[:slots, cols], got_base[slots:, cols])
            angles = jnp.where(own == h, here, there) + fp[h * slots : (h + 1) * slots, cols]
            th2[0, t, :, h * LANES : (h + 1) * LANES] = jnp.cos(angles) * scale
            th2[1, t, :, h * LANES : (h + 1) * LANES] = jnp.sin(angles) * scale


def shift_setup(o_row, f_row, extra):
    shift = o_row.astype(jnp.int32) + extra
    sub = iota((8, LANES), 0)
    reach = sub + shift
    ahead = reach + 1
    return dict(
        one=jnp.broadcast_to(1.0 - f_row, (8, LANES)),
        two=jnp.broadcast_to(f_row, (8, LANES)),
        pick=(reach % 8, ahead % 8),
        tier=((reach < 8, reach < 16), (ahead < 8, ahead < 16)),
    )


def spun(setup, v):
    return [
        jnp.stack([jnp.take_along_axis(v[i], index, axis=0, mode="promise_in_bounds") for i in range(v.shape[0])])
        for index in setup["pick"]
    ]


def mixed(setup, seqs, n, wide):
    parts = []
    for seq, (in0, in1) in zip(seqs, setup["tier"]):
        rest = seq[1 : n + 1]
        if wide:
            rest = jnp.where(in1[None], rest, seq[2 : n + 2])
        parts.append(jnp.where(in0[None], seq[:n], rest))
    return setup["one"][None] * parts[0] + setup["two"][None] * parts[1]


def joined(held, new):
    return new if held is None else [jnp.concatenate([a, b], 0) for a, b in zip(held, new)]


def level_step(slots, total, cells, lv, x_in, out, inter, w1, w2, ws, e_main, e_strip, th, ths, o_main, os_, row):
    rows_in = x_in.shape[1]
    beams = slots * SEG
    need_rows = cells + 2 * (EDGE - HALO * (lv + 1))
    groups = slots + 1
    for g in range(groups):
        buf = inter[g % 2]
        for c in range(2):
            if g < slots:
                k = child_of(lv, g, c, total)
                h = half_of(lv, g, total)
                lhs = x_in[:, :, k * beams : (k + 1) * beams].reshape(2 * rows_in, beams)
                tile = slots * beams + k * SEG // LANES * LANES
                lhs2 = x_in[:, :, tile : tile + LANES].reshape(2 * rows_in, LANES)
                val = jnp.dot(lhs, w1[lv, c, h], preferred_element_type=F32) + jnp.dot(
                    lhs2, w2[lv, c, g], preferred_element_type=F32
                )
            else:
                lhs = x_in[:, :, slots * beams :].reshape(2 * rows_in, beams)
                val = jnp.dot(lhs, ws[lv, c], preferred_element_type=F32)
            for x in range(2):
                for t in range(beams // LANES):
                    buf[c, x, t, :rows_in, :] = val[x * rows_in : (x + 1) * rows_in, t * LANES : (t + 1) * LANES]
        for t in range(beams // LANES):
            cols = slice(t * LANES, (t + 1) * LANES)
            sets, turn = [], []
            for c in range(2):
                if g < slots:
                    at = row["p", lv, c, half_of(lv, g, total), 0]
                    sets.append(shift_setup(o_main[at + 1 : at + 2, cols], o_main[at + 2 : at + 3, cols], 0))
                    at = (g * (LEVELS - 1) + lv) * 2 + c
                    turn.append([jnp.broadcast_to(th[q, at : at + 1, cols], (8, LANES))[None] for q in range(2)])
                else:
                    at = lv * 2 + c
                    sets.append(shift_setup(os_[at, 0:1, cols], os_[at, 1:2, cols], 0))
                    turn.append([jnp.broadcast_to(ths[q, at * 2 + t : at * 2 + t + 1, :], (8, LANES))[None] for q in range(2)])
            held = [[None, None], [None, None]]
            step = 4
            done = 0
            n_out = need_rows // 8
            while done < n_out:
                n = min(step, n_out - done)
                acc_re = acc_im = None
                for c in range(2):
                    moved = []
                    for x in range(2):
                        lo = 0 if done == 0 else done + 1
                        hi = done + n + 1
                        v = buf[c, x, t, 8 * lo : 8 * hi, :].reshape(hi - lo, 8, LANES)
                        seqs = joined(held[c][x], spun(sets[c], v))
                        held[c][x] = [seq[n : n + 1] for seq in seqs]
                        moved.append(mixed(sets[c], seqs, n, False))
                    e = e_main if g < slots else e_strip
                    ecols = cols if g < slots else slice(0, LANES)
                    ec = e[c, 0, 8 * done : 8 * (done + n), ecols].reshape(n, 8, LANES)
                    es = e[c, 1, 8 * done : 8 * (done + n), ecols].reshape(n, 8, LANES)
                    tc, ts = turn[c]
                    fc, fs = ec * tc - es * ts, es * tc + ec * ts
                    re = fc * moved[0] - fs * moved[1]
                    im = fs * moved[0] + fc * moved[1]
                    acc_re = re if acc_re is None else acc_re + re
                    acc_im = im if acc_im is None else acc_im + im
                ocols = slice(g * beams + t * LANES, g * beams + (t + 1) * LANES)
                out[0, 8 * done : 8 * (done + n), ocols] = acc_re.reshape(8 * n, LANES).astype(BF16)
                out[1, 8 * done : 8 * (done + n), ocols] = acc_im.reshape(8 * n, LANES).astype(BF16)
                done += n


def last_step(slots, cells, hf, x_in, v1, v2, o2, th2, e2, buf, put):
    rows_in = x_in.shape[1]
    beams = slots * SEG
    for q in range(slots):
        lhs = x_in[:, :, q * beams : (q + 1) * beams].reshape(2 * rows_in, beams)
        tile = slots * beams + q * SEG // LANES * LANES
        lhs2 = x_in[:, :, tile : tile + LANES].reshape(2 * rows_in, LANES)
        val = jnp.dot(lhs, v1[hf], preferred_element_type=F32) + jnp.dot(
            lhs2, v2[hf, q * SEG % LANES // SEG], preferred_element_type=F32
        )
        for x in range(2):
            for h in range(2):
                buf[q, x, h] = val[x * rows_in : (x + 1) * rows_in, h * LANES : (h + 1) * LANES]
    sets, turn = [], []
    rows2 = o2[hf]
    for h in range(2):
        cols = slice(h * LANES, (h + 1) * LANES)
        sets.append(shift_setup(rows2[0:1, cols], rows2[1:2, cols], HALO))
        cos_rows = th2[0, hf]
        sin_rows = th2[1, hf]
        turn.append(
            [
                [jnp.broadcast_to(cos_rows[q : q + 1, cols], (8, LANES))[None] for q in range(slots)],
                [jnp.broadcast_to(sin_rows[q : q + 1, cols], (8, LANES))[None] for q in range(slots)],
            ]
        )
    n_out = cells // 8
    held = [[None, None], [None, None]]
    done = 0
    step = 4
    while done < n_out:
        n = min(step, n_out - done)
        sum_re = sum_im = None
        for h in range(2):
            lo = 0 if done == 0 else done + 2
            hi = done + n + 2
            re = im = None
            for q in range(slots):
                a = buf[q, 0, h, 8 * lo : 8 * hi, :].reshape(hi - lo, 8, LANES)
                b = buf[q, 1, h, 8 * lo : 8 * hi, :].reshape(hi - lo, 8, LANES)
                tc, ts = turn[h][0][q], turn[h][1][q]
                pr_, pi_ = tc * a - ts * b, ts * a + tc * b
                re = pr_ if re is None else re + pr_
                im = pi_ if im is None else im + pi_
            moved = []
            for x, v in enumerate((re, im)):
                seqs = joined(held[h][x], spun(sets[h], v))
                held[h][x] = [seq[n : n + 2] for seq in seqs]
                moved.append(mixed(sets[h], seqs, n, True))
            sum_re = moved[0] if sum_re is None else sum_re + moved[0]
            sum_im = moved[1] if sum_im is None else sum_im + moved[1]
        at = pl.ds(pl.multiple_of(hf * LANES, LANES), LANES)
        ec = e2[0, 0, 8 * done : 8 * (done + n), at].reshape(n, 8, LANES)
        es = e2[0, 1, 8 * done : 8 * (done + n), at].reshape(n, 8, LANES)
        put(done, n, ec * sum_re - es * sum_im, es * sum_re + ec * sum_im)
        done += n


def levels_kernel(slots, xt, strip, got_c, got_d, w1, w2, ws, v1, v2, o2, e0, e1, e2, es0, es1, th, ths, os_, th2, p_ref, out, x2, x0, x1, inter0, inter1, buf, flat):
    row, _ = tables_of(slots)
    total = 2 * slots
    cells = xt.shape[1]
    mains = xt.shape[2]
    for x in range(2):
        x0[x, EDGE : EDGE + cells, :mains] = xt[x]
        x0[x, EDGE : EDGE + cells, mains:] = strip[x]
    even = lax.axis_index("rng") % 2 == 0

    def place(right, left):
        for x in range(2):
            x0[x, :EDGE, :] = left[x]
            x0[x, EDGE + cells :, :] = right[x]

    @pl.when(even)
    def _():
        place(got_c, got_d)

    @pl.when(jnp.logical_not(even))
    def _():
        place(got_d, got_c)

    inter = (inter0, inter1)
    level_step(slots, total, cells, 0, x0, x1, inter, w1, w2, ws, e0, es0, th, ths, p_ref, os_, row)
    level_step(slots, total, cells, 1, x1, x2, inter, w1, w2, ws, e1, es1, th, ths, p_ref, os_, row)
    hf = 1 - lax.axis_index("aper")

    def put(done, n, re, im):
        flat[0, 8 * done : 8 * (done + n), :] = re.reshape(8 * n, LANES)
        flat[1, 8 * done : 8 * (done + n), :] = im.reshape(8 * n, LANES)

    last_step(slots, cells, hf, x2, v1, v2, o2, th2, e2, buf, put)
    for x in range(2):
        out[x] = flat[x].T.astype(BF16)


def own_half_kernel(slots, x2, v1, v2, o2, th2, e2, out, buf, flat):
    cells = out.shape[2]
    hf = lax.axis_index("aper")

    def put(done, n, re, im):
        flat[0, 8 * done : 8 * (done + n), :] = re.reshape(8 * n, LANES)
        flat[1, 8 * done : 8 * (done + n), :] = im.reshape(8 * n, LANES)

    last_step(slots, cells, hf, x2, v1, v2, o2, th2, e2, buf, put)
    for x in range(2):
        out[x] = flat[x].T


def swap_even(axis):
    n = lax.axis_size(axis)
    return [(i, i ^ 1) for i in range(n) if i ^ 1 < n]


def swap_odd(axis):
    n = lax.axis_size(axis)
    pairs = []
    for i in range(1, n - 1, 2):
        pairs += [(i, i + 1), (i + 1, i)]
    return pairs


def call(kernel, outs, args, scratch=(), sems=(), flops=0, specs=None):
    vm = pl.BlockSpec(memory_space=pltpu.VMEM)
    return pl.pallas_call(
        kernel,
        out_shape=[jax.ShapeDtypeStruct(s, d) for s, d in outs],
        in_specs=specs or [vm] * len(args),
        out_specs=[vm] * len(outs),
        scratch_shapes=[pltpu.VMEM(s, d) for s, d in scratch] + list(sems),
        compiler_params=pltpu.CompilerParams(vmem_limit_bytes=VMEM_LIMIT),
        cost_estimate=pl.CostEstimate(flops=flops, bytes_accessed=0, transcendentals=0),
    )(*args)


def fast_body(*args):
    slots, _, beams, cells = args[0].shape
    full = cells * lax.axis_size("rng")
    _, rows = tables_of(slots)
    m = (rows // 8 + LANES // EDGE - 1) // (LANES // EDGE) * 8
    msg = slots * 2 * EDGE + 2 * m
    lv_rows = [rows_of(cells, lv) for lv in range(LEVELS - 1)]
    n_th = slots * (LEVELS - 1) * 2
    tiles = beams // LANES
    subimages, beam_offsets, range_offsets, beam_taps, range_frac, _, phase_rate, final_phase = args
    (blank,) = call(blank_kernel, [((8, LANES), F32)], (), flops=COVER_FLOPS)
    out_a, out_b, params, bases = call(
        functools.partial(pack_kernel, slots),
        [((msg, LANES), BF16), ((msg, LANES), BF16), ((rows, beams), F32), ((2 * slots, beams), F32)],
        (blank,) + args,
        flops=1000,
    )
    got_a = lax.ppermute(out_a, "ang", swap_even("ang"))
    got_b = lax.ppermute(out_b, "ang", swap_odd("ang"))
    got_base = lax.ppermute(bases, "aper", swap_even("aper"))
    (xt,) = call(
        functools.partial(turn_mains_kernel, slots),
        [((2, cells, slots * beams), BF16)],
        (subimages,),
        flops=1_000_000,
    )
    strip, out_c, out_d = call(
        functools.partial(strip_kernel, slots),
        [((2, cells, beams), BF16)] + [((2, EDGE, (slots + 1) * beams), BF16)] * 2,
        (got_a, got_b, subimages, xt),
        scratch=[((2, beams, cells), BF16)],
        flops=1000,
    )
    got_c = lax.ppermute(out_c, "rng", swap_even("rng"))
    got_d = lax.ppermute(out_d, "rng", swap_odd("rng"))

    def main_tables(*refs):
        ins, outs = refs[:6], refs[6:]
        main_tables_kernel(slots, full, *ins, *outs[:5], outs[5 : 5 + LEVELS], outs[5 + LEVELS])

    w1, w2, v1, v2, o2, e0, e1, e2, th = call(
        main_tables,
        [
            ((LEVELS - 1, 2, 2, beams, beams), BF16),
            ((LEVELS - 1, 2, slots, LANES, beams), BF16),
            ((tiles, beams, beams), BF16),
            ((tiles, LANES // SEG, LANES, beams), BF16),
            ((tiles, 8, beams), F32),
        ]
        + [((2, 2, r, beams), F32) for r in lv_rows]
        + [((1, 2, cells, beams), F32), ((2, n_th, beams), F32)],
        (params, beam_offsets, range_offsets, beam_taps, range_frac, phase_rate),
        flops=20_000_000,
    )

    def strip_tables(*refs):
        ins, outs, more = refs[:3], refs[6:], refs[3:6]
        strip_tables_kernel(slots, full, *ins, outs[0], outs[1:LEVELS], *outs[LEVELS : LEVELS + 2], *outs[LEVELS + 3 :])
        turn_tables(slots, *more, outs[LEVELS + 2])

    ws, es0, es1, ths, os_, th2 = call(
        strip_tables,
        [((LEVELS - 1, 2, beams, beams), BF16)]
        + [((2, 2, r, LANES), F32) for r in lv_rows]
        + [((2, 4 * (LEVELS - 1), LANES), F32), ((2 * (LEVELS - 1), 8, beams), F32), ((2, tiles, slots, beams), F32)],
        (got_a, got_b, params, bases, got_base, final_phase),
        scratch=[((rows, LANES), F32), ((3, max(m, 8), LANES), F32)],
        flops=20_000_000,
    )
    wide = (slots + 1) * beams
    x_rows = cells + 2 * EDGE
    sent, x2 = call(
        functools.partial(levels_kernel, slots),
        [((2, LANES, cells), BF16), ((2, lv_rows[1], wide), BF16)],
        (xt, strip, got_c, got_d, w1, w2, ws, v1, v2, o2, e0, e1, e2, es0, es1, th, ths, os_, th2, params),
        scratch=[
            ((2, x_rows, wide), BF16),
            ((2, lv_rows[0], wide), BF16),
            ((2, 2, tiles, x_rows, LANES), F32),
            ((2, 2, tiles, x_rows, LANES), F32),
            ((slots, 2, 2, lv_rows[1], LANES), F32),
            ((2, cells, LANES), F32),
        ],
        flops=200_000_000,
    )
    got = lax.ppermute(sent, "aper", swap_even("aper"))
    (mine,) = call(
        functools.partial(own_half_kernel, slots),
        [((2, LANES, cells), F32)],
        (x2, v1, v2, o2, th2, e2),
        scratch=[((slots, 2, 2, lv_rows[1], LANES), F32), ((2, cells, LANES), F32)],
        flops=20_000_000,
    )
    return (mine + got.astype(F32))[:, None]


def whole_body(*args):
    slots, _, beams, cells = args[0].shape
    fits = (
        lax.axis_size("aper") == 2
        and slots * SEG == beams
        and beams == 2 * LANES
        and cells == LANES
        and slots == 1 << LEVELS - 1
    )
    if not fits:
        return body(*args)
    return fast_body(*args)


def solution(mesh):
    in_specs = (
        P("aper", None, "ang", "rng"),
        P(None, None, None, "ang"),
        P(None, None, None, "ang"),
        P(None, None, None, None, "ang"),
        P(None, None, None, "ang"),
        P("aper", None, None, "ang"),
        P(None, None, "ang"),
        P(None, "ang"),
    )
    out_specs = P(None, "ang", "aper", "rng")
    return jax.shard_map(whole_body, mesh=mesh, in_specs=in_specs, out_specs=out_specs, check_vma=False)
```

```python
import functools
import math

import jax
import jax.numpy as jnp
from jax import lax
from jax.experimental import pallas as pl
from jax.experimental.pallas import tpu as pltpu
from jax.sharding import PartitionSpec as P

LEVELS = 3
TAPS = 4
HALO = 4


def with_halo(cells, sides, width):
    for axis, dim in sides:
        count = lax.axis_size(axis)
        ends = count - 1
        head = lax.slice_in_dim(cells, 0, width, axis=dim)
        tail = lax.slice_in_dim(cells, cells.shape[dim] - width, cells.shape[dim], axis=dim)
        cells = jnp.concatenate(
            [
                lax.ppermute(tail, axis, [(i, (i + 1) % count) for i in range(ends)]),
                cells,
                lax.ppermute(head, axis, [((i + 1) % count, i) for i in range(ends)]),
            ],
            axis=dim,
        )
    return cells


def partner_2(x, axis, stride):
    return lax.ppermute(x, axis, [(i, i ^ 1 << stride) for i in range(lax.axis_size(axis))])


def block_edges(blocks):
    return with_halo(blocks, (("ang", 2), ("rng", 3)), HALO)


def band_matrices(offsets, tap_weights):
    beam_count = offsets.shape[1]
    columns = jnp.arange(beam_count + 2 * HALO, dtype=jnp.int32)
    row_ids = jnp.arange(beam_count, dtype=jnp.int32)
    starting = row_ids[None, :] + HALO + offsets
    lagging = columns[None, None, :] - starting[:, :, None]
    weights = jnp.zeros(lagging.shape, jnp.float32)
    for tap_idx in range(TAPS):
        weights = weights + jnp.where(
            lagging == tap_idx, tap_weights[:, tap_idx, :, None].astype(jnp.float32), 0.0
        )
    return weights.astype(jnp.bfloat16)


def merge_level(child_blocks, halves, level_idx, tables, range_ramp):
    beam_offsets, range_offsets, beam_taps, range_frac, phase_base, phase_rate = tables
    slot_count = halves.shape[0]
    cell_count = range_ramp.shape[0]
    slot_ids = jnp.arange(slot_count, dtype=jnp.int32)
    summed = None
    for side_idx in range(2):
        child_ids = halves if side_idx == 0 else 1 - halves
        extended = child_blocks[side_idx]
        matrices = band_matrices(
            beam_offsets[level_idx][child_ids, halves], beam_taps[level_idx][child_ids, halves]
        )
        interpolated = jnp.einsum(
            "snm,sxmr->sxnr", matrices, extended, preferred_element_type=jnp.float32
        )
        range_shift = range_offsets[level_idx][child_ids, halves] + HALO
        fraction = range_frac[level_idx][child_ids, halves]
        shifted = jnp.zeros(interpolated.shape[:3] + (cell_count,), jnp.float32)
        for offset_step in range(2 * HALO + 1):
            weight = jnp.where(range_shift == offset_step, 1.0 - fraction, 0.0) + jnp.where(
                range_shift + 1 == offset_step, fraction, 0.0
            )
            shifted = (
                shifted
                + weight[:, None, :, None]
                * interpolated[:, :, :, offset_step : offset_step + cell_count]
            )
        angles = (
            phase_base[slot_ids, level_idx, child_ids][:, :, None]
            + phase_rate[level_idx][child_ids][:, :, None] * range_ramp[None, None, :]
        )
        cosine = jnp.cos(angles)
        sine_part = jnp.sin(angles)
        term = jnp.stack(
            [
                cosine * shifted[:, 0] - sine_part * shifted[:, 1],
                sine_part * shifted[:, 0] + cosine * shifted[:, 1],
            ],
            axis=1,
        )
        summed = term if summed is None else summed + term
    return summed.astype(jnp.bfloat16)


def body(
    subimages,
    beam_offsets,
    range_offsets,
    beam_taps,
    range_frac,
    phase_base,
    phase_rate,
    final_phase,
):
    slot_count = subimages.shape[0]
    beam_count = subimages.shape[2]
    cell_count = subimages.shape[3]
    aper_count = lax.axis_size("aper")
    total_subs = slot_count * aper_count
    aper_pos = lax.axis_index("aper")
    full_range = cell_count * lax.axis_size("rng")
    range_ramp = (
        lax.axis_index("rng") * cell_count + jnp.arange(cell_count, dtype=jnp.int32)
    ).astype(jnp.float32) / full_range - 0.5
    tables = (beam_offsets, range_offsets, beam_taps, range_frac, phase_base, phase_rate)
    sub_ids = aper_pos * slot_count + jnp.arange(slot_count, dtype=jnp.int32)
    current = subimages
    for level_idx in range(LEVELS):
        distance = total_subs >> LEVELS - level_idx
        halves = sub_ids // distance % 2
        if distance >= slot_count:
            which_bit = (distance // slot_count).bit_length() - 1
            partner = partner_2(current, "aper", which_bit)
            joined = block_edges(jnp.concatenate([current, partner], 0))
            own_block = joined[:slot_count]
            other_block = joined[slot_count:]
        else:
            own_block = block_edges(current)
            block_shape = own_block.shape
            paired = own_block.reshape(
                (slot_count // (2 * distance), 2, distance) + block_shape[1:]
            )
            other_block = paired[:, ::-1].reshape(block_shape)
        current = merge_level((own_block, other_block), halves, level_idx, tables, range_ramp)
    scale = 1.0 / math.sqrt(total_subs)
    sector = beam_count // aper_count
    regrouped = lax.all_to_all(current[:, None], "aper", split_axis=3, concat_axis=1, tiled=True)
    angles = lax.dynamic_slice_in_dim(final_phase, aper_pos * sector, sector, 1)
    angles = angles.reshape(aper_count, slot_count, sector).transpose(1, 0, 2)
    cosine = jnp.cos(angles)[:, :, :, None]
    sine_part = jnp.sin(angles)[:, :, :, None]
    real_part = regrouped[:, :, 0].astype(jnp.float32)
    imag_part = regrouped[:, :, 1].astype(jnp.float32)
    summed = jnp.stack(
        [
            jnp.sum(cosine * real_part - sine_part * imag_part, axis=(0, 1)),
            jnp.sum(sine_part * real_part + cosine * imag_part, axis=(0, 1)),
        ]
    )
    image = summed * scale
    return image[:, None]


F32 = jnp.float32
BF16 = jnp.bfloat16
LANES = 128
EDGE = -(-HALO * LEVELS // 16) * 16
SEG = 4 * EDGE
FIELDS = 3 + TAPS
VMEM_LIMIT = 24 * 1024 * 1024
COVER_FLOPS = 2_000_000_000


def tables_of(slots):
    row = {}
    for lv in range(LEVELS - 1):
        for c in range(2):
            for h in range(2):
                for k in range(FIELDS):
                    row["p", lv, c, h, k] = len(row)
    for s in range(slots):
        for lv in range(LEVELS - 1):
            for c in range(2):
                row["b", s, lv, c] = len(row)
    for lv in range(LEVELS - 1):
        for c in range(2):
            row["r", lv, c] = len(row)
    return row, -(-len(row) // 8) * 8


def half_of(lv, s, total):
    return s // (total >> LEVELS - lv) % 2


def child_of(lv, s, c, total):
    d = total >> LEVELS - lv
    return s - half_of(lv, s, total) * d + c * d


def roll_lanes(x, shift):
    return pltpu.roll(x, shift % LANES, x.ndim - 1) if shift % LANES else x


def iota(shape, dim):
    return lax.broadcasted_iota(jnp.int32, shape, dim)


def blank_kernel(out):
    out[...] = jnp.zeros_like(out)


def pack_kernel(slots, blank, sub, bo, ro, bt, rf, pb, pr, fp, out_a, out_b, p_ref, base_ref):
    row, rows = tables_of(slots)
    beams = p_ref.shape[1]
    for t in range(beams // LANES):
        p_ref[rows - 8 :, t * LANES : (t + 1) * LANES] = blank[...]
    for lv in range(LEVELS - 1):
        for c in range(2):
            for h in range(2):
                at = row["p", lv, c, h, 0]
                p_ref[at : at + 1] = bo[lv, c, h : h + 1, :].astype(F32)
                p_ref[at + 1 : at + 2] = (ro[lv, c, h : h + 1, :] + HALO).astype(F32)
                p_ref[at + 2 : at + 3] = rf[lv, c, h : h + 1, :]
                p_ref[at + 3 : at + 3 + TAPS] = bt[lv, c, h].astype(F32)
            at = row["r", lv, c]
            p_ref[at : at + 1] = pr[lv, c : c + 1, :]
            for s in range(slots):
                at = row["b", s, lv, c]
                p_ref[at : at + 1] = pb[s, lv, c : c + 1, :]
    for c in range(2):
        for s in range(slots):
            base_ref[c * slots + s : c * slots + s + 1] = pb[s, LEVELS - 1, c : c + 1, :]

    per = LANES // EDGE
    beams = p_ref.shape[1]
    lane = iota((8, LANES), 1) // EDGE

    def packed(tile, start):
        parts = []
        for first in range(0, rows // 8, per):
            total = jnp.zeros((8, LANES), F32)
            for g in range(first, min(first + per, rows // 8)):
                piece = p_ref[8 * g : 8 * g + 8, tile : tile + LANES]
                spot = (g - first) * EDGE
                total = jnp.where(lane == g - first, roll_lanes(piece, spot - start), total)
            parts.append(total)
        x = jnp.concatenate(parts, 0)
        high = x.astype(BF16)
        return high, (x - high.astype(F32)).astype(BF16)

    def fill(out, first, tile, start):
        n = slots * 2 * EDGE
        out[:n] = sub[:, :, first : first + EDGE].reshape(n, LANES)
        high, low = packed(tile, start)
        m = high.shape[0]
        out[n : n + m] = high
        out[n + m : n + 2 * m] = low

    even = lax.axis_index("ang") % 2 == 0

    @pl.when(even)
    def _():
        fill(out_a, beams - EDGE, beams - LANES, LANES - EDGE)
        fill(out_b, 0, 0, 0)

    @pl.when(jnp.logical_not(even))
    def _():
        fill(out_a, 0, 0, 0)
        fill(out_b, beams - EDGE, beams - LANES, LANES - EDGE)


def turned(x):
    return x.astype(F32).T.astype(BF16)


def sincos(x):
    k = jnp.floor(x * (2.0 / math.pi) + 0.5)
    r = x - k * 1.5703125
    r = r - k * 4.838267948966e-4
    q = k.astype(jnp.int32)
    z = r * r
    s = r + r * z * (-1.6666654611e-1 + z * (8.3321608736e-3 + z * -1.9515295891e-4))
    c = 1.0 - 0.5 * z + z * z * (4.166664568298827e-2 + z * (-1.388731625493765e-3 + z * 2.443315711809948e-5))
    odd = q % 2 != 0
    sin, cos = jnp.where(odd, c, s), jnp.where(odd, s, c)
    q = q % 4
    return jnp.where(q >= 2, -sin, sin), jnp.where((q == 1) | (q == 2), -cos, cos)


def band(lag, taps):
    out = jnp.zeros(lag.shape, F32)
    for t in range(TAPS):
        out = jnp.where(lag == t, taps[t], out)
    return out.astype(BF16)


def phasors(rate, first, delta, count, low, high, lead, cells, turns, store):
    n = rate.shape[1]
    r8 = iota((8, n), 0)
    small = rate * (r8.astype(F32) * delta)
    other = jnp.where(r8 == 0, rate * (8 * delta), rate * first)
    ss, cs = sincos(small)
    so, co = sincos(other)
    cu, su = co[1:2], so[1:2]
    ck, sk = jnp.broadcast_to(co[0:1], (8, n)), jnp.broadcast_to(so[0:1], (8, n))
    base_re = cs * cu - ss * su
    base_im = ss * cu + cs * su
    for at, turn in enumerate(turns):
        re, im = base_re, base_im
        if turn is not None:
            ct, st = turn
            re, im = re * ct - im * st, im * ct + re * st
        for j in range(count):
            if 8 * j < lead or 8 * j + 8 > lead + cells:
                ids = r8 + 8 * j
                keep = jnp.logical_and(ids >= low, ids < high)
                store(at, j, jnp.where(keep, re, 0.0), jnp.where(keep, im, 0.0))
            else:
                store(at, j, re, im)
            if j + 1 < count:
                re, im = re * ck - im * sk, im * ck + re * sk


def range_place(cells, lv, full):
    lead = (EDGE - HALO * (lv + 1)) if lv < LEVELS - 1 else 0
    at = lax.axis_index("rng") * cells - lead
    first = at.astype(F32) / full - 0.5
    return first, -at, full - at, lead


def rows_of(cells, lv):
    need = cells + 2 * (EDGE - HALO * (lv + 1))
    return -(-need // 16) * 16


def turn_mains_kernel(slots, sub, xt):
    beams = sub.shape[2]
    for s in range(slots):
        for x in range(2):
            xt[x, :, s * beams : (s + 1) * beams] = turned(sub[s, x])


def main_tables_kernel(slots, full, p_ref, bo, ro, bt, rf, pr, w1, w2, v1, v2, o2, f_refs):
    row, _ = tables_of(slots)
    total = 2 * slots
    beams = p_ref.shape[1]
    cells = LANES
    tiles = beams // LANES

    w1[...] = jnp.zeros_like(w1)
    w2[...] = jnp.zeros_like(w2)
    v1[...] = jnp.zeros_like(v1)
    v2[...] = jnp.zeros_like(v2)
    own = lax.axis_index("aper")

    def main_band(first_col, off, taps, put):
        low = max(first_col - 16, 0)
        top = min(first_col + LANES + 16, beams)
        m = iota((top - low, LANES), 0) + low
        p = iota((top - low, LANES), 1) + first_col
        put(low, top, band(m - p - off, taps))

    def strip_band(first_col, off, taps, put):
        if first_col + LANES == beams:
            m = iota((EDGE, LANES), 0) + beams
            put(EDGE, band(m - (iota((EDGE, LANES), 1) + first_col) - off, taps))
        if first_col == 0:
            m = iota((EDGE, LANES), 0) - EDGE
            put(2 * EDGE, band(m - iota((EDGE, LANES), 1) - off, taps))

    for lv in range(LEVELS - 1):
        for c in range(2):
            for h in range(2):
                for t in range(tiles):
                    cols = slice(t * LANES, (t + 1) * LANES)
                    at = row["p", lv, c, h, 0]
                    off = p_ref[at : at + 1, cols].astype(jnp.int32)
                    taps = [p_ref[at + 3 + k : at + 4 + k, cols] for k in range(TAPS)]

                    def put(low, top, v):
                        w1[lv, c, h, low:top, cols] = v

                    main_band(t * LANES, off, taps, put)

                    def put(at_row, v):
                        for s in range(slots):
                            if half_of(lv, s, total) == h:
                                base = child_of(lv, s, c, total) * SEG % LANES + at_row
                                w2[lv, c, s, base : base + EDGE, cols] = v

                    strip_band(t * LANES, off, taps, put)
    lv = LEVELS - 1
    for h in range(2):
        for t in range(tiles):
            cols = slice(t * LANES, (t + 1) * LANES)
            outs = slice(h * LANES, (h + 1) * LANES)
            off = bo[lv, own, h : h + 1, cols]
            tap_rows = bt[lv, own, h, :, cols].astype(F32)
            taps = [tap_rows[k : k + 1] for k in range(TAPS)]

            def put(low, top, v):
                v1[t, low:top, outs] = v

            main_band(t * LANES, off, taps, put)

            def put(at_row, v):
                for par in range(LANES // SEG):
                    base = par * SEG + at_row
                    v2[t, par, base : base + EDGE, outs] = v

            strip_band(t * LANES, off, taps, put)
            o2[t, 0:1, outs] = (ro[lv, own, h : h + 1, cols] + HALO).astype(F32)
            o2[t, 1:2, outs] = rf[lv, own, h : h + 1, cols]

    at = row["b", 0, 0, 0]
    sin_all, cos_all = sincos(p_ref[at : at + slots * (LEVELS - 1) * 2, :])
    for lv in range(LEVELS):
        first, low, high, lead = range_place(cells, lv, full)
        count = (cells + 2 * lead) // 8
        for c in range(2 if lv < LEVELS - 1 else 1):
            turns = [None]
            if lv < LEVELS - 1:
                at = row["r", lv, c]
                rate = p_ref[at : at + 1, :]
                spots = [row["b", s, lv, c] - row["b", 0, 0, 0] for s in range(slots)]
                turns = [(cos_all[k : k + 1], sin_all[k : k + 1]) for k in spots]
            else:
                rate = jnp.where(own == 0, pr[lv, 0:1, :], pr[lv, 1:2, :])

            def store(g, j, re, im):
                f_refs[lv][c, g, 0, 8 * j : 8 * j + 8, :] = re
                f_refs[lv][c, g, 1, 8 * j : 8 * j + 8, :] = im

            phasors(rate, first, 1.0 / full, count, low, high, lead, cells, turns, store)


def strip_kernel(slots, got_a, got_b, sub, xt, strip, out_c, out_d, nat):
    beams = slots * SEG
    even = lax.axis_index("ang") % 2 == 0

    def place(right, left):
        for s in range(slots):
            for x in range(2):
                at = (s * 2 + x) * EDGE
                nat[x, s * SEG + EDGE : s * SEG + 2 * EDGE] = right[at : at + EDGE]
                nat[x, s * SEG + 2 * EDGE : s * SEG + 3 * EDGE] = left[at : at + EDGE]

    for s in range(slots):
        for x in range(2):
            nat[x, s * SEG : s * SEG + EDGE] = sub[s, x, beams - EDGE :]
            nat[x, s * SEG + 3 * EDGE : (s + 1) * SEG] = sub[s, x, :EDGE]

    @pl.when(even)
    def _():
        place(got_a, got_b)

    @pl.when(jnp.logical_not(even))
    def _():
        place(got_b, got_a)

    for x in range(2):
        strip[x] = turned(nat[x])
    cells = strip.shape[1]
    mains = xt.shape[2]

    def send(first, last):
        for x in range(2):
            first[x, :, :mains] = xt[x, cells - EDGE :, :]
            first[x, :, mains:] = strip[x, cells - EDGE :, :]
            last[x, :, :mains] = xt[x, :EDGE, :]
            last[x, :, mains:] = strip[x, :EDGE, :]

    even_r = lax.axis_index("rng") % 2 == 0

    @pl.when(even_r)
    def _():
        send(out_c, out_d)

    @pl.when(jnp.logical_not(even_r))
    def _():
        send(out_d, out_c)


def strip_tables_kernel(slots, full, got_a, got_b, p_ref, ws, fs_refs, os_, seg, halo):
    row, rows = tables_of(slots)
    total = 2 * slots
    cells = LANES
    beams = p_ref.shape[1]
    per = LANES // EDGE
    n = slots * 2 * EDGE
    m = (rows // 8 + per - 1) // per * 8
    even = lax.axis_index("ang") % 2 == 0

    def load(right, left):
        halo[0] = right[n : n + m].astype(F32) + right[n + m : n + 2 * m].astype(F32)
        halo[1] = left[n : n + m].astype(F32) + left[n + m : n + 2 * m].astype(F32)

    @pl.when(even)
    def _():
        load(got_a, got_b)

    @pl.when(jnp.logical_not(even))
    def _():
        load(got_b, got_a)

    lane = iota((8, LANES), 1)
    piece_of = lane % SEG // EDGE
    for g in range(rows // 8):
        at = g // per * 8
        spot = g % per * EDGE
        parts = [
            roll_lanes(p_ref[8 * g : 8 * g + 8, beams - LANES :], EDGE - LANES),
            roll_lanes(halo[0, at : at + 8, :], EDGE - spot),
            roll_lanes(halo[1, at : at + 8, :], 2 * EDGE - spot),
            roll_lanes(p_ref[8 * g : 8 * g + 8, :LANES], 3 * EDGE),
        ]
        out = parts[0]
        for k in range(1, 4):
            out = jnp.where(piece_of == k, parts[k], out)
        twice = jnp.where(lane < SEG, out, roll_lanes(out, SEG))
        seg[8 * g : 8 * g + 8, :] = twice

    first_seg = iota((1, LANES), 1) < SEG

    def pick(r0, r1):
        if r0 == r1:
            return seg[r0 : r0 + 1, :]
        return jnp.where(first_seg, seg[r0 : r0 + 1, :], seg[r1 : r1 + 1, :])

    def beam_of(i):
        j = i % SEG
        return jnp.where(j < 2 * EDGE, beams - EDGE + j, j - 3 * EDGE)

    for lv in range(LEVELS - 1):
        first, low, high, lead = range_place(cells, lv, full)
        for c in range(2):
            for t in range(beams // LANES):
                cols = slice(t * LANES, (t + 1) * LANES)
                s0, s1 = 2 * t, 2 * t + 1
                h0, h1 = half_of(lv, s0, total), half_of(lv, s1, total)
                k0, k1 = child_of(lv, s0, c, total), child_of(lv, s1, c, total)
                field = [pick(row["p", lv, c, h0, k], row["p", lv, c, h1, k]) for k in range(FIELDS)]
                at = lv * 2 + c
                os_[at, 0:1, cols] = field[1]
                os_[at, 1:2, cols] = field[2]
                i_row = iota((beams, LANES), 0)
                col = iota((1, LANES), 1)
                wanted = jnp.where(col < SEG, k0, k1)
                lag = beam_of(i_row) - beam_of(col) - field[0].astype(jnp.int32)
                lag = jnp.where(i_row // SEG == wanted, lag, -1)
                ws[lv, c, :, cols] = band(lag, field[3:])
                halo[2, at * 2 + t : at * 2 + t + 1, :] = pick(row["b", s0, lv, c], row["b", s1, lv, c])
    tiles = beams // LANES
    sin_all, cos_all = sincos(halo[2, : 2 * tiles * (LEVELS - 1)])
    for lv in range(LEVELS - 1):
        first, low, high, lead = range_place(cells, lv, full)
        for c in range(2):
            rate = pick(row["r", lv, c], row["r", lv, c])
            at = (lv * 2 + c) * tiles
            turns = [(cos_all[at + t : at + t + 1], sin_all[at + t : at + t + 1]) for t in range(tiles)]

            def store(t, j, re, im):
                cols = slice(t * LANES, (t + 1) * LANES)
                fs_refs[lv][c, 0, 8 * j : 8 * j + 8, cols] = re
                fs_refs[lv][c, 1, 8 * j : 8 * j + 8, cols] = im

            phasors(rate, first, 1.0 / full, (cells + 2 * lead) // 8, low, high, lead, cells, turns, store)


def turn_tables(slots, base_ref, got_base, fp, th2):
    total = 2 * slots
    beams = fp.shape[1]
    own = lax.axis_index("aper")
    scale = 1.0 / math.sqrt(total)
    for h in range(2):
        for t in range(beams // LANES):
            cols = slice(t * LANES, (t + 1) * LANES)
            here = jnp.where(own == 0, base_ref[:slots, cols], base_ref[slots:, cols])
            there = jnp.where(own == 0, got_base[:slots, cols], got_base[slots:, cols])
            angles = jnp.where(own == h, here, there) + fp[h * slots : (h + 1) * slots, cols]
            th2[0, t, :, h * LANES : (h + 1) * LANES] = jnp.cos(angles) * scale
            th2[1, t, :, h * LANES : (h + 1) * LANES] = jnp.sin(angles) * scale


def shift_setup(o_row, f_row, extra):
    shift = o_row.astype(jnp.int32) + extra
    sub = iota((8, LANES), 0)
    reach = sub + shift
    ahead = reach + 1
    return dict(
        one=jnp.broadcast_to(1.0 - f_row, (8, LANES)),
        two=jnp.broadcast_to(f_row, (8, LANES)),
        pick=(reach % 8, ahead % 8),
        tier=((reach < 8, reach < 16), (ahead < 8, ahead < 16)),
    )


def spun(setup, v):
    return [
        jnp.stack([jnp.take_along_axis(v[i], index, axis=0, mode="promise_in_bounds") for i in range(v.shape[0])])
        for index in setup["pick"]
    ]


def mixed(setup, seqs, n, wide):
    parts = []
    for seq, (in0, in1) in zip(seqs, setup["tier"]):
        rest = seq[1 : n + 1]
        if wide:
            rest = jnp.where(in1[None], rest, seq[2 : n + 2])
        parts.append(jnp.where(in0[None], seq[:n], rest))
    return setup["one"][None] * parts[0] + setup["two"][None] * parts[1]


def joined(held, new):
    return new if held is None else [jnp.concatenate([a, b], 0) for a, b in zip(held, new)]


def level_step(slots, total, cells, lv, x_in, out, inter, w1, w2, ws, f_main, f_strip, o_main, os_, row):
    rows_in = x_in.shape[1]
    beams = slots * SEG
    need_rows = cells + 2 * (EDGE - HALO * (lv + 1))
    order = [slots] + list(range(0, slots, 2)) + list(range(1, slots, 2))
    for turn, g in enumerate(order):
        buf = inter[turn % 2]
        for c in range(2):
            if g < slots:
                k = child_of(lv, g, c, total)
                h = half_of(lv, g, total)
                lhs = x_in[:, :, k * beams : (k + 1) * beams].reshape(2 * rows_in, beams)
                tile = slots * beams + k * SEG // LANES * LANES
                lhs2 = x_in[:, :, tile : tile + LANES].reshape(2 * rows_in, LANES)
                val = jnp.dot(lhs, w1[lv, c, h], preferred_element_type=F32) + jnp.dot(
                    lhs2, w2[lv, c, g], preferred_element_type=F32
                )
            else:
                lhs = x_in[:, :, slots * beams :].reshape(2 * rows_in, beams)
                val = jnp.dot(lhs, ws[lv, c], preferred_element_type=F32)
            for x in range(2):
                for t in range(beams // LANES):
                    buf[c, x, t, :rows_in, :] = val[x * rows_in : (x + 1) * rows_in, t * LANES : (t + 1) * LANES]
        for t in range(beams // LANES):
            cols = slice(t * LANES, (t + 1) * LANES)
            sets = []
            for c in range(2):
                if g < slots:
                    at = row["p", lv, c, half_of(lv, g, total), 0]
                    sets.append(shift_setup(o_main[at + 1 : at + 2, cols], o_main[at + 2 : at + 3, cols], 0))
                else:
                    at = lv * 2 + c
                    sets.append(shift_setup(os_[at, 0:1, cols], os_[at, 1:2, cols], 0))
            held = [[None, None], [None, None]]
            step = 4
            done = 0
            n_out = need_rows // 8
            while done < n_out:
                n = min(step, n_out - done)
                acc_re = acc_im = None
                for c in range(2):
                    moved = []
                    for x in range(2):
                        lo = 0 if done == 0 else done + 1
                        hi = done + n + 1
                        v = buf[c, x, t, 8 * lo : 8 * hi, :].reshape(hi - lo, 8, LANES)
                        seqs = joined(held[c][x], spun(sets[c], v))
                        held[c][x] = [seq[n : n + 1] for seq in seqs]
                        moved.append(mixed(sets[c], seqs, n, False))
                    spot = slice(8 * done, 8 * (done + n))
                    if g < slots:
                        fc, fs = f_main[c, g, 0, spot, cols], f_main[c, g, 1, spot, cols]
                    else:
                        fc, fs = f_strip[c, 0, spot, cols], f_strip[c, 1, spot, cols]
                    fc, fs = fc.reshape(n, 8, LANES), fs.reshape(n, 8, LANES)
                    re = fc * moved[0] - fs * moved[1]
                    im = fs * moved[0] + fc * moved[1]
                    acc_re = re if acc_re is None else acc_re + re
                    acc_im = im if acc_im is None else acc_im + im
                ocols = slice(g * beams + t * LANES, g * beams + (t + 1) * LANES)
                out[0, 8 * done : 8 * (done + n), ocols] = acc_re.reshape(8 * n, LANES).astype(BF16)
                out[1, 8 * done : 8 * (done + n), ocols] = acc_im.reshape(8 * n, LANES).astype(BF16)
                done += n


def last_step(slots, cells, hf, x_in, v1, v2, o2, th2, e2, buf, put):
    rows_in = x_in.shape[1]
    beams = slots * SEG
    for q in list(range(0, slots, 2)) + list(range(1, slots, 2)):
        lhs = x_in[:, :, q * beams : (q + 1) * beams].reshape(2 * rows_in, beams)
        tile = slots * beams + q * SEG // LANES * LANES
        lhs2 = x_in[:, :, tile : tile + LANES].reshape(2 * rows_in, LANES)
        val = jnp.dot(lhs, v1[hf], preferred_element_type=F32) + jnp.dot(
            lhs2, v2[hf, q * SEG % LANES // SEG], preferred_element_type=F32
        )
        for x in range(2):
            for h in range(2):
                buf[q, x, h] = val[x * rows_in : (x + 1) * rows_in, h * LANES : (h + 1) * LANES]
    sets, turn = [], []
    rows2 = o2[hf]
    for h in range(2):
        cols = slice(h * LANES, (h + 1) * LANES)
        sets.append(shift_setup(rows2[0:1, cols], rows2[1:2, cols], HALO))
        cos_rows = th2[0, hf]
        sin_rows = th2[1, hf]
        turn.append(
            [
                [jnp.broadcast_to(cos_rows[q : q + 1, cols], (8, LANES))[None] for q in range(slots)],
                [jnp.broadcast_to(sin_rows[q : q + 1, cols], (8, LANES))[None] for q in range(slots)],
            ]
        )
    n_out = cells // 8
    held = [[None, None], [None, None]]
    done = 0
    step = 4
    while done < n_out:
        n = min(step, n_out - done)
        sum_re = sum_im = None
        for h in range(2):
            lo = 0 if done == 0 else done + 2
            hi = done + n + 2
            re = im = None
            for q in range(slots):
                a = buf[q, 0, h, 8 * lo : 8 * hi, :].reshape(hi - lo, 8, LANES)
                b = buf[q, 1, h, 8 * lo : 8 * hi, :].reshape(hi - lo, 8, LANES)
                tc, ts = turn[h][0][q], turn[h][1][q]
                pr_, pi_ = tc * a - ts * b, ts * a + tc * b
                re = pr_ if re is None else re + pr_
                im = pi_ if im is None else im + pi_
            moved = []
            for x, v in enumerate((re, im)):
                seqs = joined(held[h][x], spun(sets[h], v))
                held[h][x] = [seq[n : n + 2] for seq in seqs]
                moved.append(mixed(sets[h], seqs, n, True))
            sum_re = moved[0] if sum_re is None else sum_re + moved[0]
            sum_im = moved[1] if sum_im is None else sum_im + moved[1]
        at = pl.ds(pl.multiple_of(hf * LANES, LANES), LANES)
        ec = e2[0, 0, 0, 8 * done : 8 * (done + n), at].reshape(n, 8, LANES)
        es = e2[0, 0, 1, 8 * done : 8 * (done + n), at].reshape(n, 8, LANES)
        put(done, n, ec * sum_re - es * sum_im, es * sum_re + ec * sum_im)
        done += n


def levels_kernel(slots, xt, strip, got_c, got_d, w1, w2, ws, v1, v2, o2, e0, e1, e2, es0, es1, os_, th2, p_ref, out, x2, x0, x1, inter0, inter1, buf, flat):
    row, _ = tables_of(slots)
    total = 2 * slots
    cells = xt.shape[1]
    mains = xt.shape[2]
    for x in range(2):
        x0[x, EDGE : EDGE + cells, :mains] = xt[x]
        x0[x, EDGE : EDGE + cells, mains:] = strip[x]
    even = lax.axis_index("rng") % 2 == 0

    def place(right, left):
        for x in range(2):
            x0[x, :EDGE, :] = left[x]
            x0[x, EDGE + cells :, :] = right[x]

    @pl.when(even)
    def _():
        place(got_c, got_d)

    @pl.when(jnp.logical_not(even))
    def _():
        place(got_d, got_c)

    inter = (inter0, inter1)
    level_step(slots, total, cells, 0, x0, x1, inter, w1, w2, ws, e0, es0, p_ref, os_, row)
    level_step(slots, total, cells, 1, x1, x2, inter, w1, w2, ws, e1, es1, p_ref, os_, row)
    hf = 1 - lax.axis_index("aper")

    def put(done, n, re, im):
        flat[0, 8 * done : 8 * (done + n), :] = re.reshape(8 * n, LANES)
        flat[1, 8 * done : 8 * (done + n), :] = im.reshape(8 * n, LANES)

    last_step(slots, cells, hf, x2, v1, v2, o2, th2, e2, buf, put)
    for x in range(2):
        out[x] = flat[x].T.astype(BF16)


def own_half_kernel(slots, x2, v1, v2, o2, th2, e2, out, buf, flat):
    cells = out.shape[2]
    hf = lax.axis_index("aper")

    def put(done, n, re, im):
        flat[0, 8 * done : 8 * (done + n), :] = re.reshape(8 * n, LANES)
        flat[1, 8 * done : 8 * (done + n), :] = im.reshape(8 * n, LANES)

    last_step(slots, cells, hf, x2, v1, v2, o2, th2, e2, buf, put)
    for x in range(2):
        out[x] = flat[x].T


def swap_even(axis):
    n = lax.axis_size(axis)
    return [(i, i ^ 1) for i in range(n) if i ^ 1 < n]


def swap_odd(axis):
    n = lax.axis_size(axis)
    pairs = []
    for i in range(1, n - 1, 2):
        pairs += [(i, i + 1), (i + 1, i)]
    return pairs


def call(kernel, outs, args, scratch=(), sems=(), flops=0, specs=None):
    vm = pl.BlockSpec(memory_space=pltpu.VMEM)
    return pl.pallas_call(
        kernel,
        out_shape=[jax.ShapeDtypeStruct(s, d) for s, d in outs],
        in_specs=specs or [vm] * len(args),
        out_specs=[vm] * len(outs),
        scratch_shapes=[pltpu.VMEM(s, d) for s, d in scratch] + list(sems),
        compiler_params=pltpu.CompilerParams(vmem_limit_bytes=VMEM_LIMIT),
        cost_estimate=pl.CostEstimate(flops=flops, bytes_accessed=0, transcendentals=0),
    )(*args)


def fast_body(*args):
    slots, _, beams, cells = args[0].shape
    full = cells * lax.axis_size("rng")
    _, rows = tables_of(slots)
    m = (rows // 8 + LANES // EDGE - 1) // (LANES // EDGE) * 8
    msg = slots * 2 * EDGE + 2 * m
    lv_rows = [rows_of(cells, lv) for lv in range(LEVELS - 1)]
    tiles = beams // LANES
    subimages, beam_offsets, range_offsets, beam_taps, range_frac, _, phase_rate, final_phase = args
    (blank,) = call(blank_kernel, [((8, LANES), F32)], (), flops=COVER_FLOPS)
    out_a, out_b, params, bases = call(
        functools.partial(pack_kernel, slots),
        [((msg, LANES), BF16), ((msg, LANES), BF16), ((rows, beams), F32), ((2 * slots, beams), F32)],
        (blank,) + args,
        flops=1000,
    )
    got_a = lax.ppermute(out_a, "ang", swap_even("ang"))
    got_b = lax.ppermute(out_b, "ang", swap_odd("ang"))
    got_base = lax.ppermute(bases, "aper", swap_even("aper"))
    (xt,) = call(
        functools.partial(turn_mains_kernel, slots),
        [((2, cells, slots * beams), BF16)],
        (subimages,),
        flops=1_000_000,
    )
    strip, out_c, out_d = call(
        functools.partial(strip_kernel, slots),
        [((2, cells, beams), BF16)] + [((2, EDGE, (slots + 1) * beams), BF16)] * 2,
        (got_a, got_b, subimages, xt),
        scratch=[((2, beams, cells), BF16)],
        flops=1000,
    )
    got_c = lax.ppermute(out_c, "rng", swap_even("rng"))
    got_d = lax.ppermute(out_d, "rng", swap_odd("rng"))

    def main_tables(*refs):
        ins, outs = refs[:6], refs[6:]
        main_tables_kernel(slots, full, *ins, *outs[:5], outs[5:])

    w1, w2, v1, v2, o2, e0, e1, e2 = call(
        main_tables,
        [
            ((LEVELS - 1, 2, 2, beams, beams), BF16),
            ((LEVELS - 1, 2, slots, LANES, beams), BF16),
            ((tiles, beams, beams), BF16),
            ((tiles, LANES // SEG, LANES, beams), BF16),
            ((tiles, 8, beams), F32),
        ]
        + [((2, slots, 2, r, beams), F32) for r in lv_rows]
        + [((1, 1, 2, cells, beams), F32)],
        (params, beam_offsets, range_offsets, beam_taps, range_frac, phase_rate),
        flops=20_000_000,
    )

    def strip_tables(*refs):
        ins, outs, more = refs[:3], refs[6:], refs[3:6]
        strip_tables_kernel(slots, full, *ins, outs[0], outs[1:LEVELS], outs[LEVELS], *outs[LEVELS + 2 :])
        turn_tables(slots, *more, outs[LEVELS + 1])

    ws, es0, es1, os_, th2 = call(
        strip_tables,
        [((LEVELS - 1, 2, beams, beams), BF16)]
        + [((2, 2, r, beams), F32) for r in lv_rows]
        + [((2 * (LEVELS - 1), 8, beams), F32), ((2, tiles, slots, beams), F32)],
        (got_a, got_b, params, bases, got_base, final_phase),
        scratch=[((rows, LANES), F32), ((3, max(m, 8), LANES), F32)],
        flops=20_000_000,
    )
    wide = (slots + 1) * beams
    x_rows = cells + 2 * EDGE
    sent, x2 = call(
        functools.partial(levels_kernel, slots),
        [((2, LANES, cells), BF16), ((2, lv_rows[1], wide), BF16)],
        (xt, strip, got_c, got_d, w1, w2, ws, v1, v2, o2, e0, e1, e2, es0, es1, os_, th2, params),
        scratch=[
            ((2, x_rows, wide), BF16),
            ((2, lv_rows[0], wide), BF16),
            ((2, 2, tiles, x_rows, LANES), F32),
            ((2, 2, tiles, x_rows, LANES), F32),
            ((slots, 2, 2, lv_rows[1], LANES), F32),
            ((2, cells, LANES), F32),
        ],
        flops=200_000_000,
    )
    got = lax.ppermute(sent, "aper", swap_even("aper"))
    (mine,) = call(
        functools.partial(own_half_kernel, slots),
        [((2, LANES, cells), F32)],
        (x2, v1, v2, o2, th2, e2),
        scratch=[((slots, 2, 2, lv_rows[1], LANES), F32), ((2, cells, LANES), F32)],
        flops=20_000_000,
    )
    return (mine + got.astype(F32))[:, None]


def whole_body(*args):
    slots, _, beams, cells = args[0].shape
    fits = (
        lax.axis_size("aper") == 2
        and slots * SEG == beams
        and beams == 2 * LANES
        and cells == LANES
        and slots == 1 << LEVELS - 1
    )
    if not fits:
        return body(*args)
    return fast_body(*args)


def solution(mesh):
    in_specs = (
        P("aper", None, "ang", "rng"),
        P(None, None, None, "ang"),
        P(None, None, None, "ang"),
        P(None, None, None, None, "ang"),
        P(None, None, None, "ang"),
        P("aper", None, None, "ang"),
        P(None, None, "ang"),
        P(None, "ang"),
    )
    out_specs = P(None, "ang", "aper", "rng")
    return jax.shard_map(whole_body, mesh=mesh, in_specs=in_specs, out_specs=out_specs, check_vma=False)
```

```python
import functools
import math

import jax
import jax.numpy as jnp
from jax import lax
from jax.experimental import pallas as pl
from jax.experimental.pallas import tpu as pltpu
from jax.sharding import PartitionSpec as P

LEVELS = 3
TAPS = 4
HALO = 4


def with_halo(cells, sides, width):
    for axis, dim in sides:
        count = lax.axis_size(axis)
        ends = count - 1
        head = lax.slice_in_dim(cells, 0, width, axis=dim)
        tail = lax.slice_in_dim(cells, cells.shape[dim] - width, cells.shape[dim], axis=dim)
        cells = jnp.concatenate(
            [
                lax.ppermute(tail, axis, [(i, (i + 1) % count) for i in range(ends)]),
                cells,
                lax.ppermute(head, axis, [((i + 1) % count, i) for i in range(ends)]),
            ],
            axis=dim,
        )
    return cells


def partner_2(x, axis, stride):
    return lax.ppermute(x, axis, [(i, i ^ 1 << stride) for i in range(lax.axis_size(axis))])


def block_edges(blocks):
    return with_halo(blocks, (("ang", 2), ("rng", 3)), HALO)


def band_matrices(offsets, tap_weights):
    beam_count = offsets.shape[1]
    columns = jnp.arange(beam_count + 2 * HALO, dtype=jnp.int32)
    row_ids = jnp.arange(beam_count, dtype=jnp.int32)
    starting = row_ids[None, :] + HALO + offsets
    lagging = columns[None, None, :] - starting[:, :, None]
    weights = jnp.zeros(lagging.shape, jnp.float32)
    for tap_idx in range(TAPS):
        weights = weights + jnp.where(
            lagging == tap_idx, tap_weights[:, tap_idx, :, None].astype(jnp.float32), 0.0
        )
    return weights.astype(jnp.bfloat16)


def merge_level(child_blocks, halves, level_idx, tables, range_ramp):
    beam_offsets, range_offsets, beam_taps, range_frac, phase_base, phase_rate = tables
    slot_count = halves.shape[0]
    cell_count = range_ramp.shape[0]
    slot_ids = jnp.arange(slot_count, dtype=jnp.int32)
    summed = None
    for side_idx in range(2):
        child_ids = halves if side_idx == 0 else 1 - halves
        extended = child_blocks[side_idx]
        matrices = band_matrices(
            beam_offsets[level_idx][child_ids, halves], beam_taps[level_idx][child_ids, halves]
        )
        interpolated = jnp.einsum(
            "snm,sxmr->sxnr", matrices, extended, preferred_element_type=jnp.float32
        )
        range_shift = range_offsets[level_idx][child_ids, halves] + HALO
        fraction = range_frac[level_idx][child_ids, halves]
        shifted = jnp.zeros(interpolated.shape[:3] + (cell_count,), jnp.float32)
        for offset_step in range(2 * HALO + 1):
            weight = jnp.where(range_shift == offset_step, 1.0 - fraction, 0.0) + jnp.where(
                range_shift + 1 == offset_step, fraction, 0.0
            )
            shifted = (
                shifted
                + weight[:, None, :, None]
                * interpolated[:, :, :, offset_step : offset_step + cell_count]
            )
        angles = (
            phase_base[slot_ids, level_idx, child_ids][:, :, None]
            + phase_rate[level_idx][child_ids][:, :, None] * range_ramp[None, None, :]
        )
        cosine = jnp.cos(angles)
        sine_part = jnp.sin(angles)
        term = jnp.stack(
            [
                cosine * shifted[:, 0] - sine_part * shifted[:, 1],
                sine_part * shifted[:, 0] + cosine * shifted[:, 1],
            ],
            axis=1,
        )
        summed = term if summed is None else summed + term
    return summed.astype(jnp.bfloat16)


def body(
    subimages,
    beam_offsets,
    range_offsets,
    beam_taps,
    range_frac,
    phase_base,
    phase_rate,
    final_phase,
):
    slot_count = subimages.shape[0]
    beam_count = subimages.shape[2]
    cell_count = subimages.shape[3]
    aper_count = lax.axis_size("aper")
    total_subs = slot_count * aper_count
    aper_pos = lax.axis_index("aper")
    full_range = cell_count * lax.axis_size("rng")
    range_ramp = (
        lax.axis_index("rng") * cell_count + jnp.arange(cell_count, dtype=jnp.int32)
    ).astype(jnp.float32) / full_range - 0.5
    tables = (beam_offsets, range_offsets, beam_taps, range_frac, phase_base, phase_rate)
    sub_ids = aper_pos * slot_count + jnp.arange(slot_count, dtype=jnp.int32)
    current = subimages
    for level_idx in range(LEVELS):
        distance = total_subs >> LEVELS - level_idx
        halves = sub_ids // distance % 2
        if distance >= slot_count:
            which_bit = (distance // slot_count).bit_length() - 1
            partner = partner_2(current, "aper", which_bit)
            joined = block_edges(jnp.concatenate([current, partner], 0))
            own_block = joined[:slot_count]
            other_block = joined[slot_count:]
        else:
            own_block = block_edges(current)
            block_shape = own_block.shape
            paired = own_block.reshape(
                (slot_count // (2 * distance), 2, distance) + block_shape[1:]
            )
            other_block = paired[:, ::-1].reshape(block_shape)
        current = merge_level((own_block, other_block), halves, level_idx, tables, range_ramp)
    scale = 1.0 / math.sqrt(total_subs)
    sector = beam_count // aper_count
    regrouped = lax.all_to_all(current[:, None], "aper", split_axis=3, concat_axis=1, tiled=True)
    angles = lax.dynamic_slice_in_dim(final_phase, aper_pos * sector, sector, 1)
    angles = angles.reshape(aper_count, slot_count, sector).transpose(1, 0, 2)
    cosine = jnp.cos(angles)[:, :, :, None]
    sine_part = jnp.sin(angles)[:, :, :, None]
    real_part = regrouped[:, :, 0].astype(jnp.float32)
    imag_part = regrouped[:, :, 1].astype(jnp.float32)
    summed = jnp.stack(
        [
            jnp.sum(cosine * real_part - sine_part * imag_part, axis=(0, 1)),
            jnp.sum(sine_part * real_part + cosine * imag_part, axis=(0, 1)),
        ]
    )
    image = summed * scale
    return image[:, None]


F32 = jnp.float32
BF16 = jnp.bfloat16
LANES = 128
EDGE = -(-HALO * LEVELS // 16) * 16
SEG = 4 * EDGE
FIELDS = 3 + TAPS
VMEM_LIMIT = 24 * 1024 * 1024
COVER_FLOPS = 2_000_000_000


def tables_of(slots):
    row = {}
    for lv in range(LEVELS - 1):
        for c in range(2):
            for h in range(2):
                for k in range(FIELDS):
                    row["p", lv, c, h, k] = len(row)
    for s in range(slots):
        for lv in range(LEVELS - 1):
            for c in range(2):
                row["b", s, lv, c] = len(row)
    for lv in range(LEVELS - 1):
        for c in range(2):
            row["r", lv, c] = len(row)
    return row, -(-len(row) // 8) * 8


def half_of(lv, s, total):
    return s // (total >> LEVELS - lv) % 2


def child_of(lv, s, c, total):
    d = total >> LEVELS - lv
    return s - half_of(lv, s, total) * d + c * d


def roll_lanes(x, shift):
    return pltpu.roll(x, shift % LANES, x.ndim - 1) if shift % LANES else x


def iota(shape, dim):
    return lax.broadcasted_iota(jnp.int32, shape, dim)


def blank_kernel(out):
    out[...] = jnp.zeros_like(out)


def pack_kernel(slots, blank, sub, bo, ro, bt, rf, pb, pr, fp, out_a, out_b, p_ref, base_ref):
    row, rows = tables_of(slots)
    beams = p_ref.shape[1]
    for t in range(beams // LANES):
        p_ref[rows - 8 :, t * LANES : (t + 1) * LANES] = blank[...]
    for lv in range(LEVELS - 1):
        for c in range(2):
            for h in range(2):
                at = row["p", lv, c, h, 0]
                p_ref[at : at + 1] = bo[lv, c, h : h + 1, :].astype(F32)
                p_ref[at + 1 : at + 2] = (ro[lv, c, h : h + 1, :] + HALO).astype(F32)
                p_ref[at + 2 : at + 3] = rf[lv, c, h : h + 1, :]
                p_ref[at + 3 : at + 3 + TAPS] = bt[lv, c, h].astype(F32)
            at = row["r", lv, c]
            p_ref[at : at + 1] = pr[lv, c : c + 1, :]
            for s in range(slots):
                at = row["b", s, lv, c]
                p_ref[at : at + 1] = pb[s, lv, c : c + 1, :]
    for c in range(2):
        for s in range(slots):
            base_ref[c * slots + s : c * slots + s + 1] = pb[s, LEVELS - 1, c : c + 1, :]

    per = LANES // EDGE
    beams = p_ref.shape[1]
    lane = iota((8, LANES), 1) // EDGE

    def packed(tile, start):
        parts = []
        for first in range(0, rows // 8, per):
            total = jnp.zeros((8, LANES), F32)
            for g in range(first, min(first + per, rows // 8)):
                piece = p_ref[8 * g : 8 * g + 8, tile : tile + LANES]
                spot = (g - first) * EDGE
                total = jnp.where(lane == g - first, roll_lanes(piece, spot - start), total)
            parts.append(total)
        x = jnp.concatenate(parts, 0)
        high = x.astype(BF16)
        return high, (x - high.astype(F32)).astype(BF16)

    def fill(out, first, tile, start):
        n = slots * 2 * EDGE
        out[:n] = sub[:, :, first : first + EDGE].reshape(n, LANES)
        high, low = packed(tile, start)
        m = high.shape[0]
        out[n : n + m] = high
        out[n + m : n + 2 * m] = low

    even = lax.axis_index("ang") % 2 == 0

    @pl.when(even)
    def _():
        fill(out_a, beams - EDGE, beams - LANES, LANES - EDGE)
        fill(out_b, 0, 0, 0)

    @pl.when(jnp.logical_not(even))
    def _():
        fill(out_a, 0, 0, 0)
        fill(out_b, beams - EDGE, beams - LANES, LANES - EDGE)


def turned(x):
    return x.astype(F32).T.astype(BF16)


def sincos(x):
    k = jnp.floor(x * (2.0 / math.pi) + 0.5)
    r = x - k * 1.5703125
    r = r - k * 4.838267948966e-4
    q = k.astype(jnp.int32)
    z = r * r
    s = r + r * z * (-1.6666654611e-1 + z * (8.3321608736e-3 + z * -1.9515295891e-4))
    c = 1.0 - 0.5 * z + z * z * (4.166664568298827e-2 + z * (-1.388731625493765e-3 + z * 2.443315711809948e-5))
    odd = q % 2 != 0
    sin, cos = jnp.where(odd, c, s), jnp.where(odd, s, c)
    q = q % 4
    return jnp.where(q >= 2, -sin, sin), jnp.where((q == 1) | (q == 2), -cos, cos)


def band(lag, taps):
    out = jnp.zeros(lag.shape, F32)
    for t in range(TAPS):
        out = jnp.where(lag == t, taps[t], out)
    return out.astype(BF16)


def phasors(rate, first, delta, count, low, high, lead, cells, turns, store):
    n = rate.shape[1]
    r8 = iota((8, n), 0)
    small = rate * (r8.astype(F32) * delta)
    other = jnp.where(r8 == 0, rate * (8 * delta), rate * first)
    ss, cs = sincos(small)
    so, co = sincos(other)
    cu, su = co[1:2], so[1:2]
    ck, sk = jnp.broadcast_to(co[0:1], (8, n)), jnp.broadcast_to(so[0:1], (8, n))
    base_re = cs * cu - ss * su
    base_im = ss * cu + cs * su
    for at, turn in enumerate(turns):
        re, im = base_re, base_im
        if turn is not None:
            ct, st = turn
            re, im = re * ct - im * st, im * ct + re * st
        for j in range(count):
            if 8 * j < lead or 8 * j + 8 > lead + cells:
                ids = r8 + 8 * j
                keep = jnp.logical_and(ids >= low, ids < high)
                store(at, j, jnp.where(keep, re, 0.0), jnp.where(keep, im, 0.0))
            else:
                store(at, j, re, im)
            if j + 1 < count:
                re, im = re * ck - im * sk, im * ck + re * sk


def range_place(cells, lv, full):
    lead = (EDGE - HALO * (lv + 1)) if lv < LEVELS - 1 else 0
    at = lax.axis_index("rng") * cells - lead
    first = at.astype(F32) / full - 0.5
    return first, -at, full - at, lead


def rows_of(cells, lv):
    need = cells + 2 * (EDGE - HALO * (lv + 1))
    return -(-need // 16) * 16


def turn_mains_kernel(slots, sub, xt):
    beams = sub.shape[2]
    for s in range(slots):
        for x in range(2):
            xt[x, :, s * beams : (s + 1) * beams] = turned(sub[s, x])


def main_tables_kernel(slots, full, p_ref, bo, ro, bt, rf, pr, w1, w2, v1, v2, o2, f_refs):
    row, _ = tables_of(slots)
    total = 2 * slots
    beams = p_ref.shape[1]
    cells = LANES
    tiles = beams // LANES

    w1[...] = jnp.zeros_like(w1)
    w2[...] = jnp.zeros_like(w2)
    v1[...] = jnp.zeros_like(v1)
    v2[...] = jnp.zeros_like(v2)
    own = lax.axis_index("aper")

    def main_band(first_col, off, taps, put):
        low = max(first_col - 16, 0)
        top = min(first_col + LANES + 16, beams)
        m = iota((top - low, LANES), 0) + low
        p = iota((top - low, LANES), 1) + first_col
        put(low, top, band(m - p - off, taps))

    def strip_band(first_col, off, taps, put):
        if first_col + LANES == beams:
            m = iota((EDGE, LANES), 0) + beams
            put(EDGE, band(m - (iota((EDGE, LANES), 1) + first_col) - off, taps))
        if first_col == 0:
            m = iota((EDGE, LANES), 0) - EDGE
            put(2 * EDGE, band(m - iota((EDGE, LANES), 1) - off, taps))

    for lv in range(LEVELS - 1):
        for c in range(2):
            for h in range(2):
                for t in range(tiles):
                    cols = slice(t * LANES, (t + 1) * LANES)
                    at = row["p", lv, c, h, 0]
                    off = p_ref[at : at + 1, cols].astype(jnp.int32)
                    taps = [p_ref[at + 3 + k : at + 4 + k, cols] for k in range(TAPS)]

                    def put(low, top, v):
                        w1[lv, c, h, low:top, cols] = v

                    main_band(t * LANES, off, taps, put)

                    def put(at_row, v):
                        for s in range(slots):
                            if half_of(lv, s, total) == h:
                                base = child_of(lv, s, c, total) * SEG % LANES + at_row
                                w2[lv, c, s, base : base + EDGE, cols] = v

                    strip_band(t * LANES, off, taps, put)
    lv = LEVELS - 1
    for h in range(2):
        for t in range(tiles):
            cols = slice(t * LANES, (t + 1) * LANES)
            outs = slice(h * LANES, (h + 1) * LANES)
            off = bo[lv, own, h : h + 1, cols]
            tap_rows = bt[lv, own, h, :, cols].astype(F32)
            taps = [tap_rows[k : k + 1] for k in range(TAPS)]

            def put(low, top, v):
                v1[t, low:top, outs] = v

            main_band(t * LANES, off, taps, put)

            def put(at_row, v):
                for par in range(LANES // SEG):
                    base = par * SEG + at_row
                    v2[t, par, base : base + EDGE, outs] = v

            strip_band(t * LANES, off, taps, put)
            o2[t, 0:1, outs] = (ro[lv, own, h : h + 1, cols] + HALO).astype(F32)
            o2[t, 1:2, outs] = rf[lv, own, h : h + 1, cols]

    at = row["b", 0, 0, 0]
    sin_all, cos_all = sincos(p_ref[at : at + slots * (LEVELS - 1) * 2, :])
    for lv in range(LEVELS):
        first, low, high, lead = range_place(cells, lv, full)
        count = (cells + 2 * lead) // 8
        for c in range(2 if lv < LEVELS - 1 else 1):
            turns = [None]
            if lv < LEVELS - 1:
                at = row["r", lv, c]
                rate = p_ref[at : at + 1, :]
                spots = [row["b", s, lv, c] - row["b", 0, 0, 0] for s in range(slots)]
                turns = [(cos_all[k : k + 1], sin_all[k : k + 1]) for k in spots]
            else:
                rate = jnp.where(own == 0, pr[lv, 0:1, :], pr[lv, 1:2, :])

            def store(g, j, re, im):
                f_refs[lv][c, g, 0, 8 * j : 8 * j + 8, :] = re
                f_refs[lv][c, g, 1, 8 * j : 8 * j + 8, :] = im

            phasors(rate, first, 1.0 / full, count, low, high, lead, cells, turns, store)


def strip_kernel(slots, got_a, got_b, sub, xt, strip, out_c, out_d, nat):
    beams = slots * SEG
    even = lax.axis_index("ang") % 2 == 0

    def place(right, left):
        for s in range(slots):
            for x in range(2):
                at = (s * 2 + x) * EDGE
                nat[x, s * SEG + EDGE : s * SEG + 2 * EDGE] = right[at : at + EDGE]
                nat[x, s * SEG + 2 * EDGE : s * SEG + 3 * EDGE] = left[at : at + EDGE]

    for s in range(slots):
        for x in range(2):
            nat[x, s * SEG : s * SEG + EDGE] = sub[s, x, beams - EDGE :]
            nat[x, s * SEG + 3 * EDGE : (s + 1) * SEG] = sub[s, x, :EDGE]

    @pl.when(even)
    def _():
        place(got_a, got_b)

    @pl.when(jnp.logical_not(even))
    def _():
        place(got_b, got_a)

    for x in range(2):
        strip[x] = turned(nat[x])
    cells = strip.shape[1]
    mains = xt.shape[2]

    def send(first, last):
        for x in range(2):
            first[x, :, :mains] = xt[x, cells - EDGE :, :]
            first[x, :, mains:] = strip[x, cells - EDGE :, :]
            last[x, :, :mains] = xt[x, :EDGE, :]
            last[x, :, mains:] = strip[x, :EDGE, :]

    even_r = lax.axis_index("rng") % 2 == 0

    @pl.when(even_r)
    def _():
        send(out_c, out_d)

    @pl.when(jnp.logical_not(even_r))
    def _():
        send(out_d, out_c)


def strip_tables_kernel(slots, full, got_a, got_b, p_ref, ws, fs_refs, os_, seg, halo):
    row, rows = tables_of(slots)
    total = 2 * slots
    cells = LANES
    beams = p_ref.shape[1]
    per = LANES // EDGE
    n = slots * 2 * EDGE
    m = (rows // 8 + per - 1) // per * 8
    even = lax.axis_index("ang") % 2 == 0

    def load(right, left):
        halo[0] = right[n : n + m].astype(F32) + right[n + m : n + 2 * m].astype(F32)
        halo[1] = left[n : n + m].astype(F32) + left[n + m : n + 2 * m].astype(F32)

    @pl.when(even)
    def _():
        load(got_a, got_b)

    @pl.when(jnp.logical_not(even))
    def _():
        load(got_b, got_a)

    lane = iota((8, LANES), 1)
    piece_of = lane % SEG // EDGE
    for g in range(rows // 8):
        at = g // per * 8
        spot = g % per * EDGE
        parts = [
            roll_lanes(p_ref[8 * g : 8 * g + 8, beams - LANES :], EDGE - LANES),
            roll_lanes(halo[0, at : at + 8, :], EDGE - spot),
            roll_lanes(halo[1, at : at + 8, :], 2 * EDGE - spot),
            roll_lanes(p_ref[8 * g : 8 * g + 8, :LANES], 3 * EDGE),
        ]
        out = parts[0]
        for k in range(1, 4):
            out = jnp.where(piece_of == k, parts[k], out)
        twice = jnp.where(lane < SEG, out, roll_lanes(out, SEG))
        seg[8 * g : 8 * g + 8, :] = twice

    first_seg = iota((1, LANES), 1) < SEG

    def pick(r0, r1):
        if r0 == r1:
            return seg[r0 : r0 + 1, :]
        return jnp.where(first_seg, seg[r0 : r0 + 1, :], seg[r1 : r1 + 1, :])

    def beam_of(i):
        j = i % SEG
        return jnp.where(j < 2 * EDGE, beams - EDGE + j, j - 3 * EDGE)

    for lv in range(LEVELS - 1):
        first, low, high, lead = range_place(cells, lv, full)
        for c in range(2):
            for t in range(beams // LANES):
                cols = slice(t * LANES, (t + 1) * LANES)
                s0, s1 = 2 * t, 2 * t + 1
                h0, h1 = half_of(lv, s0, total), half_of(lv, s1, total)
                k0, k1 = child_of(lv, s0, c, total), child_of(lv, s1, c, total)
                field = [pick(row["p", lv, c, h0, k], row["p", lv, c, h1, k]) for k in range(FIELDS)]
                at = lv * 2 + c
                os_[at, 0:1, cols] = field[1]
                os_[at, 1:2, cols] = field[2]
                i_row = iota((beams, LANES), 0)
                col = iota((1, LANES), 1)
                wanted = jnp.where(col < SEG, k0, k1)
                lag = beam_of(i_row) - beam_of(col) - field[0].astype(jnp.int32)
                lag = jnp.where(i_row // SEG == wanted, lag, -1)
                ws[lv, c, :, cols] = band(lag, field[3:])
                halo[2, at * 2 + t : at * 2 + t + 1, :] = pick(row["b", s0, lv, c], row["b", s1, lv, c])
    tiles = beams // LANES
    sin_all, cos_all = sincos(halo[2, : 2 * tiles * (LEVELS - 1)])
    for lv in range(LEVELS - 1):
        first, low, high, lead = range_place(cells, lv, full)
        for c in range(2):
            rate = pick(row["r", lv, c], row["r", lv, c])
            at = (lv * 2 + c) * tiles
            turns = [(cos_all[at + t : at + t + 1], sin_all[at + t : at + t + 1]) for t in range(tiles)]

            def store(t, j, re, im):
                cols = slice(t * LANES, (t + 1) * LANES)
                fs_refs[lv][c, 0, 8 * j : 8 * j + 8, cols] = re
                fs_refs[lv][c, 1, 8 * j : 8 * j + 8, cols] = im

            phasors(rate, first, 1.0 / full, (cells + 2 * lead) // 8, low, high, lead, cells, turns, store)


def turn_tables(slots, base_ref, got_base, fp, th2):
    total = 2 * slots
    beams = fp.shape[1]
    own = lax.axis_index("aper")
    scale = 1.0 / math.sqrt(total)
    for h in range(2):
        for t in range(beams // LANES):
            cols = slice(t * LANES, (t + 1) * LANES)
            here = jnp.where(own == 0, base_ref[:slots, cols], base_ref[slots:, cols])
            there = jnp.where(own == 0, got_base[:slots, cols], got_base[slots:, cols])
            angles = jnp.where(own == h, here, there) + fp[h * slots : (h + 1) * slots, cols]
            th2[0, t, :, h * LANES : (h + 1) * LANES] = jnp.cos(angles) * scale
            th2[1, t, :, h * LANES : (h + 1) * LANES] = jnp.sin(angles) * scale


def shift_setup(o_row, f_row, extra):
    shift = o_row.astype(jnp.int32) + extra
    sub = iota((8, LANES), 0)
    reach = sub + shift
    ahead = reach + 1
    return dict(
        one=jnp.broadcast_to(1.0 - f_row, (8, LANES)),
        two=jnp.broadcast_to(f_row, (8, LANES)),
        pick=(reach % 8, ahead % 8),
        tier=((reach < 8, reach < 16), (ahead < 8, ahead < 16)),
    )


def spun(setup, v):
    return [
        jnp.stack([jnp.take_along_axis(v[i], index, axis=0, mode="promise_in_bounds") for i in range(v.shape[0])])
        for index in setup["pick"]
    ]


def mixed(setup, seqs, n, wide):
    parts = []
    for seq, (in0, in1) in zip(seqs, setup["tier"]):
        rest = seq[1 : n + 1]
        if wide:
            rest = jnp.where(in1[None], rest, seq[2 : n + 2])
        parts.append(jnp.where(in0[None], seq[:n], rest))
    return setup["one"][None] * parts[0] + setup["two"][None] * parts[1]


def joined(held, new):
    return new if held is None else [jnp.concatenate([a, b], 0) for a, b in zip(held, new)]


def level_step(slots, total, lv, x_in, spans, tile_at, out, inter, w1, w2, ws, f_main, f_strip, o_main, os_, row):
    beams = slots * SEG
    rows_in = x_in(0, LANES).shape[1]
    order = [slots] + list(range(0, slots, 2)) + list(range(1, slots, 2))
    for turn, g in enumerate(order):
        buf = inter[turn % 2]
        for c in range(2):
            if g < slots:
                k = child_of(lv, g, c, total)
                h = half_of(lv, g, total)
                lhs = x_in(k * beams, beams).reshape(2 * rows_in, beams)
                tile = slots * beams + k * SEG // LANES * LANES
                lhs2 = x_in(tile, LANES).reshape(2 * rows_in, LANES)
                val = jnp.dot(lhs, w1[lv, c, h], preferred_element_type=F32) + jnp.dot(
                    lhs2, w2[lv, c, g], preferred_element_type=F32
                )
            else:
                lhs = x_in(slots * beams, beams).reshape(2 * rows_in, beams)
                val = jnp.dot(lhs, ws[lv, c], preferred_element_type=F32)
            for x in range(2):
                for t in range(beams // LANES):
                    buf[c, x, t, :rows_in, :] = val[x * rows_in : (x + 1) * rows_in, t * LANES : (t + 1) * LANES]
        for t in range(beams // LANES):
            cols = slice(t * LANES, (t + 1) * LANES)
            sets = []
            for c in range(2):
                if g < slots:
                    at = row["p", lv, c, half_of(lv, g, total), 0]
                    sets.append(shift_setup(o_main[at + 1 : at + 2, cols], o_main[at + 2 : at + 3, cols], 0))
                else:
                    at = lv * 2 + c
                    sets.append(shift_setup(os_[at, 0:1, cols], os_[at, 1:2, cols], 0))
            for t0, t1 in spans:
                held = [[None, None], [None, None]]
                step = 4
                done = t0
                while done < t1:
                    n = min(step, t1 - done)
                    acc_re = acc_im = None
                    for c in range(2):
                        moved = []
                        for x in range(2):
                            lo = done if done == t0 else done + 1
                            hi = done + n + 1
                            v = buf[c, x, t, 8 * tile_at(lo) : 8 * (tile_at(hi - 1) + 1), :].reshape(hi - lo, 8, LANES)
                            seqs = joined(held[c][x], spun(sets[c], v))
                            held[c][x] = [seq[n : n + 1] for seq in seqs]
                            moved.append(mixed(sets[c], seqs, n, False))
                        spot = slice(8 * done, 8 * (done + n))
                        if g < slots:
                            fc, fs = f_main[c, g, 0, spot, cols], f_main[c, g, 1, spot, cols]
                        else:
                            fc, fs = f_strip[c, 0, spot, cols], f_strip[c, 1, spot, cols]
                        fc, fs = fc.reshape(n, 8, LANES), fs.reshape(n, 8, LANES)
                        re = fc * moved[0] - fs * moved[1]
                        im = fs * moved[0] + fc * moved[1]
                        acc_re = re if acc_re is None else acc_re + re
                        acc_im = im if acc_im is None else acc_im + im
                    ocols = slice(g * beams + t * LANES, g * beams + (t + 1) * LANES)
                    out[0, 8 * done : 8 * (done + n), ocols] = acc_re.reshape(8 * n, LANES).astype(BF16)
                    out[1, 8 * done : 8 * (done + n), ocols] = acc_im.reshape(8 * n, LANES).astype(BF16)
                    done += n


def last_step(slots, cells, hf, x_in, v1, v2, o2, th2, e2, buf, put):
    rows_in = x_in.shape[1]
    beams = slots * SEG
    for q in list(range(0, slots, 2)) + list(range(1, slots, 2)):
        lhs = x_in[:, :, q * beams : (q + 1) * beams].reshape(2 * rows_in, beams)
        tile = slots * beams + q * SEG // LANES * LANES
        lhs2 = x_in[:, :, tile : tile + LANES].reshape(2 * rows_in, LANES)
        val = jnp.dot(lhs, v1[hf], preferred_element_type=F32) + jnp.dot(
            lhs2, v2[hf, q * SEG % LANES // SEG], preferred_element_type=F32
        )
        for x in range(2):
            for h in range(2):
                buf[q, x, h] = val[x * rows_in : (x + 1) * rows_in, h * LANES : (h + 1) * LANES]
    sets, turn = [], []
    rows2 = o2[hf]
    for h in range(2):
        cols = slice(h * LANES, (h + 1) * LANES)
        sets.append(shift_setup(rows2[0:1, cols], rows2[1:2, cols], HALO))
        cos_rows = th2[0, hf]
        sin_rows = th2[1, hf]
        turn.append(
            [
                [jnp.broadcast_to(cos_rows[q : q + 1, cols], (8, LANES))[None] for q in range(slots)],
                [jnp.broadcast_to(sin_rows[q : q + 1, cols], (8, LANES))[None] for q in range(slots)],
            ]
        )
    n_out = cells // 8
    held = [[None, None], [None, None]]
    done = 0
    step = 4
    while done < n_out:
        n = min(step, n_out - done)
        sum_re = sum_im = None
        for h in range(2):
            lo = 0 if done == 0 else done + 2
            hi = done + n + 2
            re = im = None
            for q in range(slots):
                a = buf[q, 0, h, 8 * lo : 8 * hi, :].reshape(hi - lo, 8, LANES)
                b = buf[q, 1, h, 8 * lo : 8 * hi, :].reshape(hi - lo, 8, LANES)
                tc, ts = turn[h][0][q], turn[h][1][q]
                pr_, pi_ = tc * a - ts * b, ts * a + tc * b
                re = pr_ if re is None else re + pr_
                im = pi_ if im is None else im + pi_
            moved = []
            for x, v in enumerate((re, im)):
                seqs = joined(held[h][x], spun(sets[h], v))
                held[h][x] = [seq[n : n + 2] for seq in seqs]
                moved.append(mixed(sets[h], seqs, n, True))
            sum_re = moved[0] if sum_re is None else sum_re + moved[0]
            sum_im = moved[1] if sum_im is None else sum_im + moved[1]
        at = pl.ds(pl.multiple_of(hf * LANES, LANES), LANES)
        ec = e2[0, 0, 0, 8 * done : 8 * (done + n), at].reshape(n, 8, LANES)
        es = e2[0, 0, 1, 8 * done : 8 * (done + n), at].reshape(n, 8, LANES)
        put(done, n, ec * sum_re - es * sum_im, es * sum_re + ec * sum_im)
        done += n


def inner_rows(cells):
    return 2 * EDGE // 16, cells // 8


def interior_kernel(slots, xt, strip, w1, w2, ws, e0, es0, os_, p_ref, x1, inter0, inter1):
    row, _ = tables_of(slots)
    mains = xt.shape[2]
    low, top = inner_rows(xt.shape[1])

    def get(lane, width):
        return xt[:, :, lane : lane + width] if lane < mains else strip[:, :, lane - mains : lane - mains + width]

    level_step(slots, 2 * slots, 0, get, [(low, top)], lambda v: v - low, x1, (inter0, inter1), w1, w2, ws, e0, es0, p_ref, os_, row)


def levels_kernel(slots, xt, strip, got_c, got_d, inner, w1, w2, ws, v1, v2, o2, e0, e1, e2, es0, es1, os_, th2, p_ref, out, x2, x0, x1, inter0, inter1, buf, flat):
    row, _ = tables_of(slots)
    total = 2 * slots
    cells = xt.shape[1]
    mains = xt.shape[2]
    low, top = inner_rows(cells)
    for x in range(2):
        for at, spot in ((EDGE, slice(0, EDGE)), (2 * EDGE, slice(cells - EDGE, cells))):
            x0[x, at : at + EDGE, :mains] = xt[x, spot]
            x0[x, at : at + EDGE, mains:] = strip[x, spot]
        x1[x, 8 * low : 8 * top] = inner[x, 8 * low : 8 * top]
    even = lax.axis_index("rng") % 2 == 0

    def place(right, left):
        for x in range(2):
            x0[x, :EDGE, :] = left[x]
            x0[x, 3 * EDGE :, :] = right[x]

    @pl.when(even)
    def _():
        place(got_c, got_d)

    @pl.when(jnp.logical_not(even))
    def _():
        place(got_d, got_c)

    inter = (inter0, inter1)
    edge_tiles = EDGE // 4
    spans = [(0, low), (top, (cells + 2 * (EDGE - HALO)) // 8)]
    level_step(slots, total, 0, lambda lane, width: x0[:, :, lane : lane + width], spans, lambda v: v if v < edge_tiles else v - (cells + 2 * EDGE) // 8 + 2 * edge_tiles, x1, inter, w1, w2, ws, e0, es0, p_ref, os_, row)
    level_step(slots, total, 1, lambda lane, width: x1[:, :, lane : lane + width], [(0, x2.shape[1] // 8)], lambda v: v, x2, inter, w1, w2, ws, e1, es1, p_ref, os_, row)
    hf = 1 - lax.axis_index("aper")

    def put(done, n, re, im):
        flat[0, 8 * done : 8 * (done + n), :] = re.reshape(8 * n, LANES)
        flat[1, 8 * done : 8 * (done + n), :] = im.reshape(8 * n, LANES)

    last_step(slots, cells, hf, x2, v1, v2, o2, th2, e2, buf, put)
    for x in range(2):
        out[x] = flat[x].T.astype(BF16)


def own_half_kernel(slots, x2, v1, v2, o2, th2, e2, out, buf, flat):
    cells = out.shape[2]
    hf = lax.axis_index("aper")

    def put(done, n, re, im):
        flat[0, 8 * done : 8 * (done + n), :] = re.reshape(8 * n, LANES)
        flat[1, 8 * done : 8 * (done + n), :] = im.reshape(8 * n, LANES)

    last_step(slots, cells, hf, x2, v1, v2, o2, th2, e2, buf, put)
    for x in range(2):
        out[x] = flat[x].T


def swap_even(axis):
    n = lax.axis_size(axis)
    return [(i, i ^ 1) for i in range(n) if i ^ 1 < n]


def swap_odd(axis):
    n = lax.axis_size(axis)
    pairs = []
    for i in range(1, n - 1, 2):
        pairs += [(i, i + 1), (i + 1, i)]
    return pairs


def call(kernel, outs, args, scratch=(), sems=(), flops=0, specs=None):
    vm = pl.BlockSpec(memory_space=pltpu.VMEM)
    return pl.pallas_call(
        kernel,
        out_shape=[jax.ShapeDtypeStruct(s, d) for s, d in outs],
        in_specs=specs or [vm] * len(args),
        out_specs=[vm] * len(outs),
        scratch_shapes=[pltpu.VMEM(s, d) for s, d in scratch] + list(sems),
        compiler_params=pltpu.CompilerParams(vmem_limit_bytes=VMEM_LIMIT),
        cost_estimate=pl.CostEstimate(flops=flops, bytes_accessed=0, transcendentals=0),
    )(*args)


def fast_body(*args):
    slots, _, beams, cells = args[0].shape
    full = cells * lax.axis_size("rng")
    _, rows = tables_of(slots)
    m = (rows // 8 + LANES // EDGE - 1) // (LANES // EDGE) * 8
    msg = slots * 2 * EDGE + 2 * m
    lv_rows = [rows_of(cells, lv) for lv in range(LEVELS - 1)]
    tiles = beams // LANES
    subimages, beam_offsets, range_offsets, beam_taps, range_frac, _, phase_rate, final_phase = args
    (blank,) = call(blank_kernel, [((8, LANES), F32)], (), flops=COVER_FLOPS)
    out_a, out_b, params, bases = call(
        functools.partial(pack_kernel, slots),
        [((msg, LANES), BF16), ((msg, LANES), BF16), ((rows, beams), F32), ((2 * slots, beams), F32)],
        (blank,) + args,
        flops=1000,
    )
    got_a = lax.ppermute(out_a, "ang", swap_even("ang"))
    got_b = lax.ppermute(out_b, "ang", swap_odd("ang"))
    got_base = lax.ppermute(bases, "aper", swap_even("aper"))

    def main_tables(*refs):
        ins, xt, outs = refs[1:7], refs[7], refs[8:]
        turn_mains_kernel(slots, refs[0], xt)
        main_tables_kernel(slots, full, *ins, *outs[:5], outs[5:])

    xt, w1, w2, v1, v2, o2, e0, e1, e2 = call(
        main_tables,
        [
            ((2, cells, slots * beams), BF16),
            ((LEVELS - 1, 2, 2, beams, beams), BF16),
            ((LEVELS - 1, 2, slots, LANES, beams), BF16),
            ((tiles, beams, beams), BF16),
            ((tiles, LANES // SEG, LANES, beams), BF16),
            ((tiles, 8, beams), F32),
        ]
        + [((2, slots, 2, r, beams), F32) for r in lv_rows]
        + [((1, 1, 2, cells, beams), F32)],
        (subimages, params, beam_offsets, range_offsets, beam_taps, range_frac, phase_rate),
        flops=20_000_000,
    )

    strip, out_c, out_d = call(
        functools.partial(strip_kernel, slots),
        [((2, cells, beams), BF16)] + [((2, EDGE, (slots + 1) * beams), BF16)] * 2,
        (got_a, got_b, subimages, xt),
        scratch=[((2, beams, cells), BF16)],
        flops=1000,
    )
    got_c = lax.ppermute(out_c, "rng", swap_even("rng"))
    got_d = lax.ppermute(out_d, "rng", swap_odd("rng"))

    def strip_tables(*refs):
        ins, outs, more = refs[:3], refs[6:], refs[3:6]
        strip_tables_kernel(slots, full, *ins, outs[0], outs[1:LEVELS], outs[LEVELS], *outs[LEVELS + 2 :])
        turn_tables(slots, *more, outs[LEVELS + 1])

    ws, es0, es1, os_, th2 = call(
        strip_tables,
        [((LEVELS - 1, 2, beams, beams), BF16)]
        + [((2, 2, r, beams), F32) for r in lv_rows]
        + [((2 * (LEVELS - 1), 8, beams), F32), ((2, tiles, slots, beams), F32)],
        (got_a, got_b, params, bases, got_base, final_phase),
        scratch=[((rows, LANES), F32), ((3, max(m, 8), LANES), F32)],
        flops=20_000_000,
    )
    wide = (slots + 1) * beams
    (inner,) = call(
        functools.partial(interior_kernel, slots),
        [((2, lv_rows[0], wide), BF16)],
        (xt, strip, w1, w2, ws, e0, es0, os_, params),
        scratch=[((2, 2, tiles, cells, LANES), F32)] * 2,
        flops=100_000_000,
    )
    x_rows = cells + 2 * EDGE
    sent, x2 = call(
        functools.partial(levels_kernel, slots),
        [((2, LANES, cells), BF16), ((2, lv_rows[1], wide), BF16)],
        (xt, strip, got_c, got_d, inner, w1, w2, ws, v1, v2, o2, e0, e1, e2, es0, es1, os_, th2, params),
        scratch=[
            ((2, 4 * EDGE, wide), BF16),
            ((2, lv_rows[0], wide), BF16),
            ((2, 2, tiles, x_rows, LANES), F32),
            ((2, 2, tiles, x_rows, LANES), F32),
            ((slots, 2, 2, lv_rows[1], LANES), F32),
            ((2, cells, LANES), F32),
        ],
        flops=200_000_000,
    )
    got = lax.ppermute(sent, "aper", swap_even("aper"))
    (mine,) = call(
        functools.partial(own_half_kernel, slots),
        [((2, LANES, cells), F32)],
        (x2, v1, v2, o2, th2, e2),
        scratch=[((slots, 2, 2, lv_rows[1], LANES), F32), ((2, cells, LANES), F32)],
        flops=20_000_000,
    )
    return (mine + got.astype(F32))[:, None]


def whole_body(*args):
    slots, _, beams, cells = args[0].shape
    fits = (
        lax.axis_size("aper") == 2
        and slots * SEG == beams
        and beams == 2 * LANES
        and cells == LANES
        and slots == 1 << LEVELS - 1
    )
    if not fits:
        return body(*args)
    return fast_body(*args)


def solution(mesh):
    in_specs = (
        P("aper", None, "ang", "rng"),
        P(None, None, None, "ang"),
        P(None, None, None, "ang"),
        P(None, None, None, None, "ang"),
        P(None, None, None, "ang"),
        P("aper", None, None, "ang"),
        P(None, None, "ang"),
        P(None, "ang"),
    )
    out_specs = P(None, "ang", "aper", "rng")
    return jax.shard_map(whole_body, mesh=mesh, in_specs=in_specs, out_specs=out_specs, check_vma=False)
```

```python
import functools
import math

import jax
import jax.numpy as jnp
from jax import lax
from jax.experimental import pallas as pl
from jax.experimental.pallas import tpu as pltpu
from jax.sharding import PartitionSpec as P

LEVELS = 3
TAPS = 4
HALO = 4


def with_halo(cells, sides, width):
    for axis, dim in sides:
        count = lax.axis_size(axis)
        ends = count - 1
        head = lax.slice_in_dim(cells, 0, width, axis=dim)
        tail = lax.slice_in_dim(cells, cells.shape[dim] - width, cells.shape[dim], axis=dim)
        cells = jnp.concatenate(
            [
                lax.ppermute(tail, axis, [(i, (i + 1) % count) for i in range(ends)]),
                cells,
                lax.ppermute(head, axis, [((i + 1) % count, i) for i in range(ends)]),
            ],
            axis=dim,
        )
    return cells


def partner_2(x, axis, stride):
    return lax.ppermute(x, axis, [(i, i ^ 1 << stride) for i in range(lax.axis_size(axis))])


def block_edges(blocks):
    return with_halo(blocks, (("ang", 2), ("rng", 3)), HALO)


def band_matrices(offsets, tap_weights):
    beam_count = offsets.shape[1]
    columns = jnp.arange(beam_count + 2 * HALO, dtype=jnp.int32)
    row_ids = jnp.arange(beam_count, dtype=jnp.int32)
    starting = row_ids[None, :] + HALO + offsets
    lagging = columns[None, None, :] - starting[:, :, None]
    weights = jnp.zeros(lagging.shape, jnp.float32)
    for tap_idx in range(TAPS):
        weights = weights + jnp.where(
            lagging == tap_idx, tap_weights[:, tap_idx, :, None].astype(jnp.float32), 0.0
        )
    return weights.astype(jnp.bfloat16)


def merge_level(child_blocks, halves, level_idx, tables, range_ramp):
    beam_offsets, range_offsets, beam_taps, range_frac, phase_base, phase_rate = tables
    slot_count = halves.shape[0]
    cell_count = range_ramp.shape[0]
    slot_ids = jnp.arange(slot_count, dtype=jnp.int32)
    summed = None
    for side_idx in range(2):
        child_ids = halves if side_idx == 0 else 1 - halves
        extended = child_blocks[side_idx]
        matrices = band_matrices(
            beam_offsets[level_idx][child_ids, halves], beam_taps[level_idx][child_ids, halves]
        )
        interpolated = jnp.einsum(
            "snm,sxmr->sxnr", matrices, extended, preferred_element_type=jnp.float32
        )
        range_shift = range_offsets[level_idx][child_ids, halves] + HALO
        fraction = range_frac[level_idx][child_ids, halves]
        shifted = jnp.zeros(interpolated.shape[:3] + (cell_count,), jnp.float32)
        for offset_step in range(2 * HALO + 1):
            weight = jnp.where(range_shift == offset_step, 1.0 - fraction, 0.0) + jnp.where(
                range_shift + 1 == offset_step, fraction, 0.0
            )
            shifted = (
                shifted
                + weight[:, None, :, None]
                * interpolated[:, :, :, offset_step : offset_step + cell_count]
            )
        angles = (
            phase_base[slot_ids, level_idx, child_ids][:, :, None]
            + phase_rate[level_idx][child_ids][:, :, None] * range_ramp[None, None, :]
        )
        cosine = jnp.cos(angles)
        sine_part = jnp.sin(angles)
        term = jnp.stack(
            [
                cosine * shifted[:, 0] - sine_part * shifted[:, 1],
                sine_part * shifted[:, 0] + cosine * shifted[:, 1],
            ],
            axis=1,
        )
        summed = term if summed is None else summed + term
    return summed.astype(jnp.bfloat16)


def body(
    subimages,
    beam_offsets,
    range_offsets,
    beam_taps,
    range_frac,
    phase_base,
    phase_rate,
    final_phase,
):
    slot_count = subimages.shape[0]
    beam_count = subimages.shape[2]
    cell_count = subimages.shape[3]
    aper_count = lax.axis_size("aper")
    total_subs = slot_count * aper_count
    aper_pos = lax.axis_index("aper")
    full_range = cell_count * lax.axis_size("rng")
    range_ramp = (
        lax.axis_index("rng") * cell_count + jnp.arange(cell_count, dtype=jnp.int32)
    ).astype(jnp.float32) / full_range - 0.5
    tables = (beam_offsets, range_offsets, beam_taps, range_frac, phase_base, phase_rate)
    sub_ids = aper_pos * slot_count + jnp.arange(slot_count, dtype=jnp.int32)
    current = subimages
    for level_idx in range(LEVELS):
        distance = total_subs >> LEVELS - level_idx
        halves = sub_ids // distance % 2
        if distance >= slot_count:
            which_bit = (distance // slot_count).bit_length() - 1
            partner = partner_2(current, "aper", which_bit)
            joined = block_edges(jnp.concatenate([current, partner], 0))
            own_block = joined[:slot_count]
            other_block = joined[slot_count:]
        else:
            own_block = block_edges(current)
            block_shape = own_block.shape
            paired = own_block.reshape(
                (slot_count // (2 * distance), 2, distance) + block_shape[1:]
            )
            other_block = paired[:, ::-1].reshape(block_shape)
        current = merge_level((own_block, other_block), halves, level_idx, tables, range_ramp)
    scale = 1.0 / math.sqrt(total_subs)
    sector = beam_count // aper_count
    regrouped = lax.all_to_all(current[:, None], "aper", split_axis=3, concat_axis=1, tiled=True)
    angles = lax.dynamic_slice_in_dim(final_phase, aper_pos * sector, sector, 1)
    angles = angles.reshape(aper_count, slot_count, sector).transpose(1, 0, 2)
    cosine = jnp.cos(angles)[:, :, :, None]
    sine_part = jnp.sin(angles)[:, :, :, None]
    real_part = regrouped[:, :, 0].astype(jnp.float32)
    imag_part = regrouped[:, :, 1].astype(jnp.float32)
    summed = jnp.stack(
        [
            jnp.sum(cosine * real_part - sine_part * imag_part, axis=(0, 1)),
            jnp.sum(sine_part * real_part + cosine * imag_part, axis=(0, 1)),
        ]
    )
    image = summed * scale
    return image[:, None]


F32 = jnp.float32
BF16 = jnp.bfloat16
LANES = 128
REACH = HALO * LEVELS
EDGE = -(-REACH // 16) * 16
SEG = 4 * EDGE
FIELDS = 3 + TAPS
VMEM_LIMIT = 24 * 1024 * 1024
COVER_FLOPS = 2_000_000_000


def tables_of(slots):
    row = {}
    for lv in range(LEVELS - 1):
        for c in range(2):
            for h in range(2):
                for k in range(FIELDS):
                    row["p", lv, c, h, k] = len(row)
    for s in range(slots):
        for lv in range(LEVELS - 1):
            for c in range(2):
                row["b", s, lv, c] = len(row)
    for lv in range(LEVELS - 1):
        for c in range(2):
            row["r", lv, c] = len(row)
    return row, -(-len(row) // 8) * 8


def half_of(lv, s, total):
    return s // (total >> LEVELS - lv) % 2


def child_of(lv, s, c, total):
    d = total >> LEVELS - lv
    return s - half_of(lv, s, total) * d + c * d


def roll_lanes(x, shift):
    return pltpu.roll(x, shift % LANES, x.ndim - 1) if shift % LANES else x


def iota(shape, dim):
    return lax.broadcasted_iota(jnp.int32, shape, dim)


def blank_kernel(out):
    out[...] = jnp.zeros_like(out)


def pack_kernel(slots, blank, sub, bo, ro, bt, rf, pb, pr, fp, out_a, out_b, p_ref, base_ref):
    row, rows = tables_of(slots)
    beams = p_ref.shape[1]
    for t in range(beams // LANES):
        p_ref[rows - 8 :, t * LANES : (t + 1) * LANES] = blank[...]
    for lv in range(LEVELS - 1):
        for c in range(2):
            for h in range(2):
                at = row["p", lv, c, h, 0]
                p_ref[at : at + 1] = bo[lv, c, h : h + 1, :].astype(F32)
                p_ref[at + 1 : at + 2] = (ro[lv, c, h : h + 1, :] + HALO).astype(F32)
                p_ref[at + 2 : at + 3] = rf[lv, c, h : h + 1, :]
                p_ref[at + 3 : at + 3 + TAPS] = bt[lv, c, h].astype(F32)
            at = row["r", lv, c]
            p_ref[at : at + 1] = pr[lv, c : c + 1, :]
            for s in range(slots):
                at = row["b", s, lv, c]
                p_ref[at : at + 1] = pb[s, lv, c : c + 1, :]
    for c in range(2):
        for s in range(slots):
            base_ref[c * slots + s : c * slots + s + 1] = pb[s, LEVELS - 1, c : c + 1, :]

    per = LANES // EDGE
    beams = p_ref.shape[1]
    lane = iota((8, LANES), 1) // EDGE

    def packed(tile, start):
        parts = []
        for first in range(0, rows // 8, per):
            total = jnp.zeros((8, LANES), F32)
            for g in range(first, min(first + per, rows // 8)):
                piece = p_ref[8 * g : 8 * g + 8, tile : tile + LANES]
                spot = (g - first) * EDGE
                total = jnp.where(lane == g - first, roll_lanes(piece, spot - start), total)
            parts.append(total)
        x = jnp.concatenate(parts, 0)
        high = x.astype(BF16)
        return high, (x - high.astype(F32)).astype(BF16)

    def fill(out, first, tile, start):
        n = slots * 2 * EDGE
        out[:n] = sub[:, :, first : first + EDGE].reshape(n, LANES)
        high, low = packed(tile, start)
        m = high.shape[0]
        out[n : n + m] = high
        out[n + m : n + 2 * m] = low

    even = lax.axis_index("ang") % 2 == 0

    @pl.when(even)
    def _():
        fill(out_a, beams - EDGE, beams - LANES, LANES - EDGE)
        fill(out_b, 0, 0, 0)

    @pl.when(jnp.logical_not(even))
    def _():
        fill(out_a, 0, 0, 0)
        fill(out_b, beams - EDGE, beams - LANES, LANES - EDGE)


def turned(x):
    return x.astype(F32).T.astype(BF16)


def sincos(x):
    k = jnp.floor(x * (2.0 / math.pi) + 0.5)
    r = x - k * 1.5703125
    r = r - k * 4.838267948966e-4
    q = k.astype(jnp.int32)
    z = r * r
    s = r + r * z * (-1.6666654611e-1 + z * (8.3321608736e-3 + z * -1.9515295891e-4))
    c = 1.0 - 0.5 * z + z * z * (4.166664568298827e-2 + z * (-1.388731625493765e-3 + z * 2.443315711809948e-5))
    odd = q % 2 != 0
    sin, cos = jnp.where(odd, c, s), jnp.where(odd, s, c)
    q = q % 4
    return jnp.where(q >= 2, -sin, sin), jnp.where((q == 1) | (q == 2), -cos, cos)


def band(lag, taps):
    out = jnp.zeros(lag.shape, F32)
    for t in range(TAPS):
        out = jnp.where(lag == t, taps[t], out)
    return out.astype(BF16)


def phasors(rate, first, delta, count, low, high, lead, cells, turns, store):
    n = rate.shape[1]
    r8 = iota((8, n), 0)
    small = rate * (r8.astype(F32) * delta)
    other = jnp.where(r8 == 0, rate * (8 * delta), rate * first)
    ss, cs = sincos(small)
    so, co = sincos(other)
    cu, su = co[1:2], so[1:2]
    ck, sk = jnp.broadcast_to(co[0:1], (8, n)), jnp.broadcast_to(so[0:1], (8, n))
    base_re = cs * cu - ss * su
    base_im = ss * cu + cs * su
    for at, turn in enumerate(turns):
        re, im = base_re, base_im
        if turn is not None:
            ct, st = turn
            re, im = re * ct - im * st, im * ct + re * st
        for j in range(count):
            if 8 * j < lead or 8 * j + 8 > lead + cells:
                ids = r8 + 8 * j
                keep = jnp.logical_and(ids >= low, ids < high)
                store(at, j, jnp.where(keep, re, 0.0), jnp.where(keep, im, 0.0))
            else:
                store(at, j, re, im)
            if j + 1 < count:
                re, im = re * ck - im * sk, im * ck + re * sk


def range_place(cells, lv, full):
    lead = (EDGE - HALO * (lv + 1)) if lv < LEVELS - 1 else 0
    at = lax.axis_index("rng") * cells - lead
    first = at.astype(F32) / full - 0.5
    return first, -at, full - at, lead


def rows_of(cells, lv):
    need = cells + 2 * (EDGE - HALO * (lv + 1))
    return -(-need // 16) * 16


def turn_mains_kernel(slots, sub, xt):
    beams = sub.shape[2]
    for s in range(slots):
        for x in range(2):
            xt[x, :, s * beams : (s + 1) * beams] = turned(sub[s, x])


def main_tables_kernel(slots, full, p_ref, bo, ro, bt, rf, pr, w1, w2, v1, v2, o2, f_refs):
    row, _ = tables_of(slots)
    total = 2 * slots
    beams = p_ref.shape[1]
    cells = LANES
    tiles = beams // LANES

    w1[...] = jnp.zeros_like(w1)
    w2[...] = jnp.zeros_like(w2)
    v1[...] = jnp.zeros_like(v1)
    v2[...] = jnp.zeros_like(v2)
    own = lax.axis_index("aper")

    def main_band(first_col, off, taps, put):
        low = max(first_col - 16, 0)
        top = min(first_col + LANES + 16, beams)
        m = iota((top - low, LANES), 0) + low
        p = iota((top - low, LANES), 1) + first_col
        put(low, top, band(m - p - off, taps))

    def strip_band(first_col, off, taps, put):
        if first_col + LANES == beams:
            m = iota((EDGE, LANES), 0) + beams
            put(EDGE, band(m - (iota((EDGE, LANES), 1) + first_col) - off, taps))
        if first_col == 0:
            m = iota((EDGE, LANES), 0) - EDGE
            put(2 * EDGE, band(m - iota((EDGE, LANES), 1) - off, taps))

    for lv in range(LEVELS - 1):
        for c in range(2):
            for h in range(2):
                for t in range(tiles):
                    cols = slice(t * LANES, (t + 1) * LANES)
                    at = row["p", lv, c, h, 0]
                    off = p_ref[at : at + 1, cols].astype(jnp.int32)
                    taps = [p_ref[at + 3 + k : at + 4 + k, cols] for k in range(TAPS)]

                    def put(low, top, v):
                        w1[lv, c, h, low:top, cols] = v

                    main_band(t * LANES, off, taps, put)

                    def put(at_row, v):
                        for s in range(slots):
                            if half_of(lv, s, total) == h:
                                base = child_of(lv, s, c, total) * SEG % LANES + at_row
                                w2[lv, c, s, base : base + EDGE, cols] = v

                    strip_band(t * LANES, off, taps, put)
    lv = LEVELS - 1
    for h in range(2):
        for t in range(tiles):
            cols = slice(t * LANES, (t + 1) * LANES)
            outs = slice(h * LANES, (h + 1) * LANES)
            off = bo[lv, own, h : h + 1, cols]
            tap_rows = bt[lv, own, h, :, cols].astype(F32)
            taps = [tap_rows[k : k + 1] for k in range(TAPS)]

            def put(low, top, v):
                v1[t, low:top, outs] = v

            main_band(t * LANES, off, taps, put)

            def put(at_row, v):
                for par in range(LANES // SEG):
                    base = par * SEG + at_row
                    v2[t, par, base : base + EDGE, outs] = v

            strip_band(t * LANES, off, taps, put)
            o2[t, 0:1, outs] = (ro[lv, own, h : h + 1, cols] + HALO).astype(F32)
            o2[t, 1:2, outs] = rf[lv, own, h : h + 1, cols]

    at = row["b", 0, 0, 0]
    sin_all, cos_all = sincos(p_ref[at : at + slots * (LEVELS - 1) * 2, :])
    for lv in range(LEVELS):
        first, low, high, lead = range_place(cells, lv, full)
        count = (cells + 2 * lead) // 8
        for c in range(2 if lv < LEVELS - 1 else 1):
            turns = [None]
            if lv < LEVELS - 1:
                at = row["r", lv, c]
                rate = p_ref[at : at + 1, :]
                spots = [row["b", s, lv, c] - row["b", 0, 0, 0] for s in range(slots)]
                turns = [(cos_all[k : k + 1], sin_all[k : k + 1]) for k in spots]
            else:
                rate = jnp.where(own == 0, pr[lv, 0:1, :], pr[lv, 1:2, :])

            def store(g, j, re, im):
                f_refs[lv][c, g, 0, 8 * j : 8 * j + 8, :] = re
                f_refs[lv][c, g, 1, 8 * j : 8 * j + 8, :] = im

            phasors(rate, first, 1.0 / full, count, low, high, lead, cells, turns, store)


def strip_kernel(slots, got_a, got_b, sub, xt, strip, out_c, out_d, nat):
    beams = slots * SEG
    even = lax.axis_index("ang") % 2 == 0

    def place(right, left):
        for s in range(slots):
            for x in range(2):
                at = (s * 2 + x) * EDGE
                nat[x, s * SEG + EDGE : s * SEG + 2 * EDGE] = right[at : at + EDGE]
                nat[x, s * SEG + 2 * EDGE : s * SEG + 3 * EDGE] = left[at : at + EDGE]

    for s in range(slots):
        for x in range(2):
            nat[x, s * SEG : s * SEG + EDGE] = sub[s, x, beams - EDGE :]
            nat[x, s * SEG + 3 * EDGE : (s + 1) * SEG] = sub[s, x, :EDGE]

    @pl.when(even)
    def _():
        place(got_a, got_b)

    @pl.when(jnp.logical_not(even))
    def _():
        place(got_b, got_a)

    for x in range(2):
        strip[x] = turned(nat[x])
    cells = strip.shape[1]
    mains = xt.shape[2]

    def send(first, last):
        for x in range(2):
            spot = slice(x * REACH, (x + 1) * REACH)
            first[spot, :mains] = xt[x, cells - REACH :, :]
            first[spot, mains:] = strip[x, cells - REACH :, :]
            last[spot, :mains] = xt[x, :REACH, :]
            last[spot, mains:] = strip[x, :REACH, :]

    even_r = lax.axis_index("rng") % 2 == 0

    @pl.when(even_r)
    def _():
        send(out_c, out_d)

    @pl.when(jnp.logical_not(even_r))
    def _():
        send(out_d, out_c)


def strip_tables_kernel(slots, full, got_a, got_b, p_ref, ws, fs_refs, os_, seg, halo):
    row, rows = tables_of(slots)
    total = 2 * slots
    cells = LANES
    beams = p_ref.shape[1]
    per = LANES // EDGE
    n = slots * 2 * EDGE
    m = (rows // 8 + per - 1) // per * 8
    even = lax.axis_index("ang") % 2 == 0

    def load(right, left):
        halo[0] = right[n : n + m].astype(F32) + right[n + m : n + 2 * m].astype(F32)
        halo[1] = left[n : n + m].astype(F32) + left[n + m : n + 2 * m].astype(F32)

    @pl.when(even)
    def _():
        load(got_a, got_b)

    @pl.when(jnp.logical_not(even))
    def _():
        load(got_b, got_a)

    lane = iota((8, LANES), 1)
    piece_of = lane % SEG // EDGE
    for g in range(rows // 8):
        at = g // per * 8
        spot = g % per * EDGE
        parts = [
            roll_lanes(p_ref[8 * g : 8 * g + 8, beams - LANES :], EDGE - LANES),
            roll_lanes(halo[0, at : at + 8, :], EDGE - spot),
            roll_lanes(halo[1, at : at + 8, :], 2 * EDGE - spot),
            roll_lanes(p_ref[8 * g : 8 * g + 8, :LANES], 3 * EDGE),
        ]
        out = parts[0]
        for k in range(1, 4):
            out = jnp.where(piece_of == k, parts[k], out)
        twice = jnp.where(lane < SEG, out, roll_lanes(out, SEG))
        seg[8 * g : 8 * g + 8, :] = twice

    first_seg = iota((1, LANES), 1) < SEG

    def pick(r0, r1):
        if r0 == r1:
            return seg[r0 : r0 + 1, :]
        return jnp.where(first_seg, seg[r0 : r0 + 1, :], seg[r1 : r1 + 1, :])

    def beam_of(i):
        j = i % SEG
        return jnp.where(j < 2 * EDGE, beams - EDGE + j, j - 3 * EDGE)

    for lv in range(LEVELS - 1):
        first, low, high, lead = range_place(cells, lv, full)
        for c in range(2):
            for t in range(beams // LANES):
                cols = slice(t * LANES, (t + 1) * LANES)
                s0, s1 = 2 * t, 2 * t + 1
                h0, h1 = half_of(lv, s0, total), half_of(lv, s1, total)
                k0, k1 = child_of(lv, s0, c, total), child_of(lv, s1, c, total)
                field = [pick(row["p", lv, c, h0, k], row["p", lv, c, h1, k]) for k in range(FIELDS)]
                at = lv * 2 + c
                os_[at, 0:1, cols] = field[1]
                os_[at, 1:2, cols] = field[2]
                i_row = iota((beams, LANES), 0)
                col = iota((1, LANES), 1)
                wanted = jnp.where(col < SEG, k0, k1)
                lag = beam_of(i_row) - beam_of(col) - field[0].astype(jnp.int32)
                lag = jnp.where(i_row // SEG == wanted, lag, -1)
                ws[lv, c, :, cols] = band(lag, field[3:])
                halo[2, at * 2 + t : at * 2 + t + 1, :] = pick(row["b", s0, lv, c], row["b", s1, lv, c])
    tiles = beams // LANES
    sin_all, cos_all = sincos(halo[2, : 2 * tiles * (LEVELS - 1)])
    for lv in range(LEVELS - 1):
        first, low, high, lead = range_place(cells, lv, full)
        for c in range(2):
            rate = pick(row["r", lv, c], row["r", lv, c])
            at = (lv * 2 + c) * tiles
            turns = [(cos_all[at + t : at + t + 1], sin_all[at + t : at + t + 1]) for t in range(tiles)]

            def store(t, j, re, im):
                cols = slice(t * LANES, (t + 1) * LANES)
                fs_refs[lv][c, 0, 8 * j : 8 * j + 8, cols] = re
                fs_refs[lv][c, 1, 8 * j : 8 * j + 8, cols] = im

            phasors(rate, first, 1.0 / full, (cells + 2 * lead) // 8, low, high, lead, cells, turns, store)


def turn_tables(slots, base_ref, got_base, fp, th2):
    total = 2 * slots
    beams = fp.shape[1]
    own = lax.axis_index("aper")
    scale = 1.0 / math.sqrt(total)
    for h in range(2):
        for t in range(beams // LANES):
            cols = slice(t * LANES, (t + 1) * LANES)
            here = jnp.where(own == 0, base_ref[:slots, cols], base_ref[slots:, cols])
            there = jnp.where(own == 0, got_base[:slots, cols], got_base[slots:, cols])
            angles = jnp.where(own == h, here, there) + fp[h * slots : (h + 1) * slots, cols]
            th2[0, t, :, h * LANES : (h + 1) * LANES] = jnp.cos(angles) * scale
            th2[1, t, :, h * LANES : (h + 1) * LANES] = jnp.sin(angles) * scale


def shift_setup(o_row, f_row, extra):
    shift = o_row.astype(jnp.int32) + extra
    sub = iota((8, LANES), 0)
    reach = sub + shift
    ahead = reach + 1
    return dict(
        one=jnp.broadcast_to(1.0 - f_row, (8, LANES)),
        two=jnp.broadcast_to(f_row, (8, LANES)),
        pick=(reach % 8, ahead % 8),
        tier=((reach < 8, reach < 16), (ahead < 8, ahead < 16)),
    )


def spun(setup, v):
    return [
        jnp.stack([jnp.take_along_axis(v[i], index, axis=0, mode="promise_in_bounds") for i in range(v.shape[0])])
        for index in setup["pick"]
    ]


def mixed(setup, seqs, n, wide):
    parts = []
    for seq, (in0, in1) in zip(seqs, setup["tier"]):
        rest = seq[1 : n + 1]
        if wide:
            rest = jnp.where(in1[None], rest, seq[2 : n + 2])
        parts.append(jnp.where(in0[None], seq[:n], rest))
    return setup["one"][None] * parts[0] + setup["two"][None] * parts[1]


def joined(held, new):
    return new if held is None else [jnp.concatenate([a, b], 0) for a, b in zip(held, new)]


def level_step(slots, total, lv, x_in, spans, tile_at, out, inter, w1, w2, ws, f_main, f_strip, o_main, os_, row):
    beams = slots * SEG
    rows_in = x_in(0, LANES).shape[1]
    order = [slots] + list(range(0, slots, 2)) + list(range(1, slots, 2))
    for turn, g in enumerate(order):
        buf = inter[turn % 2]
        for c in range(2):
            if g < slots:
                k = child_of(lv, g, c, total)
                h = half_of(lv, g, total)
                lhs = x_in(k * beams, beams).reshape(2 * rows_in, beams)
                tile = slots * beams + k * SEG // LANES * LANES
                lhs2 = x_in(tile, LANES).reshape(2 * rows_in, LANES)
                val = jnp.dot(lhs, w1[lv, c, h], preferred_element_type=F32) + jnp.dot(
                    lhs2, w2[lv, c, g], preferred_element_type=F32
                )
            else:
                lhs = x_in(slots * beams, beams).reshape(2 * rows_in, beams)
                val = jnp.dot(lhs, ws[lv, c], preferred_element_type=F32)
            for x in range(2):
                for t in range(beams // LANES):
                    buf[c, x, t, :rows_in, :] = val[x * rows_in : (x + 1) * rows_in, t * LANES : (t + 1) * LANES]
        for t in range(beams // LANES):
            cols = slice(t * LANES, (t + 1) * LANES)
            sets = []
            for c in range(2):
                if g < slots:
                    at = row["p", lv, c, half_of(lv, g, total), 0]
                    sets.append(shift_setup(o_main[at + 1 : at + 2, cols], o_main[at + 2 : at + 3, cols], 0))
                else:
                    at = lv * 2 + c
                    sets.append(shift_setup(os_[at, 0:1, cols], os_[at, 1:2, cols], 0))
            for t0, t1 in spans:
                held = [[None, None], [None, None]]
                step = 4
                done = t0
                while done < t1:
                    n = min(step, t1 - done)
                    acc_re = acc_im = None
                    for c in range(2):
                        moved = []
                        for x in range(2):
                            lo = done if done == t0 else done + 1
                            hi = done + n + 1
                            v = buf[c, x, t, 8 * tile_at(lo) : 8 * (tile_at(hi - 1) + 1), :].reshape(hi - lo, 8, LANES)
                            seqs = joined(held[c][x], spun(sets[c], v))
                            held[c][x] = [seq[n : n + 1] for seq in seqs]
                            moved.append(mixed(sets[c], seqs, n, False))
                        spot = slice(8 * done, 8 * (done + n))
                        if g < slots:
                            fc, fs = f_main[c, g, 0, spot, cols], f_main[c, g, 1, spot, cols]
                        else:
                            fc, fs = f_strip[c, 0, spot, cols], f_strip[c, 1, spot, cols]
                        fc, fs = fc.reshape(n, 8, LANES), fs.reshape(n, 8, LANES)
                        re = fc * moved[0] - fs * moved[1]
                        im = fs * moved[0] + fc * moved[1]
                        acc_re = re if acc_re is None else acc_re + re
                        acc_im = im if acc_im is None else acc_im + im
                    ocols = slice(g * beams + t * LANES, g * beams + (t + 1) * LANES)
                    out[0, 8 * done : 8 * (done + n), ocols] = acc_re.reshape(8 * n, LANES).astype(BF16)
                    out[1, 8 * done : 8 * (done + n), ocols] = acc_im.reshape(8 * n, LANES).astype(BF16)
                    done += n


def last_step(slots, cells, hf, x_in, v1, v2, o2, th2, e2, buf, put):
    rows_in = x_in.shape[1]
    beams = slots * SEG
    for q in list(range(0, slots, 2)) + list(range(1, slots, 2)):
        lhs = x_in[:, :, q * beams : (q + 1) * beams].reshape(2 * rows_in, beams)
        tile = slots * beams + q * SEG // LANES * LANES
        lhs2 = x_in[:, :, tile : tile + LANES].reshape(2 * rows_in, LANES)
        val = jnp.dot(lhs, v1[hf], preferred_element_type=F32) + jnp.dot(
            lhs2, v2[hf, q * SEG % LANES // SEG], preferred_element_type=F32
        )
        for x in range(2):
            for h in range(2):
                buf[q, x, h] = val[x * rows_in : (x + 1) * rows_in, h * LANES : (h + 1) * LANES]
    sets, turn = [], []
    rows2 = o2[hf]
    for h in range(2):
        cols = slice(h * LANES, (h + 1) * LANES)
        sets.append(shift_setup(rows2[0:1, cols], rows2[1:2, cols], HALO))
        cos_rows = th2[0, hf]
        sin_rows = th2[1, hf]
        turn.append(
            [
                [jnp.broadcast_to(cos_rows[q : q + 1, cols], (8, LANES))[None] for q in range(slots)],
                [jnp.broadcast_to(sin_rows[q : q + 1, cols], (8, LANES))[None] for q in range(slots)],
            ]
        )
    n_out = cells // 8
    held = [[None, None], [None, None]]
    done = 0
    step = 4
    while done < n_out:
        n = min(step, n_out - done)
        sum_re = sum_im = None
        for h in range(2):
            lo = 0 if done == 0 else done + 2
            hi = done + n + 2
            re = im = None
            for q in range(slots):
                a = buf[q, 0, h, 8 * lo : 8 * hi, :].reshape(hi - lo, 8, LANES)
                b = buf[q, 1, h, 8 * lo : 8 * hi, :].reshape(hi - lo, 8, LANES)
                tc, ts = turn[h][0][q], turn[h][1][q]
                pr_, pi_ = tc * a - ts * b, ts * a + tc * b
                re = pr_ if re is None else re + pr_
                im = pi_ if im is None else im + pi_
            moved = []
            for x, v in enumerate((re, im)):
                seqs = joined(held[h][x], spun(sets[h], v))
                held[h][x] = [seq[n : n + 2] for seq in seqs]
                moved.append(mixed(sets[h], seqs, n, True))
            sum_re = moved[0] if sum_re is None else sum_re + moved[0]
            sum_im = moved[1] if sum_im is None else sum_im + moved[1]
        at = pl.ds(pl.multiple_of(hf * LANES, LANES), LANES)
        ec = e2[0, 0, 0, 8 * done : 8 * (done + n), at].reshape(n, 8, LANES)
        es = e2[0, 0, 1, 8 * done : 8 * (done + n), at].reshape(n, 8, LANES)
        put(done, n, ec * sum_re - es * sum_im, es * sum_re + ec * sum_im)
        done += n


def inner_rows(cells):
    return 2 * EDGE // 16, cells // 8


def interior_kernel(slots, xt, strip, w1, w2, ws, e0, es0, e1, es1, os_, p_ref, x1, x2, inter0, inter1):
    row, _ = tables_of(slots)
    mains = xt.shape[2]
    low, top = inner_rows(xt.shape[1])

    def get(lane, width):
        return xt[:, :, lane : lane + width] if lane < mains else strip[:, :, lane - mains : lane - mains + width]

    level_step(slots, 2 * slots, 0, get, [(low, top)], lambda v: v - low, x1, (inter0, inter1), w1, w2, ws, e0, es0, p_ref, os_, row)

    def again(lane, width):
        return x1[:, 8 * low : 8 * top, lane : lane + width]

    level_step(slots, 2 * slots, 1, again, [(low, top - 2)], lambda v: v - low, x2, (inter0, inter1), w1, w2, ws, e1, es1, p_ref, os_, row)


def levels_kernel(slots, xt, strip, got_c, got_d, inner, inner2, w1, w2, ws, v1, v2, o2, e0, e1, e2, es0, es1, os_, th2, p_ref, out, x2, x0, x1, inter0, inter1, buf, flat):
    row, _ = tables_of(slots)
    total = 2 * slots
    cells = xt.shape[1]
    mains = xt.shape[2]
    low, top = inner_rows(cells)
    for x in range(2):
        for at, spot in ((EDGE, slice(0, EDGE)), (2 * EDGE, slice(cells - EDGE, cells))):
            x0[x, at : at + EDGE, :mains] = xt[x, spot]
            x0[x, at : at + EDGE, mains:] = strip[x, spot]
        x1[x, 8 * low : 8 * low + 16] = inner[x, 8 * low : 8 * low + 16]
        x1[x, 8 * top - 16 : 8 * top] = inner[x, 8 * top - 16 : 8 * top]
        x2[x, 8 * low : 8 * top - 16] = inner2[x, 8 * low : 8 * top - 16]
        for at in (0, 3 * EDGE):
            x0[x, at : at + EDGE, :] = jnp.zeros((EDGE, x0.shape[2]), BF16)
    even = lax.axis_index("rng") % 2 == 0

    def place(right, left):
        for x in range(2):
            spot = slice(x * REACH, (x + 1) * REACH)
            x0[x, EDGE - REACH : EDGE, :] = left[spot]
            x0[x, 3 * EDGE : 3 * EDGE + REACH, :] = right[spot]

    @pl.when(even)
    def _():
        place(got_c, got_d)

    @pl.when(jnp.logical_not(even))
    def _():
        place(got_d, got_c)

    inter = (inter0, inter1)
    edge_tiles = EDGE // 4
    spans = [(0, low), (top, (cells + 2 * (EDGE - HALO)) // 8)]
    level_step(slots, total, 0, lambda lane, width: x0[:, :, lane : lane + width], spans, lambda v: v if v < edge_tiles else v - (cells + 2 * EDGE) // 8 + 2 * edge_tiles, x1, inter, w1, w2, ws, e0, es0, p_ref, os_, row)
    first, last = 8 * low + 16, 8 * top - 16

    def ends(lane, width):
        lanes = slice(lane, lane + width)
        return jnp.concatenate([x1[:, :first, lanes], x1[:, last:, lanes]], 1)

    spans = [(0, low), (top - 2, x2.shape[1] // 8)]
    level_step(slots, total, 1, ends, spans, lambda v: v if v < first // 8 else v - (last - first) // 8, x2, inter, w1, w2, ws, e1, es1, p_ref, os_, row)
    hf = 1 - lax.axis_index("aper")

    def put(done, n, re, im):
        flat[0, 8 * done : 8 * (done + n), :] = re.reshape(8 * n, LANES)
        flat[1, 8 * done : 8 * (done + n), :] = im.reshape(8 * n, LANES)

    last_step(slots, cells, hf, x2, v1, v2, o2, th2, e2, buf, put)
    for x in range(2):
        out[x] = flat[x].T.astype(BF16)


def own_half_kernel(slots, x2, v1, v2, o2, th2, e2, out, buf, flat):
    cells = out.shape[2]
    hf = lax.axis_index("aper")

    def put(done, n, re, im):
        flat[0, 8 * done : 8 * (done + n), :] = re.reshape(8 * n, LANES)
        flat[1, 8 * done : 8 * (done + n), :] = im.reshape(8 * n, LANES)

    last_step(slots, cells, hf, x2, v1, v2, o2, th2, e2, buf, put)
    for x in range(2):
        out[x] = flat[x].T


def swap_even(axis):
    n = lax.axis_size(axis)
    return [(i, i ^ 1) for i in range(n) if i ^ 1 < n]


def swap_odd(axis):
    n = lax.axis_size(axis)
    pairs = []
    for i in range(1, n - 1, 2):
        pairs += [(i, i + 1), (i + 1, i)]
    return pairs


def call(kernel, outs, args, scratch=(), sems=(), flops=0, specs=None):
    vm = pl.BlockSpec(memory_space=pltpu.VMEM)
    return pl.pallas_call(
        kernel,
        out_shape=[jax.ShapeDtypeStruct(s, d) for s, d in outs],
        in_specs=specs or [vm] * len(args),
        out_specs=[vm] * len(outs),
        scratch_shapes=[pltpu.VMEM(s, d) for s, d in scratch] + list(sems),
        compiler_params=pltpu.CompilerParams(vmem_limit_bytes=VMEM_LIMIT),
        cost_estimate=pl.CostEstimate(flops=flops, bytes_accessed=0, transcendentals=0),
    )(*args)


def fast_body(*args):
    slots, _, beams, cells = args[0].shape
    full = cells * lax.axis_size("rng")
    _, rows = tables_of(slots)
    m = (rows // 8 + LANES // EDGE - 1) // (LANES // EDGE) * 8
    msg = slots * 2 * EDGE + 2 * m
    lv_rows = [rows_of(cells, lv) for lv in range(LEVELS - 1)]
    tiles = beams // LANES
    subimages, beam_offsets, range_offsets, beam_taps, range_frac, _, phase_rate, final_phase = args
    (blank,) = call(blank_kernel, [((8, LANES), F32)], (), flops=COVER_FLOPS)
    out_a, out_b, params, bases = call(
        functools.partial(pack_kernel, slots),
        [((msg, LANES), BF16), ((msg, LANES), BF16), ((rows, beams), F32), ((2 * slots, beams), F32)],
        (blank,) + args,
        flops=1000,
    )
    got_a = lax.ppermute(out_a, "ang", swap_even("ang"))
    got_b = lax.ppermute(out_b, "ang", swap_odd("ang"))
    got_base = lax.ppermute(bases, "aper", swap_even("aper"))

    def main_tables(*refs):
        ins, xt, outs = refs[1:7], refs[7], refs[8:]
        turn_mains_kernel(slots, refs[0], xt)
        main_tables_kernel(slots, full, *ins, *outs[:5], outs[5:])

    xt, w1, w2, v1, v2, o2, e0, e1, e2 = call(
        main_tables,
        [
            ((2, cells, slots * beams), BF16),
            ((LEVELS - 1, 2, 2, beams, beams), BF16),
            ((LEVELS - 1, 2, slots, LANES, beams), BF16),
            ((tiles, beams, beams), BF16),
            ((tiles, LANES // SEG, LANES, beams), BF16),
            ((tiles, 8, beams), F32),
        ]
        + [((2, slots, 2, r, beams), F32) for r in lv_rows]
        + [((1, 1, 2, cells, beams), F32)],
        (subimages, params, beam_offsets, range_offsets, beam_taps, range_frac, phase_rate),
        flops=20_000_000,
    )

    strip, out_c, out_d = call(
        functools.partial(strip_kernel, slots),
        [((2, cells, beams), BF16)] + [((2 * REACH, (slots + 1) * beams), BF16)] * 2,
        (got_a, got_b, subimages, xt),
        scratch=[((2, beams, cells), BF16)],
        flops=1000,
    )
    got_c = lax.ppermute(out_c, "rng", swap_even("rng"))
    got_d = lax.ppermute(out_d, "rng", swap_odd("rng"))

    def strip_tables(*refs):
        ins, outs, more = refs[:3], refs[6:], refs[3:6]
        strip_tables_kernel(slots, full, *ins, outs[0], outs[1:LEVELS], outs[LEVELS], *outs[LEVELS + 2 :])
        turn_tables(slots, *more, outs[LEVELS + 1])

    ws, es0, es1, os_, th2 = call(
        strip_tables,
        [((LEVELS - 1, 2, beams, beams), BF16)]
        + [((2, 2, r, beams), F32) for r in lv_rows]
        + [((2 * (LEVELS - 1), 8, beams), F32), ((2, tiles, slots, beams), F32)],
        (got_a, got_b, params, bases, got_base, final_phase),
        scratch=[((rows, LANES), F32), ((3, max(m, 8), LANES), F32)],
        flops=20_000_000,
    )
    wide = (slots + 1) * beams
    inner, inner2 = call(
        functools.partial(interior_kernel, slots),
        [((2, lv_rows[0], wide), BF16), ((2, lv_rows[1], wide), BF16)],
        (xt, strip, w1, w2, ws, e0, es0, e1, es1, os_, params),
        scratch=[((2, 2, tiles, cells, LANES), F32)] * 2,
        flops=100_000_000,
    )
    x_rows = cells + 2 * EDGE
    sent, x2 = call(
        functools.partial(levels_kernel, slots),
        [((2, LANES, cells), BF16), ((2, lv_rows[1], wide), BF16)],
        (xt, strip, got_c, got_d, inner, inner2, w1, w2, ws, v1, v2, o2, e0, e1, e2, es0, es1, os_, th2, params),
        scratch=[
            ((2, 4 * EDGE, wide), BF16),
            ((2, lv_rows[0], wide), BF16),
            ((2, 2, tiles, x_rows, LANES), F32),
            ((2, 2, tiles, x_rows, LANES), F32),
            ((slots, 2, 2, lv_rows[1], LANES), F32),
            ((2, cells, LANES), F32),
        ],
        flops=200_000_000,
    )
    got = lax.ppermute(sent, "aper", swap_even("aper"))
    (mine,) = call(
        functools.partial(own_half_kernel, slots),
        [((2, LANES, cells), F32)],
        (x2, v1, v2, o2, th2, e2),
        scratch=[((slots, 2, 2, lv_rows[1], LANES), F32), ((2, cells, LANES), F32)],
        flops=20_000_000,
    )
    return (mine + got.astype(F32))[:, None]


def whole_body(*args):
    slots, _, beams, cells = args[0].shape
    fits = (
        lax.axis_size("aper") == 2
        and slots * SEG == beams
        and beams == 2 * LANES
        and cells == LANES
        and slots == 1 << LEVELS - 1
    )
    if not fits:
        return body(*args)
    return fast_body(*args)


def solution(mesh):
    in_specs = (
        P("aper", None, "ang", "rng"),
        P(None, None, None, "ang"),
        P(None, None, None, "ang"),
        P(None, None, None, None, "ang"),
        P(None, None, None, "ang"),
        P("aper", None, None, "ang"),
        P(None, None, "ang"),
        P(None, "ang"),
    )
    out_specs = P(None, "ang", "aper", "rng")
    return jax.shard_map(whole_body, mesh=mesh, in_specs=in_specs, out_specs=out_specs, check_vma=False)
```
